32 devices in a mesh: grp: 2 (over core), gx: 4 (over z), gy: 4 (over y, x).
Axes of the slice: x: 2, y: 2, z: 4, core: 2. Of those that a mesh axis runs over, the one named last changes fastest.
Arguments:
- coarse_ez: float32 [256, 1024], P('gx', ('grp', 'gy')), may hold values from -6 to 6
- coarse_hx: float32 [256, 1024], P('gx', ('grp', 'gy')), may hold values from -6 to 6
- coarse_hy: float32 [256, 1024], P('gx', ('grp', 'gy')), may hold values from -6 to 6
- coarse_ids: int32 [256, 1024], P('gx', ('grp', 'gy')), may hold values from 0 to 7
- mat_eps: float32 [8], replicated, may hold values from 1 to 12
- mat_sig: float32 [8], replicated, may hold values from 0 to 0.5
- fine_ez: float32 [4, 8, 32, 2304], P(None, ('grp', 'gy'), 'gx'), may hold values from -6 to 6
- fine_hx: float32 [4, 8, 32, 2304], P(None, ('grp', 'gy'), 'gx'), may hold values from -6 to 6
- fine_hy: float32 [4, 8, 32, 2304], P(None, ('grp', 'gy'), 'gx'), may hold values from -6 to 6
- fine_ids: int32 [4, 8, 32, 2304], P(None, ('grp', 'gy'), 'gx'), may hold values from 0 to 7
- boxes: int32 [4, 8, 32, 4], P('gx', ('grp', 'gy')), may hold values from 1 to 14, as said below
- src_cells: int32 [4], replicated, may hold values from 0 to 262143
- src_wave: float32 [3, 4], replicated, may hold values from -6 to 6
- rcv_cells: int32 [128], replicated, may hold values from 0 to 262143
Outputs:
- end_ez: float32 [256, 1024], P('gx', ('grp', 'gy'))
- end_hx: float32 [256, 1024], P('gx', ('grp', 'gy'))
- end_hy: float32 [256, 1024], P('gx', ('grp', 'gy'))
- end_fine_ez: float32 [4, 8, 32, 2304], P(None, ('grp', 'gy'), 'gx')
- end_fine_hx: float32 [4, 8, 32, 2304], P(None, ('grp', 'gy'), 'gx')
- end_fine_hy: float32 [4, 8, 32, 2304], P(None, ('grp', 'gy'), 'gx')
- traces: float32 [3, 128], replicated
The draws below stay inside these ranges and needn't reach their ends.
Inputs may be any that keep to these rules, and one draw needn't show every extreme that they name: `boxes`: each box lies one cell or more inside its tile: corner + size <= 15; sizes are 4 to 14, drawn independently for every subgrid.
All inputs are finite; a program needn't handle non-finite values.
Results may differ from the reference program's by a relative error of at most 0.00011.
Values sent between devices are 32-bit elements; how exact they have to be, the bound alone decides.
No kernel may reach another device: no remote copies, remote signals or barrier semaphores. Data moves between devices by JAX's collectives and lax.ppermute only.
A program may use at most 64 MiB of HBM per device.

```python
import math
import jax
import jax.numpy as jnp

TILE = 16
FINE = 48
CAP = 32
STEPS = 3
NMAT = 8
NSRC = 4
NRCV = 128
BLOCKS_X = 4
BLOCKS_Y = 8
NX = 256
NY = 1024


def draw_boxes(key, part):
    first, second, third, fourth = jax.random.split(jax.random.fold_in(key, 17), 4)
    shape = (BLOCKS_X, BLOCKS_Y, CAP)
    size_i = jax.random.randint(first, shape, 4, TILE - 1)
    size_j = jax.random.randint(second, shape, 4, TILE - 1)
    corner_i = jax.random.randint(third, shape, 1, TILE - size_i)
    corner_j = jax.random.randint(fourth, shape, 1, TILE - size_j)
    return jnp.stack([corner_i, corner_j, size_i, size_j], -1).astype(jnp.int32)


def plant(entries, stream_key, low, largest):
    shape = entries.shape
    index_at = [jax.random.randint(jax.random.fold_in(stream_key, axis), (), 0, shape[axis]) for axis in range(len(shape))]
    entries = entries.at[tuple(index_at)].set(low)
    longest = shape.index(max(shape))
    index_at[longest] = (index_at[longest] + 1) % shape[longest]
    return entries.at[tuple(index_at)].set(largest)


def block_levels(key, dims, shards, least, top_value):
    level = 1.0
    for axis_at, shards_of in shards:
        steps = jax.random.uniform(jax.random.fold_in(jax.random.fold_in(key, 6), axis_at), (shards_of,), jnp.float32, least / len(shards), top_value / len(shards))
        level = level * jnp.repeat(jnp.exp(steps), dims[axis_at] // shards_of).reshape((-1,) + (1,) * (len(dims) - 1 - axis_at))
    return level


def bell_draw(rng, dims, spread, reach, cuts=(), kind=jnp.bfloat16):
    entries = spread * jax.random.normal(rng, dims, jnp.float32)
    if cuts:
        entries = entries * block_levels(rng, dims, cuts, -0.22, 0.18)
    return jnp.clip(entries, -reach, reach).astype(kind)


def setup_inputs(seed: int = 0) -> dict:
    splits = jax.random.split(jax.random.key(seed), 15)
    return {
        "coarse_ez": bell_draw(splits[0], (NX, NY), 1.0, 6.0, ((0, 4), (1, 8)), jnp.float32),
        "coarse_hx": bell_draw(splits[1], (NX, NY), 1.0, 6.0, ((0, 4), (1, 8)), jnp.float32),
        "coarse_hy": bell_draw(splits[2], (NX, NY), 1.0, 6.0, ((0, 4), (1, 8)), jnp.float32),
        "coarse_ids": plant(jax.random.randint(splits[3], (NX, NY), 0, NMAT), jax.random.fold_in(splits[3], 1), 0, NMAT - 1).astype(jnp.int32),
        "mat_eps": jnp.clip(jnp.exp(jax.random.uniform(splits[4], (NMAT,), jnp.float32, math.log(1.0), math.log(12.0))), 1.0, 12.0),
        "mat_sig": jnp.clip(jax.random.uniform(splits[5], (NMAT,), jnp.float32, 0.0, 0.5), 0.0, 0.5),
        "fine_ez": bell_draw(splits[6], (BLOCKS_X, BLOCKS_Y, CAP, FINE * FINE), 1.0, 6.0, ((1, 8), (2, 4)), jnp.float32),
        "fine_hx": bell_draw(splits[7], (BLOCKS_X, BLOCKS_Y, CAP, FINE * FINE), 1.0, 6.0, ((1, 8), (2, 4)), jnp.float32),
        "fine_hy": bell_draw(splits[8], (BLOCKS_X, BLOCKS_Y, CAP, FINE * FINE), 1.0, 6.0, ((1, 8), (2, 4)), jnp.float32),
        "fine_ids": plant(jax.random.randint(splits[9], (BLOCKS_X, BLOCKS_Y, CAP, FINE * FINE), 0, NMAT), jax.random.fold_in(splits[9], 1), 0, NMAT - 1).astype(jnp.int32),
        "boxes": draw_boxes(jax.random.fold_in(splits[14], 71), 0),
        "src_cells": plant(jax.random.randint(splits[11], (NSRC,), 0, NX * NY), jax.random.fold_in(splits[11], 1), 0, (NX * NY) - 1).astype(jnp.int32),
        "src_wave": bell_draw(splits[12], (STEPS, NSRC), 1.0, 6.0, (), jnp.float32),
        "rcv_cells": plant(jax.random.randint(splits[13], (NRCV,), 0, NX * NY), jax.random.fold_in(splits[13], 1), 0, (NX * NY) - 1).astype(jnp.int32),
    }


COURANT = 0.5
HCOEF = 0.5


def coefficients(ids, eps_table, sig_table, ratio):
    damp = jnp.zeros(ids.shape, jnp.float32)
    gain = jnp.zeros(ids.shape, jnp.float32)
    for material in range(eps_table.shape[0]):
        loss = sig_table[material] / (eps_table[material] * ratio)
        hit = ids == material
        damp = jnp.where(hit, (1.0 - loss) / (1.0 + loss), damp)
        gain = jnp.where(hit, COURANT / (eps_table[material] * (1.0 + loss)), gain)
    return damp, gain


def box_masks(boxes, cells, scale):
    coarse_of = jnp.arange(cells, dtype=jnp.int32) // scale
    low_i = boxes[..., 0:1]
    low_j = boxes[..., 1:2]
    high_i = low_i + boxes[..., 2:3]
    high_j = low_j + boxes[..., 3:4]
    rows_in = (coarse_of >= low_i) & (coarse_of < high_i)
    cols_in = (coarse_of >= low_j) & (coarse_of < high_j)
    rows_mid = (coarse_of > low_i) & (coarse_of < high_i - 1)
    cols_mid = (coarse_of > low_j) & (coarse_of < high_j - 1)
    inbox = rows_in[..., :, None] & cols_in[..., None, :]
    middle = rows_mid[..., :, None] & cols_mid[..., None, :]
    return inbox, middle


def flat_masks(boxes):
    width = TILE * 3
    index = jnp.arange(width * width, dtype=jnp.int32)
    coarse_i = index // width // 3
    coarse_j = index % width // 3
    low_i = boxes[..., 0:1]
    low_j = boxes[..., 1:2]
    high_i = low_i + boxes[..., 2:3]
    high_j = low_j + boxes[..., 3:4]
    inbox = (coarse_i >= low_i) & (coarse_i < high_i) & (coarse_j >= low_j) & (coarse_j < high_j)
    middle = (coarse_i > low_i) & (coarse_i < high_i - 1) & (coarse_j > low_j) & (coarse_j < high_j - 1)
    return inbox, middle


def to_tiles(field, blocks_x, blocks_y):
    rows, cols = field.shape
    along_x = rows // blocks_x // TILE
    along_y = cols // blocks_y // TILE
    shaped = field.reshape(blocks_x, along_x, TILE, blocks_y, along_y, TILE)
    shaped = shaped.transpose(0, 3, 1, 4, 2, 5)
    return shaped.reshape(blocks_x, blocks_y, along_x * along_y, TILE, TILE)


def from_tiles(tiles, block_rows, block_cols):
    blocks_x, blocks_y = tiles.shape[0], tiles.shape[1]
    along_x = block_rows // TILE
    along_y = block_cols // TILE
    shaped = tiles.reshape(blocks_x, blocks_y, along_x, along_y, TILE, TILE)
    shaped = shaped.transpose(0, 2, 4, 1, 3, 5)
    return shaped.reshape(blocks_x * block_rows, blocks_y * block_cols)


def pad_last(array, before, after):
    widths = [(0, 0)] * (array.ndim - 1) + [(before, after)]
    return jnp.pad(array, widths)


def fine_substep(fine_ez, fine_hx, fine_hy, damp, gain, inbox, middle, border, cycle_value):
    width = TILE * 3
    column = jnp.arange(width * width, dtype=jnp.int32) % width
    ez_next_col = jnp.where(column < width - 1, pad_last(fine_ez[..., 1:], 0, 1), 0.0)
    ez_next_row = pad_last(fine_ez[..., width:], 0, width)
    fine_hx = jnp.where(inbox, fine_hx - HCOEF * (ez_next_col - fine_ez), 0.0)
    fine_hy = jnp.where(inbox, fine_hy + HCOEF * (ez_next_row - fine_ez), 0.0)
    hy_prev = pad_last(fine_hy[..., :-width], width, 0)
    hx_prev = jnp.where(column > 0, pad_last(fine_hx[..., :-1], 1, 0), 0.0)
    curl = (fine_hy - hy_prev) - (fine_hx - hx_prev)
    inner = damp * fine_ez + gain * curl
    fine_ez = jnp.where(middle, inner, jnp.where(border, cycle_value, 0.0))
    return fine_ez, fine_hx, fine_hy


def upsample(tiles):
    lead = tiles.shape[:-2]
    wide = jnp.repeat(jnp.repeat(tiles, 3, axis=-2), 3, axis=-1)
    return wide.reshape(lead + (TILE * TILE * 9,))


def cell_means(fine_ez):
    lead = fine_ez.shape[:-1]
    shaped = fine_ez.reshape(lead + (TILE, 3, TILE, 3))
    return jnp.sum(shaped, axis=(-3, -1)) / 9.0


def fine_round(fine_ez, fine_hx, fine_hy, damp, gain, inbox, middle, border, old_tiles, new_tiles):
    for sub in range(1, 4):
        weight = sub / 3.0
        cycle_value = upsample((1.0 - weight) * old_tiles + weight * new_tiles)
        fine_ez, fine_hx, fine_hy = fine_substep(fine_ez, fine_hx, fine_hy, damp, gain, inbox, middle, border, cycle_value)
    return fine_ez, fine_hx, fine_hy


def reference(coarse_ez, coarse_hx, coarse_hy, coarse_ids, mat_eps, mat_sig, fine_ez, fine_hx, fine_hy, fine_ids, boxes, src_cells, src_wave, rcv_cells):
    blocks_x = boxes.shape[0]
    blocks_y = boxes.shape[1]
    rows, cols = coarse_ez.shape
    block_rows = rows // blocks_x
    block_cols = cols // blocks_y
    damp, gain = coefficients(coarse_ids, mat_eps, mat_sig, 1.0)
    fine_damp, fine_gain = coefficients(fine_ids, mat_eps, mat_sig, 3.0)
    inbox, middle = flat_masks(boxes)
    border = inbox & jnp.logical_not(middle)
    coarse_mid = from_tiles(box_masks(boxes, TILE, 1)[1], block_rows, block_cols)
    ez, hx, hy = coarse_ez, coarse_hx, coarse_hy
    samples = []
    for step in range(STEPS):
        ez_next_col = jnp.pad(ez[:, 1:], ((0, 0), (0, 1)))
        ez_next_row = jnp.pad(ez[1:, :], ((0, 1), (0, 0)))
        hx = hx - HCOEF * (ez_next_col - ez)
        hy = hy + HCOEF * (ez_next_row - ez)
        hy_prev = jnp.pad(hy[:-1, :], ((1, 0), (0, 0)))
        hx_prev = jnp.pad(hx[:, :-1], ((0, 0), (1, 0)))
        curl = (hy - hy_prev) - (hx - hx_prev)
        drive = jnp.zeros((rows * cols,), jnp.float32).at[src_cells].add(src_wave[step]).reshape(rows, cols)
        new = damp * ez + gain * curl + drive
        old_tiles = to_tiles(ez, blocks_x, blocks_y)
        new_tiles = to_tiles(new, blocks_x, blocks_y)
        fine_ez, fine_hx, fine_hy = fine_round(fine_ez, fine_hx, fine_hy, fine_damp, fine_gain, inbox, middle, border, old_tiles, new_tiles)
        back = from_tiles(cell_means(fine_ez), block_rows, block_cols)
        ez = jnp.where(coarse_mid, back, new)
        samples.append(ez.reshape(-1)[rcv_cells])
    return ez, hx, hy, fine_ez, fine_hx, fine_hy, jnp.stack(samples)
```

```python
import functools

import jax
import jax.numpy as jnp
from jax import lax
from jax.experimental import pallas as pl
from jax.experimental.pallas import tpu as pltpu
from jax.sharding import PartitionSpec as P

TILE = 16
STEPS = 3
SUBSTEPS = 3
LANES = 128
FIELDS = 4
WINDOW = 24
BOX_ROW = FIELDS * WINDOW
MESSAGE = BOX_ROW + 8
PLANES = 9

COURANT = 0.5
HCOEF = 0.5
F32 = jnp.float32
BF16 = jnp.bfloat16
I32 = jnp.int32
COLS = ("grp", "gy")


def iota(shape, axis):
    return lax.broadcasted_iota(I32, shape, axis)


def vmem():
    return pl.BlockSpec(memory_space=pltpu.VMEM)


def smem():
    return pl.BlockSpec(memory_space=pltpu.SMEM)


def params():
    return pltpu.CompilerParams(vmem_limit_bytes=24 * 1024 * 1024)


def cost(flops):
    return pl.CostEstimate(flops=flops, bytes_accessed=1 << 20, transcendentals=0)


def call(kernel, outs, ins, args, scratch=(), flops=1 << 20):
    return pl.pallas_call(
        kernel,
        out_shape=outs,
        in_specs=ins,
        out_specs=jax.tree.map(lambda _: vmem(), outs),
        scratch_shapes=list(scratch),
        compiler_params=params(),
        cost_estimate=cost(flops),
    )(*args)


def f32(*shape):
    return jax.ShapeDtypeStruct(shape, F32)


def ring(value, axis, steps):
    count = lax.axis_size(axis)
    return lax.ppermute(value, axis, [(k, (k + steps) % count) for k in range(count)])


def pack_kernel(owners, ez, hx, hy, ids, boxes, *outs):
    me = lax.axis_index("gx")
    tiles = ez.shape[0] // 8
    sub = iota((8, LANES), 0)
    for d in range(owners):
        g = lax.rem(me + d, owners)
        here = pl.multiple_of(g * TILE, TILE)
        after = pl.multiple_of(lax.rem(2 * g + 2, tiles) * 8, 8)
        before = pl.multiple_of(lax.rem(2 * g + tiles - 1, tiles) * 8, 8)
        for f, ref in enumerate((ez, hx, hy, ids)):
            outs[d][f * WINDOW : f * WINDOW + TILE, :] = ref[pl.ds(here, TILE), :].astype(F32)
            edge = jnp.where(sub < 4, ref[pl.ds(after, 8), :], ref[pl.ds(before, 8), :])
            outs[d][f * WINDOW + TILE : (f + 1) * WINDOW, :] = edge.astype(F32)
        outs[d][BOX_ROW:MESSAGE, :] = jnp.zeros((8, LANES), F32)
        some = boxes[pl.ds(pl.multiple_of(g * 8, 8), 8), :]
        outs[d][BOX_ROW:MESSAGE, 0:4] = some.astype(F32)


def block_of(owners, d):
    return lax.rem(lax.axis_index("gx") + owners - d, owners)


def assemble(owners, received, store):
    me = lax.axis_index("gx")
    sub = iota((8, LANES), 0)
    for d in range(owners):
        store[block_of(owners, d)] = received[d][...]
    for f in range(FIELDS):
        at = f * WINDOW + TILE
        edges = [store[a, at : at + 8, :] for a in range(owners)]
        for a in range(owners):
            before = jnp.where(me == 0, edges[max(a - 1, 0)], edges[a])
            after = jnp.where(me == owners - 1, edges[min(a + 1, owners - 1)], edges[a])
            store[a, at : at + 8, :] = jnp.where(sub < 4, after, before)


def edges_kernel(owners, *refs):
    received, out, store = refs[:owners], refs[owners], refs[owners + 1]
    assemble(owners, received, store)
    lane = iota((WINDOW, LANES), 1)
    total = jnp.zeros((WINDOW, LANES), F32)
    for a in range(owners):
        for f in range(FIELDS):
            at = 8 * (a * FIELDS + f)
            moved = pltpu.roll(store[a, f * WINDOW : (f + 1) * WINDOW, :], at + 3, 1)
            total = jnp.where((lane >= at) & (lane < at + 6), moved, total)
    out[...] = total


def source_lane(t):
    plane = t >> 7
    u = (plane * 11) >> 5
    v = plane - 3 * u
    return (3 * ((t >> 4) & 7) + u) * (3 * TILE) + 3 * (t & 15) + v


def halves(x):
    high = x.astype(BF16)
    return high, (x - high.astype(F32)).astype(BF16)


def materials(ids, eps, sig, ratio):
    damp = jnp.zeros(ids.shape, F32)
    gain = jnp.zeros(ids.shape, F32)
    ones = jnp.ones((8, LANES), F32)
    for m in range(eps.shape[0]):
        e, s = ones * eps[m], ones * sig[m]
        loss = s / (e * ratio)
        d = (1.0 - loss) / (1.0 + loss)
        g = COURANT / (e * (1.0 + loss))
        hit = ids == float(m)
        damp = jnp.where(hit, jnp.broadcast_to(d[0:1, 0:1], ids.shape), damp)
        gain = jnp.where(hit, jnp.broadcast_to(g[0:1, 0:1], ids.shape), gain)
    return damp, gain


def spread_kernel(eps, sig, fez, fhx, fhy, ids, oez, ohx, ohy, odamp, ogain, left):
    count = fez.shape[0]
    rows = 2 * count
    span = PLANES * LANES
    for h in range(2):
        lanes = slice(h * span, (h + 1) * span)
        for f, ref in enumerate((fez, fhx, fhy)):
            high, low = halves(ref[:, lanes])
            left[2 * f * rows + h * count : 2 * f * rows + (h + 1) * count, :] = high
            left[(2 * f + 1) * rows + h * count : (2 * f + 1) * rows + (h + 1) * count, :] = low
        at = 6 * rows + h * count
        left[at : at + count, :] = ids[:, lanes].astype(F32).astype(BF16)

    def emit(plane, planes):
        width = planes * LANES
        want = source_lane(plane * LANES + iota((1, width), 1))
        table = jnp.where(iota((span, width), 0) == want, 1.0, 0.0).astype(BF16)
        got = jnp.dot(left[...], table, preferred_element_type=F32)
        parts = [got[k * rows : (k + 1) * rows] for k in range(7)]
        damp, gain = materials(parts[6], eps, sig, 3.0)
        for ref, value in (
            (oez, parts[0] + parts[1]),
            (ohx, 2.0 * (parts[2] + parts[3])),
            (ohy, 2.0 * (parts[4] + parts[5])),
            (odamp, damp),
            (ogain, 0.5 * gain),
        ):
            for k in range(planes):
                ref[plane + k] = value[:, k * LANES : (k + 1) * LANES]

    def pair(n, carry):
        emit(2 * n, 2)
        return carry

    lax.fori_loop(0, PLANES // 2, pair, 0)
    emit(PLANES - 1, 1)


def gather_kernel(ez, hx, hy, oez, ohx, ohy, left):
    rows = ez.shape[1]
    count = rows // 2
    span = PLANES * LANES
    for f, ref in enumerate((ez, hx, hy)):
        for p in range(PLANES):
            high, low = halves(ref[p])
            left[2 * f * rows : (2 * f + 1) * rows, p * LANES : (p + 1) * LANES] = high
            left[(2 * f + 1) * rows : (2 * f + 2) * rows, p * LANES : (p + 1) * LANES] = low

    def emit(at, width):
        have = source_lane(iota((span, width), 0))
        table = jnp.where(have == iota((span, width), 1) + at, 1.0, 0.0).astype(BF16)
        got = jnp.dot(left[...], table, preferred_element_type=F32)
        for f, ref in enumerate((oez, ohx, ohy)):
            value = got[2 * f * rows : (2 * f + 1) * rows] + got[(2 * f + 1) * rows : (2 * f + 2) * rows]
            for h in range(2):
                start = pl.multiple_of(h * span + at, LANES)
                ref[:, pl.ds(start, width)] = value[h * count : (h + 1) * count]

    def pair(n, carry):
        emit(pl.multiple_of(n * 2 * LANES, LANES), 2 * LANES)
        return carry

    lax.fori_loop(0, PLANES // 2, pair, 0)
    emit((PLANES - 1) * LANES, LANES)


def swap_blocks(x):
    block = iota((8, LANES), 1) >> 4
    sub = iota((8, LANES), 0)
    x = jnp.take_along_axis(x, (block + sub) & 7, axis=0)
    x = pltpu.roll(x, 0, 1, stride=TILE, stride_axis=0)
    return jnp.take_along_axis(x, (block - sub) & 7, axis=0)


def step_kernel(owners, all_rows, all_cols, *refs):
    received = refs[:owners]
    from_left, from_right, fez, fhx, fhy, fdamp, fgain = refs[owners : owners + 7]
    eps, sig, src, wave, rcv = refs[owners + 7 : owners + 12]
    at = owners + 12
    oez, ohx, ohy = refs[at : at + 3]
    back = refs[at + 3 : at + 3 + owners]
    trace = refs[at + 3 + owners]
    scratch = refs[at + 4 + owners :]
    store, ez, hx, hy, damp, gain, half, drive, mid, cyc, box, held, mdamp, mgain = scratch
    wide = 2 * LANES
    me = lax.axis_index("gx")
    column = lax.axis_index("grp") * lax.axis_size("gy") + lax.axis_index("gy")
    rows = owners * TILE

    assemble(owners, received, store)
    lane = iota((WINDOW, LANES), 1)
    row = iota((WINDOW, wide), 0)
    row = jnp.where(row < 20, row, row - WINDOW)
    col = iota((WINDOW, wide), 1)
    col = jnp.where(col < LANES + 64, col, col - wide)
    all_col = col + column * LANES
    cells = []
    for a in range(owners):
        all_row = row + (a * rows + me * TILE)
        valid = (all_row >= 0) & (all_row < all_rows) & (all_col >= 0) & (all_col < all_cols)
        cells.append(jnp.where(valid, all_row * all_cols + all_col, -1))
        fields = []
        for f in range(FIELDS):
            k = 8 * (a * FIELDS + f)
            after = pltpu.roll(from_right[...], LANES - (k + 3), 1)
            before = pltpu.roll(from_left[...], (LANES - 3 - k) % LANES, 1)
            side = jnp.where(lane < 3, after, jnp.where(lane >= LANES - 3, before, 0.0))
            main = store[a, f * WINDOW : (f + 1) * WINDOW, :]
            both = jnp.concatenate([main, side], axis=1)
            fields.append(jnp.where(valid, both, 0.0))
        ez[a], hx[a], hy[a] = fields[:3]
        d, g = materials(fields[3], eps, sig, 1.0)
        damp[a] = jnp.where(valid, d, 0.0)
        gain[a] = jnp.where(valid, g, 0.0)
        half[a] = jnp.where(valid, HCOEF, 0.0)
    for n in range(STEPS):
        for a in range(owners):
            total = jnp.zeros((WINDOW, wide), F32)
            for k in range(src.shape[0]):
                total = total + jnp.where(cells[a] == src[k], wave[n, k], 0.0)
            drive[n, a] = total

    tile_lane = iota((8, LANES), 1)
    tile_col = (tile_lane & 15).astype(F32)
    for a in range(owners):
        sizes = store[a, BOX_ROW:MESSAGE, :]
        low_i, low_j, size_i, size_j = (sizes[:, k : k + 1] for k in range(4))
        high_i, high_j = low_i + size_i, low_j + size_j
        for h in range(2):
            i = (8 * h + (tile_lane >> 4)).astype(F32)
            inside = (i >= low_i) & (i < high_i) & (tile_col >= low_j) & (tile_col < high_j)
            middle = (i > low_i) & (i < high_i - 1) & (tile_col > low_j) & (tile_col < high_j - 1)
            at_rows = slice((h * owners + a) * 8, (h * owners + a + 1) * 8)
            mid[at_rows] = jnp.where(middle, 1.0, 0.0)
            box[at_rows] = jnp.where(inside, 1.0, 0.0)
            held[at_rows] = swap_blocks(ez[a, 8 * h : 8 * h + 8, 0:LANES])
    for p in range(PLANES):
        mdamp[p] = fdamp[p] * mid[...]
        mgain[p] = fgain[p] * mid[...]
        oez[p], ohx[p], ohy[p] = fez[p], fhx[p], fhy[p]

    count = 8 * owners
    lanes = iota((count, LANES), 1)
    first, second = slice(0, count), slice(count, 2 * count)

    def after_row(ref, p):
        a, b = (pltpu.roll(ref[p, s], LANES - TILE, 1) for s in (first, second))
        return jnp.where(lanes < LANES - TILE, a, b), b

    def before_row(ref, p):
        a, b = (pltpu.roll(ref[p, s], TILE, 1) for s in (first, second))
        return a, jnp.where(lanes < TILE, a, b)

    def substep(m, new_tiles):
        weight = (m + 1).astype(F32) * (1.0 / SUBSTEPS)
        cyc[...] = (box[...] - mid[...]) * ((1.0 - weight) * held[...] + weight * new_tiles)
        down = [after_row(oez, v) for v in range(3)]
        for u in range(3):
            for v in range(3):
                p = 3 * u + v
                for h, s in enumerate((first, second)):
                    e = oez[p, s]
                    right = oez[p + 1, s] if v < 2 else pltpu.roll(oez[3 * u, s], LANES - 1, 1)
                    below = oez[p + 3, s] if u < 2 else down[v][h]
                    ohx[p, s] = ohx[p, s] - (right - e)
                    ohy[p, s] = ohy[p, s] + (below - e)
        up = [before_row(ohy, 6 + v) for v in range(3)]
        for u in range(3):
            for v in range(3):
                p = 3 * u + v
                for h, s in enumerate((first, second)):
                    left = ohx[p - 1, s] if v > 0 else pltpu.roll(ohx[3 * u + 2, s], 1, 1)
                    above = ohy[p - 3, s] if u > 0 else up[v][h]
                    curl = (ohy[p, s] - above) - (ohx[p, s] - left)
                    oez[p, s] = mdamp[p, s] * oez[p, s] + mgain[p, s] * curl + cyc[s]
        return new_tiles

    def step(n, carry):
        for a in range(owners):
            e = ez[a]
            x = hx[a] - half[a] * (pltpu.roll(e, wide - 1, 1) - e)
            y = hy[a] + half[a] * (pltpu.roll(e, WINDOW - 1, 0) - e)
            curl = (y - pltpu.roll(y, 1, 0)) - (x - pltpu.roll(x, 1, 1))
            hx[a], hy[a] = x, y
            ez[a] = damp[a] * e + gain[a] * curl + drive[n, a]
        new_tiles = jnp.concatenate(
            [
                swap_blocks(ez[a, 8 * h : 8 * h + 8, 0:LANES])
                for h in range(2)
                for a in range(owners)
            ],
            axis=0,
        )
        lax.fori_loop(0, SUBSTEPS, substep, new_tiles)
        total = oez[0]
        for p in range(1, PLANES):
            total = total + oez[p]
        now = jnp.where(mid[...] > 0.0, total / 9.0, new_tiles)
        held[...] = now
        picked = []
        for a in range(owners):
            for h in range(2):
                image = swap_blocks(now[(h * owners + a) * 8 : (h * owners + a + 1) * 8])
                ez[a, 8 * h : 8 * h + 8, 0:LANES] = image
                picked.append(image)
        image = jnp.concatenate(picked, axis=0)
        block = iota((owners * TILE, LANES), 0)
        image_row = (block >> 4) * rows + me * TILE + (block & 15)
        row_hit = jnp.where(image_row == rcv[0:1, :], 1.0, 0.0)
        col_hit = iota((LANES, rcv.shape[1]), 0) + column * LANES == rcv[1:2, :]
        mixed = lax.dot_general(
            image,
            row_hit,
            (((0,), (0,)), ((), ())),
            precision=lax.Precision.HIGHEST,
            preferred_element_type=F32,
        )
        trace[pl.ds(n, 1), :] = jnp.sum(jnp.where(col_hit, mixed, 0.0), axis=0, keepdims=True)
        return carry

    trace[...] = jnp.zeros(trace.shape, F32)
    lax.fori_loop(0, STEPS, step, 0)
    for p in range(PLANES):
        ohx[p] = 0.5 * (ohx[p] * box[...])
        ohy[p] = 0.5 * (ohy[p] * box[...])
    for d in range(owners):
        a = block_of(owners, d)
        for f, ref in enumerate((ez, hx, hy)):
            back[d][f * TILE : (f + 1) * TILE, :] = ref[a, 0:TILE, 0:LANES]


def place_kernel(owners, *refs):
    pieces = refs[:owners]
    traces = refs[owners]
    outs = refs[owners + 1 : owners + 4]
    out_trace = refs[owners + 4]
    me = lax.axis_index("gx")
    for d in range(owners):
        g = lax.rem(me + d, owners)
        for f in range(3):
            outs[f][pl.ds(pl.multiple_of(g * TILE, TILE), TILE), :] = pieces[d][f * TILE : (f + 1) * TILE, :]
    out_trace[...] = jnp.sum(traces[...], axis=0)[0:STEPS]


def fast_shards(
    all_rows,
    coarse_ez,
    coarse_hx,
    coarse_hy,
    coarse_ids,
    mat_eps,
    mat_sig,
    fine_ez,
    fine_hx,
    fine_hy,
    fine_ids,
    boxes,
    src_cells,
    src_wave,
    rcv_cells,
):
    owners = lax.axis_size("gx")
    rows, cols = coarse_ez.shape
    all_cols = cols * lax.axis_size(COLS)
    fine_shape = fine_ez.shape
    count = fine_shape[0] * fine_shape[2]
    receivers = rcv_cells.shape[0]
    flat = [x.reshape(count, fine_shape[-1]) for x in (fine_ez, fine_hx, fine_hy, fine_ids)]
    messages = call(
        functools.partial(pack_kernel, owners),
        tuple(f32(MESSAGE, cols) for _ in range(owners)),
        [vmem()] * 5,
        (coarse_ez, coarse_hx, coarse_hy, coarse_ids, boxes.reshape(boxes.shape[2:])),
    )
    received = [messages[0]] + [ring(messages[d], "gx", d) for d in range(1, owners)]
    planes = call(
        spread_kernel,
        tuple(f32(PLANES, 2 * count, LANES) for _ in range(5)),
        [smem()] * 2 + [vmem()] * 4,
        (mat_eps, mat_sig, *flat),
        [pltpu.VMEM((14 * count, PLANES * LANES), BF16)],
        1 << 31,
    )
    edges = call(
        functools.partial(edges_kernel, owners),
        f32(WINDOW, LANES),
        [vmem()] * owners,
        received,
        [pltpu.VMEM((owners, MESSAGE, LANES), F32)],
    )
    from_left = ring(edges, COLS, 1)
    from_right = ring(edges, COLS, -1)
    picks = jnp.stack([rcv_cells // all_cols, rcv_cells % all_cols])
    window = (owners, WINDOW, 2 * LANES)
    tiles = (2 * count, LANES)
    results = call(
        functools.partial(step_kernel, owners, all_rows, all_cols),
        tuple(f32(PLANES, 2 * count, LANES) for _ in range(3))
        + tuple(f32(3 * TILE, LANES) for _ in range(owners))
        + (f32(8, receivers),),
        [vmem()] * (owners + 7) + [smem()] * 4 + [vmem()],
        (*received, from_left, from_right, *planes, mat_eps, mat_sig, src_cells, src_wave, picks),
        [pltpu.VMEM((owners, MESSAGE, LANES), F32)]
        + [pltpu.VMEM(window, F32)] * 6
        + [pltpu.VMEM((STEPS,) + window, F32)]
        + [pltpu.VMEM(tiles, F32)] * 4
        + [pltpu.VMEM((PLANES,) + tiles, F32)] * 2,
        1 << 30,
    )
    fine, back, trace = results[:3], results[3 : 3 + owners], results[3 + owners]
    every = ("grp", "gx", "gy")
    copies = jnp.broadcast_to(trace[None], (lax.axis_size(every),) + trace.shape)
    traces = lax.all_to_all(copies, every, 0, 0)
    pieces = [back[0]] + [ring(back[d], "gx", owners - d) for d in range(1, owners)]
    finals = call(
        gather_kernel,
        tuple(f32(count, fine_shape[-1]) for _ in range(3)),
        [vmem()] * 3,
        fine,
        [pltpu.VMEM((12 * count, PLANES * LANES), BF16)],
        1 << 31,
    )
    ends = call(
        functools.partial(place_kernel, owners),
        tuple(f32(rows, cols) for _ in range(3)) + (f32(STEPS, receivers),),
        [vmem()] * (owners + 1),
        (*pieces, traces),
    )
    return (*ends[:3], *(x.reshape(fine_shape) for x in finals), ends[3])


def passed_along(value, axis, steps):
    count = lax.axis_size(axis)
    initial, last = (max(0, -steps), min(count, count - steps))
    return lax.ppermute(value, axis, [(source, source + steps) for source in range(initial, last)])


def coefficients(ids, eps_table, sig_table, ratio):
    damp = jnp.zeros(ids.shape, jnp.float32)
    gain = jnp.zeros(ids.shape, jnp.float32)
    for material in range(eps_table.shape[0]):
        loss = sig_table[material] / (eps_table[material] * ratio)
        hit = ids == material
        damp = jnp.where(hit, (1.0 - loss) / (1.0 + loss), damp)
        gain = jnp.where(hit, COURANT / (eps_table[material] * (1.0 + loss)), gain)
    return (damp, gain)


def box_masks(boxes, cells, scale):
    coarse_of = jnp.arange(cells, dtype=jnp.int32) // scale
    low_i = boxes[..., 0:1]
    low_j = boxes[..., 1:2]
    high_i = low_i + boxes[..., 2:3]
    high_j = low_j + boxes[..., 3:4]
    rows_in = (coarse_of >= low_i) & (coarse_of < high_i)
    cols_in = (coarse_of >= low_j) & (coarse_of < high_j)
    rows_mid = (coarse_of > low_i) & (coarse_of < high_i - 1)
    cols_mid = (coarse_of > low_j) & (coarse_of < high_j - 1)
    inbox = rows_in[..., :, None] & cols_in[..., None, :]
    middle = rows_mid[..., :, None] & cols_mid[..., None, :]
    return (inbox, middle)


def flat_masks(boxes):
    width = TILE * 3
    index = jnp.arange(width * width, dtype=jnp.int32)
    coarse_i = index // width // 3
    coarse_j = index % width // 3
    low_i = boxes[:, 0:1]
    low_j = boxes[:, 1:2]
    high_i = low_i + boxes[:, 2:3]
    high_j = low_j + boxes[:, 3:4]
    inbox = (coarse_i >= low_i) & (coarse_i < high_i) & (coarse_j >= low_j) & (coarse_j < high_j)
    middle = (
        (coarse_i > low_i) & (coarse_i < high_i - 1) & (coarse_j > low_j) & (coarse_j < high_j - 1)
    )
    return (inbox, middle)


def spread_table():
    width = TILE * 3
    index = jnp.arange(width * width, dtype=jnp.int32)
    owner = index // width // 3 * TILE + index % width // 3
    return (jnp.arange(TILE * TILE, dtype=jnp.int32)[:, None] == owner[None, :]).astype(jnp.float32)


def to_flat_tiles(field):
    rows, cols = field.shape
    along_x = rows // TILE
    along_y = cols // TILE
    shaped = field.reshape(along_x, TILE, along_y, TILE).transpose(0, 2, 1, 3)
    return shaped.reshape(1, 1, along_x * along_y, TILE * TILE)


def from_tiles(tiles, block_rows, block_cols):
    along_x = block_rows // TILE
    along_y = block_cols // TILE
    shaped = tiles.reshape(along_x, along_y, TILE, TILE).transpose(0, 2, 1, 3)
    return shaped.reshape(block_rows, block_cols)


def pad_last(array, before, after):
    widths = [(0, 0)] * (array.ndim - 1) + [(before, after)]
    return jnp.pad(array, widths)


def fine_substep(fine_ez, fine_hx, fine_hy, damp, gain, inbox, middle, border, cycle_value):
    width = TILE * 3
    column = jnp.arange(width * width, dtype=jnp.int32) % width
    ez_next_col = jnp.where(column < width - 1, pad_last(fine_ez[..., 1:], 0, 1), 0.0)
    ez_next_row = pad_last(fine_ez[..., width:], 0, width)
    fine_hx = jnp.where(inbox, fine_hx - HCOEF * (ez_next_col - fine_ez), 0.0)
    fine_hy = jnp.where(inbox, fine_hy + HCOEF * (ez_next_row - fine_ez), 0.0)
    hy_prev = pad_last(fine_hy[..., :-width], width, 0)
    hx_prev = jnp.where(column > 0, pad_last(fine_hx[..., :-1], 1, 0), 0.0)
    curl = fine_hy - hy_prev - (fine_hx - hx_prev)
    inner = damp * fine_ez + gain * curl
    fine_ez = jnp.where(middle, inner, jnp.where(border, cycle_value, 0.0))
    return (fine_ez, fine_hx, fine_hy)


def fine_round(
    fine_ez, fine_hx, fine_hy, damp, gain, inbox, middle, border, old_tiles, new_tiles, spread
):
    for sub in range(1, 4):
        weight = sub / 3.0
        mixed = (1.0 - weight) * old_tiles + weight * new_tiles
        cycle_value = jnp.dot(
            mixed, spread, precision=lax.Precision.HIGHEST, preferred_element_type=jnp.float32
        )
        fine_ez, fine_hx, fine_hy = fine_substep(
            fine_ez, fine_hx, fine_hy, damp, gain, inbox, middle, border, cycle_value
        )
    return (fine_ez, fine_hx, fine_hy)


def coarse_magnetic(ez, hx, hy):
    below = passed_along(ez[:1, :], "gx", -1)
    beside = passed_along(ez[:, :1], ("grp", "gy"), -1)
    ez_next_row = jnp.concatenate([ez[1:, :], below], axis=0)
    ez_next_col = jnp.concatenate([ez[:, 1:], beside], axis=1)
    hx = hx - HCOEF * (ez_next_col - ez)
    hy = hy + HCOEF * (ez_next_row - ez)
    above = passed_along(hy[-1:, :], "gx", 1)
    before = passed_along(hx[:, -1:], ("grp", "gy"), 1)
    hy_prev = jnp.concatenate([above, hy[:-1, :]], axis=0)
    hx_prev = jnp.concatenate([before, hx[:, :-1]], axis=1)
    curl = hy - hy_prev - (hx - hx_prev)
    return (hx, hy, curl)


def shards(
    coarse_ez,
    coarse_hx,
    coarse_hy,
    coarse_ids,
    mat_eps,
    mat_sig,
    fine_ez,
    fine_hx,
    fine_hy,
    fine_ids,
    boxes,
    src_cells,
    src_wave,
    rcv_cells,
):
    rows, cols = coarse_ez.shape
    fine_shape = fine_ez.shape
    flat_cells = fine_shape[-1]
    means_shape = fine_shape[:-1] + (TILE * TILE,)
    row_start = lax.axis_index("gx") * rows
    col_start = lax.axis_index(("grp", "gy")) * cols
    all_cols = cols * lax.axis_size(("grp", "gy"))
    spread = spread_table()
    damp, gain = coefficients(coarse_ids, mat_eps, mat_sig, 1.0)
    fine_damp, fine_gain = coefficients(fine_ids.reshape(-1, flat_cells), mat_eps, mat_sig, 3.0)
    owned_boxes = lax.all_to_all(boxes, "gx", split_axis=2, concat_axis=0, tiled=True).reshape(
        -1, 4
    )
    inbox, middle = flat_masks(owned_boxes)
    border = inbox & jnp.logical_not(middle)
    coarse_mid = from_tiles(box_masks(boxes, TILE, 1)[1], rows, cols)
    src_rows = (
        jnp.arange(rows, dtype=jnp.int32)[None, :] == (src_cells // all_cols - row_start)[:, None]
    ).astype(jnp.float32)
    src_cols = (
        jnp.arange(cols, dtype=jnp.int32)[None, :] == (src_cells % all_cols - col_start)[:, None]
    ).astype(jnp.float32)
    rcv_rows = (
        jnp.arange(rows, dtype=jnp.int32)[None, :] == (rcv_cells // all_cols - row_start)[:, None]
    ).astype(jnp.float32)
    rcv_cols = (
        jnp.arange(cols, dtype=jnp.int32)[None, :] == (rcv_cells % all_cols - col_start)[:, None]
    ).astype(jnp.float32)
    ez, hx, hy = (coarse_ez, coarse_hx, coarse_hy)
    field_ez = fine_ez.reshape(-1, flat_cells)
    field_hx = fine_hx.reshape(-1, flat_cells)
    field_hy = fine_hy.reshape(-1, flat_cells)
    held = lax.all_to_all(to_flat_tiles(ez), "gx", split_axis=2, concat_axis=0, tiled=True).reshape(
        -1, TILE * TILE
    )
    samples = []
    for step in range(STEPS):
        hx, hy, curl = coarse_magnetic(ez, hx, hy)
        weighted = src_rows * src_wave[step][:, None]
        drive = jnp.dot(
            weighted.T,
            src_cols,
            precision=lax.Precision.HIGHEST,
            preferred_element_type=jnp.float32,
        )
        new = damp * ez + gain * curl + drive
        old_tiles = held
        new_tiles = lax.all_to_all(
            to_flat_tiles(new), "gx", split_axis=2, concat_axis=0, tiled=True
        ).reshape(-1, TILE * TILE)
        held = new_tiles
        field_ez, field_hx, field_hy = fine_round(
            field_ez,
            field_hx,
            field_hy,
            fine_damp,
            fine_gain,
            inbox,
            middle,
            border,
            old_tiles,
            new_tiles,
            spread,
        )
        sums = lax.dot_general(
            field_ez,
            spread,
            (((1,), (1,)), ((), ())),
            precision=lax.Precision.HIGHEST,
            preferred_element_type=jnp.float32,
        )
        means = (sums / 9.0).reshape(means_shape)
        back = lax.all_to_all(means, "gx", split_axis=0, concat_axis=2, tiled=True)
        ez = jnp.where(coarse_mid, from_tiles(back, rows, cols), new)
        picked = jnp.dot(
            rcv_rows, ez, precision=lax.Precision.HIGHEST, preferred_element_type=jnp.float32
        )
        samples.append(jnp.sum(picked * rcv_cols, axis=1))
    traces = lax.psum(jnp.stack(samples), ("grp", "gx", "gy"))
    return (
        ez,
        hx,
        hy,
        field_ez.reshape(fine_shape),
        field_hx.reshape(fine_shape),
        field_hy.reshape(fine_shape),
        traces,
    )


def solution(mesh):
    placed = (
        P("gx", ("grp", "gy")),
        P("gx", ("grp", "gy")),
        P("gx", ("grp", "gy")),
        P("gx", ("grp", "gy")),
        P(),
        P(),
        P(None, ("grp", "gy"), "gx", None),
        P(None, ("grp", "gy"), "gx", None),
        P(None, ("grp", "gy"), "gx", None),
        P(None, ("grp", "gy"), "gx", None),
        P("gx", ("grp", "gy"), None, None),
        P(),
        P(),
        P(),
    )
    def body(*args):
        rows, cols = args[0].shape
        owned = args[6].shape[2] * TILE
        if cols == LANES and owned == cols and rows == lax.axis_size("gx") * TILE:
            return fast_shards(rows * lax.axis_size("gx"), *args)
        return shards(*args)

    return jax.shard_map(
        body,
        mesh=mesh,
        in_specs=placed,
        out_specs=(
            P("gx", ("grp", "gy")),
            P("gx", ("grp", "gy")),
            P("gx", ("grp", "gy")),
            P(None, ("grp", "gy"), "gx", None),
            P(None, ("grp", "gy"), "gx", None),
            P(None, ("grp", "gy"), "gx", None),
            P(),
        ),
        check_vma=False,
    )
```

```python
import functools

import jax
import jax.numpy as jnp
from jax import lax
from jax.experimental import pallas as pl
from jax.experimental.pallas import tpu as pltpu
from jax.sharding import PartitionSpec as P

TILE = 16
STEPS = 3
SUBSTEPS = 3
LANES = 128
FIELDS = 4
WINDOW = 24
HALO = FIELDS * TILE
MESSAGE = HALO + 24
PLANES = 9
WIDE = 2 * LANES
GROUP = 6

COURANT = 0.5
HCOEF = 0.5
F32 = jnp.float32
BF16 = jnp.bfloat16
I32 = jnp.int32
COLS = ("grp", "gy")


def iota(shape, axis):
    return lax.broadcasted_iota(I32, shape, axis)


def f32(*shape):
    return jax.ShapeDtypeStruct(shape, F32)


def kept(*shape, dtype=F32):
    return pltpu.VMEM(shape, dtype)


def call(kernel, outs, args, scratch=(), far=(), near=(), far_outs=(), flops=1 << 20):
    vmem, hbm = (pl.BlockSpec(memory_space=m) for m in (pltpu.VMEM, pltpu.HBM))
    args = [
        pltpu.with_memory_space_constraint(x, pltpu.HBM)
        if k in far
        else pltpu.with_memory_space_constraint(x, pltpu.VMEM)
        if k in near
        else x
        for k, x in enumerate(args)
    ]
    return pl.pallas_call(
        kernel,
        out_shape=outs,
        in_specs=[hbm if k in far else vmem for k in range(len(args))],
        out_specs=tuple(hbm if k in far_outs else vmem for k in range(len(outs))),
        scratch_shapes=list(scratch),
        compiler_params=pltpu.CompilerParams(vmem_limit_bytes=16 * 1024 * 1024),
        cost_estimate=pl.CostEstimate(flops=flops, bytes_accessed=1 << 20, transcendentals=0),
    )(*args)


def copies(sources, targets, sems):
    moves = [
        pltpu.make_async_copy(source, target, sems.at[k])
        for k, (source, target) in enumerate(zip(sources, targets))
    ]
    for move in moves:
        move.start()
    return moves


def ring(value, axis, steps):
    count = lax.axis_size(axis)
    return lax.ppermute(value, axis, [(k, (k + steps) % count) for k in range(count)])


def pack_kernel(owners, *refs):
    sources, outs = refs[:11], refs[11 : 11 + owners]
    coarse_kinds, fine_kinds = refs[11 + owners : 13 + owners]
    fine, held = refs[13 + owners : 17 + owners], refs[17 + owners : 22 + owners]
    kinds, sems = refs[22 + owners : 24 + owners], refs[24 + owners]
    moves = copies(sources, (*held, *kinds, *fine), sems)
    for move in moves[:7]:
        move.wait()
    count = kinds[0].shape[0]
    for ref, ratio, scale in zip((coarse_kinds, fine_kinds), (1.0, 3.0), (1.0, 0.5)):
        for m, (damp, gain) in enumerate(lists(*kinds, ratio)):
            ref[m : m + 1, :] = damp
            ref[count + m : count + m + 1, :] = scale * gain
    ez, hx, hy, ids, boxes = held
    me = lax.axis_index("gx")
    tiles = ez.shape[0] // 8
    count = boxes.shape[1]
    sub = iota((8, LANES), 0)
    lines = jnp.concatenate([boxes[...].astype(F32), jnp.zeros((4, LANES - count), F32)], axis=1)
    low, high, left, top = (jnp.broadcast_to(lines[k : k + 1, :], (8, LANES)) for k in range(4))
    for d in range(owners):
        g = lax.rem(me + d, owners)
        here = pl.multiple_of(g * TILE, TILE)
        after = pl.multiple_of(lax.rem(2 * g + 2, tiles) * 8, 8)
        before = pl.multiple_of(lax.rem(2 * g + tiles - 1, tiles) * 8, 8)
        edges = []
        for f, ref in enumerate((ez, hx, hy, ids)):
            outs[d][f * TILE : (f + 1) * TILE, :] = ref[pl.ds(here, TILE), :].astype(F32)
            edge = jnp.where(sub < 4, ref[pl.ds(after, 8), :], ref[pl.ds(before, 8), :])
            edges.append(edge.astype(F32))
        around_ez, around_hx, around_hy, around_ids = edges
        outs[d][HALO : HALO + 8, :] = jnp.where(sub == 3, low, jnp.where(sub == 4, high, around_ez))
        inner = jnp.where(sub < 4, pltpu.roll(around_ids, 2, 0), pltpu.roll(around_ids, 6, 0))
        outs[d][HALO + 8 : HALO + 16, :] = jnp.where((sub >= 2) & (sub < 6), inner, around_hx)
        outs[d][HALO + 16 : HALO + 24, :] = jnp.where(
            sub == 2, left, jnp.where(sub == 3, top, around_hy)
        )
    for move in moves[7:]:
        move.wait()


def block_of(owners, d):
    return lax.rem(lax.axis_index("gx") + owners - d, owners)


def edges_kernel(owners, *refs):
    received, table = refs[:owners], refs[owners]
    out, windows, boxes, store = refs[owners + 1 :]
    me = lax.axis_index("gx")
    sub = iota((8, LANES), 0)
    for d in range(owners):
        store[block_of(owners, d)] = received[d][...]
    around = [
        [store[a, HALO + 8 * k : HALO + 8 * k + 8, :] for a in range(owners)] for k in range(3)
    ]
    row = iota((WINDOW, LANES), 0)
    row = jnp.where(row < 20, row, row - WINDOW)
    lane = iota((WINDOW, LANES), 1)
    total = jnp.zeros((WINDOW, LANES), F32)
    for a in range(owners):
        for k, at in enumerate((3, 4, 18, 19)):
            boxes[a, k : k + 1, :] = store[a, HALO + at : HALO + at + 1, :]
        tiles = []
        for tile in around:
            after = jnp.where(me == owners - 1, tile[min(a + 1, owners - 1)], tile[a])
            before = jnp.where(me == 0, tile[max(a - 1, 0)], tile[a])
            tiles.append(jnp.where(sub < 4, after, before))
        inner = jnp.where(sub < 4, pltpu.roll(tiles[1], 6, 0), pltpu.roll(tiles[1], 2, 0))
        fields = [
            jnp.concatenate([store[a, f * TILE : (f + 1) * TILE, :], tile], axis=0)
            for f, tile in enumerate((*tiles, inner))
        ]
        all_row = row + (a * owners * TILE + me * TILE)
        valid = (all_row >= 0) & (all_row < owners * owners * TILE)
        damp = jnp.zeros((WINDOW, LANES), F32)
        gain = jnp.zeros((WINDOW, LANES), F32)
        kinds = table.shape[0] // 2
        for m in range(kinds):
            hit = fields[3] == float(m)
            damp = jnp.where(hit, table[m : m + 1, :], damp)
            gain = jnp.where(hit, table[kinds + m : kinds + m + 1, :], gain)
        for f, value in enumerate((*fields[:3], damp, gain)):
            value = jnp.where(valid, value, 0.0)
            windows[f, a] = value
            at = GROUP * (f * owners + a)
            total = jnp.where((lane >= at) & (lane < at + GROUP), pltpu.roll(value, at + 3, 1), total)
    out[...] = total


def lane_of():
    return iota((8, LANES), 1)


def third_of(x, start):
    return lax.rem(x + start, 3)


def choose(parts, which):
    return jnp.where(which == 0, parts[0], jnp.where(which == 1, parts[1], parts[2]))


def take(x, lanes):
    return jnp.take_along_axis(x, lanes & (LANES - 1), axis=1)


def in_block(block):
    return ((block & 7) << 4) | (lane_of() & 15)


def halves(x):
    high = x.astype(BF16)
    return high, (x - high.astype(F32)).astype(BF16)


def thirds(x):
    high = x.astype(BF16)
    rest = x - high.astype(F32)
    return high, *halves(rest)


def lists(eps, sig, ratio):
    ones = jnp.ones((1, LANES), F32)
    both = []
    for m in range(eps.shape[0]):
        e, s = ones * eps[m], ones * sig[m]
        loss = s / (e * ratio)
        both.append(((1.0 - loss) / (1.0 + loss), COURANT / (e * (1.0 + loss))))
    return both


def each_group(count, body):
    def group(n, carry):
        tiles = pl.ds(pl.multiple_of(8 * n, 8), 8)
        for h in range(2):
            body(h, tiles, pl.ds(pl.multiple_of(h * count + 8 * n, 8), 8))
        return carry

    lax.fori_loop(0, count // 8, group, 0)


def spread_kernel(fez, fhx, fhy, ids, kinds, oez, ohx, ohy, odamp, ogain, rows):
    count = fez.shape[0]
    half = kinds.shape[0] // 2
    lane, block = lane_of(), lane_of() >> 4
    for v in range(3):

        def by_column(h, tiles, at, v=v):
            for f, ref in enumerate((fez, fhx, fhy, ids)):
                for r in range(3):
                    first = 9 * h + 3 * r
                    parts = [ref[tiles, k * LANES : (k + 1) * LANES] for k in range(first, first + 3)]
                    part = choose(parts, third_of(lane, 2 * v)).astype(F32)
                    rows[f, v, r, at] = take(part, 3 * lane + v)

        each_group(count, by_column)
    for u in range(3):

        def by_row(h, tiles, at, u=u):
            for f in range(4):
                for v in range(3):
                    part = choose([rows[f, v, r, at] for r in range(3)], third_of(block, 2 * u))
                    value = take(part, in_block(3 * block + u))
                    if f == 0:
                        oez[3 * u + v, at] = value
                    elif f < 3:
                        (ohx, ohy)[f - 1][3 * u + v, at] = 2.0 * value
                    else:
                        damp = jnp.zeros((8, LANES), F32)
                        gain = jnp.zeros((8, LANES), F32)
                        for m in range(half):
                            hit = value == float(m)
                            damp = jnp.where(hit, kinds[m : m + 1, :], damp)
                            gain = jnp.where(hit, kinds[half + m : half + m + 1, :], gain)
                        odamp[3 * u + v, at] = damp
                        ogain[3 * u + v, at] = gain

        each_group(count, by_row)


def gather_kernel(ez, hx, hy, *refs):
    outs, (flat, rows, cells, sems) = refs[:3], refs[3:]
    count = ez.shape[1] // 2
    lane, block = lane_of(), lane_of() >> 4
    for u in range(3):

        def by_row(h, tiles, at, u=u):
            for f, ref in enumerate((ez, hx, hy)):
                for v in range(3):
                    rows[f, v, u, at] = take(ref[3 * u + v, at], in_block(3 * (block - u)))

        each_group(count, by_row)
    for v in range(3):

        def by_column(h, tiles, at, v=v):
            for f in range(3):
                parts = [rows[f, v, u, at] for u in range(3)]
                for r in range(3):
                    part = choose(parts, third_of(block, 2 * r))
                    cells[f, r, v, at] = take(part, 43 * (lane - v))

        each_group(count, by_column)
    moves = []
    for f in range(3):

        def join(h, tiles, at, f=f):
            for r in range(3):
                parts = [cells[f, r, v, at] for v in range(3)]
                for k in range(3):
                    place = 9 * h + 3 * r + k
                    value = choose(parts, third_of(lane, 2 * k))
                    flat[f, tiles, place * LANES : (place + 1) * LANES] = value

        each_group(count, join)
        moves.append(pltpu.make_async_copy(flat.at[f], outs[f], sems.at[f]))
        moves[-1].start()
    for move in moves:
        move.wait()


def swap_blocks(x):
    block = iota((8, LANES), 1) >> 4
    sub = iota((8, LANES), 0)
    x = jnp.take_along_axis(x, (block + sub) & 7, axis=0)
    x = pltpu.roll(x, 0, 1, stride=TILE, stride_axis=0)
    return jnp.take_along_axis(x, (block - sub) & 7, axis=0)


def rows_of(owners, h, a):
    return slice((h * owners + a) * 8, (h * owners + a + 1) * 8)


def column_of():
    return lax.axis_index("grp") * lax.axis_size("gy") + lax.axis_index("gy")


def ready_kernel(owners, all_cols, *refs):
    windows, boxes, fdamp, fgain, far_src, far_wave, far_rcv = refs[:7]
    mdamp, mgain, mid, box, held, half, drive, row_hit, col_hit = refs[7:16]
    src, wave, rcv, sems = refs[16:]
    moves = copies((far_src, far_wave, far_rcv), (src, wave, rcv), sems)
    me = lax.axis_index("gx")
    column = column_of()
    rows = owners * TILE
    lane = iota((8, LANES), 1)
    sub = iota((8, LANES), 0)
    tile_col = (lane & 15).astype(F32)
    for a in range(owners):
        mine = lane == 8 * me + sub
        low_i, low_j, size_i, size_j = (
            jnp.sum(jnp.where(mine, boxes[a, k : k + 1, :], 0.0), axis=1, keepdims=True)
            for k in range(4)
        )
        high_i, high_j = low_i + size_i, low_j + size_j
        for h in range(2):
            i = (8 * h + (lane >> 4)).astype(F32)
            inside = (i >= low_i) & (i < high_i) & (tile_col >= low_j) & (tile_col < high_j)
            middle = (i > low_i) & (i < high_i - 1) & (tile_col > low_j) & (tile_col < high_j - 1)
            at = rows_of(owners, h, a)
            mid[at] = jnp.where(middle, 1.0, 0.0)
            box[at] = jnp.where(inside, 1.0, 0.0)
            held[at] = swap_blocks(windows[0, a, 8 * h : 8 * h + 8, :])
    for p in range(PLANES):
        mdamp[p] = fdamp[p] * mid[...]
        mgain[p] = fgain[p] * mid[...]
    for move in moves:
        move.wait()
    receivers = rcv[...]
    at_row = lax.div(receivers, all_cols)
    image = lax.rem(iota((3 * rows, LANES), 0), rows)
    image_row = (image >> 4) * rows + me * TILE + (image & 15)
    row_hit[...] = jnp.where(image_row == at_row, 1.0, 0.0).astype(BF16)
    at_col = receivers - at_row * all_cols - column * LANES
    col_hit[...] = jnp.where(iota((LANES, LANES), 0) == at_col, 1.0, 0.0)
    row = iota((WINDOW, WIDE), 0)
    row = jnp.where(row < 20, row, row - WINDOW)
    col = iota((WINDOW, WIDE), 1)
    col = jnp.where(col < LANES + 64, col, col - WIDE)
    all_col = col + column * LANES
    for a in range(owners):
        all_row = row + (a * rows + me * TILE)
        valid = (all_row >= 0) & (all_row < owners * rows) & (all_col >= 0) & (all_col < all_cols)
        cells = jnp.where(valid, all_row * all_cols + all_col, -1)
        half[a] = jnp.where(valid, HCOEF, 0.0)
        for n in range(STEPS):
            total = jnp.zeros((WINDOW, WIDE), F32)
            for k in range(src.shape[0]):
                total = total + jnp.where(cells == src[k], wave[n, k], 0.0)
            drive[n, a] = total


def step_kernel(owners, *refs):
    (windows, from_left, from_right, fez, fhx, fhy, mdamp, mgain, mid, box, first_held, half, drive,
     row_hit, col_hit) = refs[:15]
    oez, ohx, ohy = refs[15:18]
    back = refs[18 : 18 + owners]
    traces = refs[18 + owners]
    ez, hx, hy, damp, gain, held, fresh, picked = refs[19 + owners :]
    column = column_of()
    lane = iota((WINDOW, LANES), 1)
    no_left = column == 0
    no_right = column == lax.axis_size(COLS) - 1
    right = jnp.where(no_right, 0.0, from_right[...])
    left = jnp.where(no_left, 0.0, from_left[...])
    for f, ref in enumerate((ez, hx, hy, damp, gain)):
        for a in range(owners):
            at = GROUP * (f * owners + a)
            after = pltpu.roll(right, LANES - (at + 3), 1)
            before = pltpu.roll(left, (LANES - 3 - at) % LANES, 1)
            side = jnp.where(lane < 3, after, jnp.where(lane >= LANES - 3, before, 0.0))
            ref[a, :, 0:LANES] = windows[f, a]
            ref[a, :, LANES:WIDE] = side
    held[...] = first_held[...]
    for p in range(PLANES):
        oez[p], ohx[p], ohy[p] = fez[p], fhx[p], fhy[p]
    lanes = iota((8, LANES), 1)
    places = [(u, v, h) for u in range(3) for v in range(3) for h in range(2)]

    def substep(m, carry):
        weight = (m + 1).astype(F32) * (1.0 / SUBSTEPS)
        for a in range(owners):
            at = [rows_of(owners, h, a) for h in range(2)]
            cyc = [
                (box[s] - mid[s]) * ((1.0 - weight) * held[s] + weight * fresh[s]) for s in at
            ]
            e = {(u, v, h): oez[3 * u + v, at[h]] for u, v, h in places}
            x, y = {}, {}
            down = {(v, h): pltpu.roll(e[0, v, h], LANES - TILE, 1) for v in range(3) for h in range(2)}
            for v in range(3):
                down[v, 0] = jnp.where(lanes < LANES - TILE, down[v, 0], down[v, 1])
            for u, v, h in places:
                p = 3 * u + v
                beside = e[u, v + 1, h] if v < 2 else pltpu.roll(e[u, 0, h], LANES - 1, 1)
                below = e[u + 1, v, h] if u < 2 else down[v, h]
                x[u, v, h] = ohx[p, at[h]] - (beside - e[u, v, h])
                y[u, v, h] = ohy[p, at[h]] + (below - e[u, v, h])
                ohx[p, at[h]], ohy[p, at[h]] = x[u, v, h], y[u, v, h]
            up = {(v, h): pltpu.roll(y[2, v, h], TILE, 1) for v in range(3) for h in range(2)}
            for v in range(3):
                up[v, 1] = jnp.where(lanes < TILE, up[v, 0], up[v, 1])
            for u, v, h in places:
                p = 3 * u + v
                beside = x[u, v - 1, h] if v > 0 else pltpu.roll(x[u, 2, h], 1, 1)
                above = y[u - 1, v, h] if u > 0 else up[v, h]
                curl = (y[u, v, h] - above) - (x[u, v, h] - beside)
                oez[p, at[h]] = mdamp[p, at[h]] * e[u, v, h] + mgain[p, at[h]] * curl + cyc[h]
        return carry

    def pick(n):
        image = jnp.concatenate([ez[a, 0:TILE, 0:LANES] for a in range(owners)], axis=0)
        mixed = lax.dot_general(
            jnp.concatenate(thirds(image), axis=0),
            row_hit[...],
            (((0,), (0,)), ((), ())),
            preferred_element_type=F32,
        )
        picked[pl.ds(n, 1), :] = jnp.sum(mixed * col_hit[...], axis=0, keepdims=True)

    def step(n, carry):
        pick(lax.rem(n + STEPS - 1, STEPS))
        for a in range(owners):
            e = ez[a]
            x = hx[a] - half[a] * (pltpu.roll(e, WIDE - 1, 1) - e)
            y = hy[a] + half[a] * (pltpu.roll(e, WINDOW - 1, 0) - e)
            curl = (y - pltpu.roll(y, 1, 0)) - (x - pltpu.roll(x, 1, 1))
            hx[a], hy[a] = x, y
            new = damp[a] * e + gain[a] * curl + drive[n, a]
            ez[a] = new
            for h in range(2):
                fresh[rows_of(owners, h, a)] = swap_blocks(new[8 * h : 8 * h + 8, 0:LANES])
        lax.fori_loop(0, SUBSTEPS, substep, 0)
        for a in range(owners):
            for h in range(2):
                s = rows_of(owners, h, a)
                total = oez[0, s]
                for p in range(1, PLANES):
                    total = total + oez[p, s]
                now = jnp.where(mid[s] > 0.0, total * (1.0 / PLANES), fresh[s])
                held[s] = now
                ez[a, 8 * h : 8 * h + 8, 0:LANES] = swap_blocks(now)
        return carry

    lax.fori_loop(0, STEPS, step, 0)
    pick(STEPS - 1)
    for p in range(PLANES):
        ohx[p] = 0.5 * (ohx[p] * box[...])
        ohy[p] = 0.5 * (ohy[p] * box[...])
    for d in range(owners):
        a = block_of(owners, d)
        for f, ref in enumerate((ez, hx, hy)):
            back[d][f * TILE : (f + 1) * TILE, :] = ref[a, 0:TILE, 0:LANES]
    for k in range(traces.shape[0]):
        traces[k] = picked[0:STEPS, :]


def place_kernel(owners, *refs):
    pieces = refs[:owners]
    traces = refs[owners]
    outs = refs[owners + 1 : owners + 4]
    out_trace = refs[owners + 4]
    me = lax.axis_index("gx")
    for d in range(owners):
        here = pl.multiple_of(lax.rem(me + d, owners) * TILE, TILE)
        for f in range(3):
            outs[f][pl.ds(here, TILE), :] = pieces[d][f * TILE : (f + 1) * TILE, :]
    out_trace[...] = jnp.sum(traces[...], axis=0)


def fast_shards(
    coarse_ez, coarse_hx, coarse_hy, coarse_ids, mat_eps, mat_sig,
    fine_ez, fine_hx, fine_hy, fine_ids, boxes, src_cells, src_wave, rcv_cells,
):
    owners = lax.axis_size("gx")
    every = ("grp", "gx", "gy")
    rows, cols = coarse_ez.shape
    all_cols = cols * lax.axis_size(COLS)
    fine_shape = fine_ez.shape
    count = fine_shape[0] * fine_shape[2]
    cells = fine_shape[-1]
    flat = [x.reshape(count, cells) for x in (fine_ez, fine_hx, fine_hy, fine_ids)]
    corners = boxes.reshape(boxes.shape[2:]).T
    block = pltpu.VMEM((rows, cols), F32)
    kinds = mat_eps.shape[0]
    *messages, coarse_kinds, fine_kinds, tile_ez, tile_hx, tile_hy, tile_ids = call(
        functools.partial(pack_kernel, owners),
        tuple(f32(MESSAGE, cols) for _ in range(owners))
        + (kept(2 * kinds, LANES),) * 2
        + (kept(count, cells),) * 3
        + (kept(count, cells, dtype=I32),),
        (coarse_ez, coarse_hx, coarse_hy, coarse_ids, corners, mat_eps, mat_sig, *flat),
        [block] * 3
        + [pltpu.VMEM((rows, cols), I32), pltpu.VMEM(corners.shape, I32)]
        + [pltpu.SMEM((kinds,), F32)] * 2
        + [pltpu.SemaphoreType.DMA((11,))],
        far=range(11),
    )
    received = [messages[0]] + [ring(messages[d], "gx", d) for d in range(1, owners)]
    planes = kept(PLANES, 2 * count, LANES)
    *fields, fdamp, fgain = call(
        spread_kernel,
        (planes,) * 5,
        (tile_ez, tile_hx, tile_hy, tile_ids, fine_kinds),
        [pltpu.VMEM((4, 3, 3, 2 * count, LANES), F32)],
        flops=1 << 31,
    )
    edges, windows, lines = call(
        functools.partial(edges_kernel, owners),
        (f32(WINDOW, LANES), kept(5, owners, WINDOW, LANES), kept(owners, 8, LANES)),
        (*received, coarse_kinds),
        [pltpu.VMEM((owners, MESSAGE, LANES), F32)],
    )
    from_left = ring(edges, COLS, 1)
    from_right = ring(edges, COLS, -1)
    receivers = rcv_cells.shape[0]
    window = (owners, WINDOW, WIDE)
    tiles = kept(2 * count, LANES)
    ready = call(
        functools.partial(ready_kernel, owners, all_cols),
        (planes, planes, tiles, tiles, tiles, kept(*window), kept(STEPS, *window))
        + (kept(3 * owners * TILE, receivers, dtype=BF16), kept(LANES, receivers)),
        (windows, lines, fdamp, fgain, src_cells, src_wave, rcv_cells.reshape(1, receivers)),
        [pltpu.SMEM(src_cells.shape, I32), pltpu.SMEM(src_wave.shape, F32)]
        + [pltpu.VMEM((1, receivers), I32), pltpu.SemaphoreType.DMA((3,))],
        far=(4, 5, 6),
        flops=1 << 30,
    )
    *results, traces = call(
        functools.partial(step_kernel, owners),
        (planes,) * 3
        + tuple(f32(3 * TILE, LANES) for _ in range(owners))
        + (f32(lax.axis_size(every), STEPS, receivers),),
        (windows, from_left, from_right, *fields, *ready),
        [pltpu.VMEM(window, F32)] * 5
        + [pltpu.VMEM(tiles.shape, F32)] * 2
        + [pltpu.VMEM((8, receivers), F32)],
        flops=1 << 30,
    )
    fine, back = results[:3], results[3:]
    traces = lax.all_to_all(traces, every, 0, 0)
    pieces = [back[0]] + [ring(back[d], "gx", owners - d) for d in range(1, owners)]
    finals = call(
        gather_kernel,
        (f32(count, cells),) * 3,
        fine,
        [pltpu.VMEM((3, count, cells), F32)]
        + [pltpu.VMEM((3, 3, 3, 2 * count, LANES), F32)] * 2
        + [pltpu.SemaphoreType.DMA((3,))],
        far_outs=range(3),
        flops=1 << 31,
    )
    ends = call(
        functools.partial(place_kernel, owners),
        (f32(rows, cols),) * 3 + (f32(STEPS, receivers),),
        (*pieces, traces),
    )
    return (*ends[:3], *(x.reshape(fine_shape) for x in finals), ends[3])


def passed_along(value, axis, steps):
    count = lax.axis_size(axis)
    initial, last = (max(0, -steps), min(count, count - steps))
    return lax.ppermute(value, axis, [(source, source + steps) for source in range(initial, last)])


def coefficients(ids, eps_table, sig_table, ratio):
    damp = jnp.zeros(ids.shape, jnp.float32)
    gain = jnp.zeros(ids.shape, jnp.float32)
    for material in range(eps_table.shape[0]):
        loss = sig_table[material] / (eps_table[material] * ratio)
        hit = ids == material
        damp = jnp.where(hit, (1.0 - loss) / (1.0 + loss), damp)
        gain = jnp.where(hit, COURANT / (eps_table[material] * (1.0 + loss)), gain)
    return (damp, gain)


def box_masks(boxes, cells, scale):
    coarse_of = jnp.arange(cells, dtype=jnp.int32) // scale
    low_i = boxes[..., 0:1]
    low_j = boxes[..., 1:2]
    high_i = low_i + boxes[..., 2:3]
    high_j = low_j + boxes[..., 3:4]
    rows_in = (coarse_of >= low_i) & (coarse_of < high_i)
    cols_in = (coarse_of >= low_j) & (coarse_of < high_j)
    rows_mid = (coarse_of > low_i) & (coarse_of < high_i - 1)
    cols_mid = (coarse_of > low_j) & (coarse_of < high_j - 1)
    inbox = rows_in[..., :, None] & cols_in[..., None, :]
    middle = rows_mid[..., :, None] & cols_mid[..., None, :]
    return (inbox, middle)


def flat_masks(boxes):
    width = TILE * 3
    index = jnp.arange(width * width, dtype=jnp.int32)
    coarse_i = index // width // 3
    coarse_j = index % width // 3
    low_i = boxes[:, 0:1]
    low_j = boxes[:, 1:2]
    high_i = low_i + boxes[:, 2:3]
    high_j = low_j + boxes[:, 3:4]
    inbox = (coarse_i >= low_i) & (coarse_i < high_i) & (coarse_j >= low_j) & (coarse_j < high_j)
    middle = (
        (coarse_i > low_i) & (coarse_i < high_i - 1) & (coarse_j > low_j) & (coarse_j < high_j - 1)
    )
    return (inbox, middle)


def spread_table():
    width = TILE * 3
    index = jnp.arange(width * width, dtype=jnp.int32)
    owner = index // width // 3 * TILE + index % width // 3
    return (jnp.arange(TILE * TILE, dtype=jnp.int32)[:, None] == owner[None, :]).astype(jnp.float32)


def to_flat_tiles(field):
    rows, cols = field.shape
    along_x = rows // TILE
    along_y = cols // TILE
    shaped = field.reshape(along_x, TILE, along_y, TILE).transpose(0, 2, 1, 3)
    return shaped.reshape(1, 1, along_x * along_y, TILE * TILE)


def from_tiles(tiles, block_rows, block_cols):
    along_x = block_rows // TILE
    along_y = block_cols // TILE
    shaped = tiles.reshape(along_x, along_y, TILE, TILE).transpose(0, 2, 1, 3)
    return shaped.reshape(block_rows, block_cols)


def pad_last(array, before, after):
    widths = [(0, 0)] * (array.ndim - 1) + [(before, after)]
    return jnp.pad(array, widths)


def fine_substep(fine_ez, fine_hx, fine_hy, damp, gain, inbox, middle, border, cycle_value):
    width = TILE * 3
    column = jnp.arange(width * width, dtype=jnp.int32) % width
    ez_next_col = jnp.where(column < width - 1, pad_last(fine_ez[..., 1:], 0, 1), 0.0)
    ez_next_row = pad_last(fine_ez[..., width:], 0, width)
    fine_hx = jnp.where(inbox, fine_hx - HCOEF * (ez_next_col - fine_ez), 0.0)
    fine_hy = jnp.where(inbox, fine_hy + HCOEF * (ez_next_row - fine_ez), 0.0)
    hy_prev = pad_last(fine_hy[..., :-width], width, 0)
    hx_prev = jnp.where(column > 0, pad_last(fine_hx[..., :-1], 1, 0), 0.0)
    curl = fine_hy - hy_prev - (fine_hx - hx_prev)
    inner = damp * fine_ez + gain * curl
    fine_ez = jnp.where(middle, inner, jnp.where(border, cycle_value, 0.0))
    return (fine_ez, fine_hx, fine_hy)


def fine_round(
    fine_ez, fine_hx, fine_hy, damp, gain, inbox, middle, border, old_tiles, new_tiles, spread
):
    for sub in range(1, 4):
        weight = sub / 3.0
        mixed = (1.0 - weight) * old_tiles + weight * new_tiles
        cycle_value = jnp.dot(
            mixed, spread, precision=lax.Precision.HIGHEST, preferred_element_type=jnp.float32
        )
        fine_ez, fine_hx, fine_hy = fine_substep(
            fine_ez, fine_hx, fine_hy, damp, gain, inbox, middle, border, cycle_value
        )
    return (fine_ez, fine_hx, fine_hy)


def coarse_magnetic(ez, hx, hy):
    below = passed_along(ez[:1, :], "gx", -1)
    beside = passed_along(ez[:, :1], ("grp", "gy"), -1)
    ez_next_row = jnp.concatenate([ez[1:, :], below], axis=0)
    ez_next_col = jnp.concatenate([ez[:, 1:], beside], axis=1)
    hx = hx - HCOEF * (ez_next_col - ez)
    hy = hy + HCOEF * (ez_next_row - ez)
    above = passed_along(hy[-1:, :], "gx", 1)
    before = passed_along(hx[:, -1:], ("grp", "gy"), 1)
    hy_prev = jnp.concatenate([above, hy[:-1, :]], axis=0)
    hx_prev = jnp.concatenate([before, hx[:, :-1]], axis=1)
    curl = hy - hy_prev - (hx - hx_prev)
    return (hx, hy, curl)


def shards(
    coarse_ez,
    coarse_hx,
    coarse_hy,
    coarse_ids,
    mat_eps,
    mat_sig,
    fine_ez,
    fine_hx,
    fine_hy,
    fine_ids,
    boxes,
    src_cells,
    src_wave,
    rcv_cells,
):
    rows, cols = coarse_ez.shape
    fine_shape = fine_ez.shape
    flat_cells = fine_shape[-1]
    means_shape = fine_shape[:-1] + (TILE * TILE,)
    row_start = lax.axis_index("gx") * rows
    col_start = lax.axis_index(("grp", "gy")) * cols
    all_cols = cols * lax.axis_size(("grp", "gy"))
    spread = spread_table()
    damp, gain = coefficients(coarse_ids, mat_eps, mat_sig, 1.0)
    fine_damp, fine_gain = coefficients(fine_ids.reshape(-1, flat_cells), mat_eps, mat_sig, 3.0)
    owned_boxes = lax.all_to_all(boxes, "gx", split_axis=2, concat_axis=0, tiled=True).reshape(
        -1, 4
    )
    inbox, middle = flat_masks(owned_boxes)
    border = inbox & jnp.logical_not(middle)
    coarse_mid = from_tiles(box_masks(boxes, TILE, 1)[1], rows, cols)
    src_rows = (
        jnp.arange(rows, dtype=jnp.int32)[None, :] == (src_cells // all_cols - row_start)[:, None]
    ).astype(jnp.float32)
    src_cols = (
        jnp.arange(cols, dtype=jnp.int32)[None, :] == (src_cells % all_cols - col_start)[:, None]
    ).astype(jnp.float32)
    rcv_rows = (
        jnp.arange(rows, dtype=jnp.int32)[None, :] == (rcv_cells // all_cols - row_start)[:, None]
    ).astype(jnp.float32)
    rcv_cols = (
        jnp.arange(cols, dtype=jnp.int32)[None, :] == (rcv_cells % all_cols - col_start)[:, None]
    ).astype(jnp.float32)
    ez, hx, hy = (coarse_ez, coarse_hx, coarse_hy)
    field_ez = fine_ez.reshape(-1, flat_cells)
    field_hx = fine_hx.reshape(-1, flat_cells)
    field_hy = fine_hy.reshape(-1, flat_cells)
    held = lax.all_to_all(to_flat_tiles(ez), "gx", split_axis=2, concat_axis=0, tiled=True).reshape(
        -1, TILE * TILE
    )
    samples = []
    for step in range(STEPS):
        hx, hy, curl = coarse_magnetic(ez, hx, hy)
        weighted = src_rows * src_wave[step][:, None]
        drive = jnp.dot(
            weighted.T,
            src_cols,
            precision=lax.Precision.HIGHEST,
            preferred_element_type=jnp.float32,
        )
        new = damp * ez + gain * curl + drive
        old_tiles = held
        new_tiles = lax.all_to_all(
            to_flat_tiles(new), "gx", split_axis=2, concat_axis=0, tiled=True
        ).reshape(-1, TILE * TILE)
        held = new_tiles
        field_ez, field_hx, field_hy = fine_round(
            field_ez,
            field_hx,
            field_hy,
            fine_damp,
            fine_gain,
            inbox,
            middle,
            border,
            old_tiles,
            new_tiles,
            spread,
        )
        sums = lax.dot_general(
            field_ez,
            spread,
            (((1,), (1,)), ((), ())),
            precision=lax.Precision.HIGHEST,
            preferred_element_type=jnp.float32,
        )
        means = (sums / 9.0).reshape(means_shape)
        back = lax.all_to_all(means, "gx", split_axis=0, concat_axis=2, tiled=True)
        ez = jnp.where(coarse_mid, from_tiles(back, rows, cols), new)
        picked = jnp.dot(
            rcv_rows, ez, precision=lax.Precision.HIGHEST, preferred_element_type=jnp.float32
        )
        samples.append(jnp.sum(picked * rcv_cols, axis=1))
    traces = lax.psum(jnp.stack(samples), ("grp", "gx", "gy"))
    return (
        ez,
        hx,
        hy,
        field_ez.reshape(fine_shape),
        field_hx.reshape(fine_shape),
        field_hy.reshape(fine_shape),
        traces,
    )


def solution(mesh):
    placed = (
        P("gx", ("grp", "gy")),
        P("gx", ("grp", "gy")),
        P("gx", ("grp", "gy")),
        P("gx", ("grp", "gy")),
        P(),
        P(),
        P(None, ("grp", "gy"), "gx", None),
        P(None, ("grp", "gy"), "gx", None),
        P(None, ("grp", "gy"), "gx", None),
        P(None, ("grp", "gy"), "gx", None),
        P("gx", ("grp", "gy"), None, None),
        P(),
        P(),
        P(),
    )
    def body(*args):
        rows, cols = args[0].shape
        owners = lax.axis_size("gx")
        strips = cols == LANES and args[6].shape[2] * TILE == cols and rows == owners * TILE
        if strips and 5 * GROUP * owners <= LANES and args[13].shape[0] == LANES:
            return fast_shards(*args)
        return shards(*args)

    return jax.shard_map(
        body,
        mesh=mesh,
        in_specs=placed,
        out_specs=(
            P("gx", ("grp", "gy")),
            P("gx", ("grp", "gy")),
            P("gx", ("grp", "gy")),
            P(None, ("grp", "gy"), "gx", None),
            P(None, ("grp", "gy"), "gx", None),
            P(None, ("grp", "gy"), "gx", None),
            P(),
        ),
        check_vma=False,
    )
```

```python
import functools

import jax
import jax.numpy as jnp
from jax import lax
from jax.experimental import pallas as pl
from jax.experimental.pallas import tpu as pltpu
from jax.sharding import PartitionSpec as P

TILE = 16
STEPS = 3
SUBSTEPS = 3
LANES = 128
FIELDS = 4
WINDOW = 24
HALO = FIELDS * TILE
MESSAGE = HALO + 24
PLANES = 9
WIDE = 2 * LANES
GROUP = 6

COURANT = 0.5
HCOEF = 0.5
F32 = jnp.float32
BF16 = jnp.bfloat16
I32 = jnp.int32
COLS = ("grp", "gy")


def iota(shape, axis):
    return lax.broadcasted_iota(I32, shape, axis)


def f32(*shape):
    return jax.ShapeDtypeStruct(shape, F32)


def kept(*shape, dtype=F32):
    return pltpu.VMEM(shape, dtype)


def call(kernel, outs, args, scratch=(), far=(), near=(), far_outs=(), flops=1 << 20):
    vmem, hbm = (pl.BlockSpec(memory_space=m) for m in (pltpu.VMEM, pltpu.HBM))
    args = [
        pltpu.with_memory_space_constraint(x, pltpu.HBM)
        if k in far
        else pltpu.with_memory_space_constraint(x, pltpu.VMEM)
        if k in near
        else x
        for k, x in enumerate(args)
    ]
    return pl.pallas_call(
        kernel,
        out_shape=outs,
        in_specs=[hbm if k in far else vmem for k in range(len(args))],
        out_specs=tuple(hbm if k in far_outs else vmem for k in range(len(outs))),
        scratch_shapes=list(scratch),
        compiler_params=pltpu.CompilerParams(vmem_limit_bytes=16 * 1024 * 1024),
        cost_estimate=pl.CostEstimate(flops=flops, bytes_accessed=1 << 20, transcendentals=0),
    )(*args)


def copies(sources, targets, sems):
    moves = [
        pltpu.make_async_copy(source, target, sems.at[k])
        for k, (source, target) in enumerate(zip(sources, targets))
    ]
    for move in moves:
        move.start()
    return moves


def ring(value, axis, steps):
    count = lax.axis_size(axis)
    return lax.ppermute(value, axis, [(k, (k + steps) % count) for k in range(count)])


def pack_kernel(owners, *refs):
    sources, outs = refs[:5], refs[5 : 5 + owners]
    held, sems = refs[5 + owners : 10 + owners], refs[10 + owners]
    for move in copies(sources, held, sems):
        move.wait()
    ez, hx, hy, ids, boxes = held
    me = lax.axis_index("gx")
    tiles = ez.shape[0] // 8
    count = boxes.shape[1]
    sub = iota((8, LANES), 0)
    lines = jnp.concatenate([boxes[...].astype(F32), jnp.zeros((4, LANES - count), F32)], axis=1)
    low, high, left, top = (jnp.broadcast_to(lines[k : k + 1, :], (8, LANES)) for k in range(4))
    for d in range(owners):
        g = lax.rem(me + d, owners)
        here = pl.multiple_of(g * TILE, TILE)
        after = pl.multiple_of(lax.rem(2 * g + 2, tiles) * 8, 8)
        before = pl.multiple_of(lax.rem(2 * g + tiles - 1, tiles) * 8, 8)
        edges = []
        for f, ref in enumerate((ez, hx, hy, ids)):
            outs[d][f * TILE : (f + 1) * TILE, :] = ref[pl.ds(here, TILE), :].astype(F32)
            edge = jnp.where(sub < 4, ref[pl.ds(after, 8), :], ref[pl.ds(before, 8), :])
            edges.append(edge.astype(F32))
        around_ez, around_hx, around_hy, around_ids = edges
        outs[d][HALO : HALO + 8, :] = jnp.where(sub == 3, low, jnp.where(sub == 4, high, around_ez))
        inner = jnp.where(sub < 4, pltpu.roll(around_ids, 2, 0), pltpu.roll(around_ids, 6, 0))
        outs[d][HALO + 8 : HALO + 16, :] = jnp.where((sub >= 2) & (sub < 6), inner, around_hx)
        outs[d][HALO + 16 : HALO + 24, :] = jnp.where(
            sub == 2, left, jnp.where(sub == 3, top, around_hy)
        )


def block_of(owners, d):
    return lax.rem(lax.axis_index("gx") + owners - d, owners)


def edges_kernel(owners, *refs):
    received, table = refs[:owners], refs[owners]
    out, windows, boxes, store = refs[owners + 1 :]
    me = lax.axis_index("gx")
    sub = iota((8, LANES), 0)
    for d in range(owners):
        store[block_of(owners, d)] = received[d][...]
    around = [
        [store[a, HALO + 8 * k : HALO + 8 * k + 8, :] for a in range(owners)] for k in range(3)
    ]
    row = iota((WINDOW, LANES), 0)
    row = jnp.where(row < 20, row, row - WINDOW)
    lane = iota((WINDOW, LANES), 1)
    total = jnp.zeros((WINDOW, LANES), F32)
    for a in range(owners):
        for k, at in enumerate((3, 4, 18, 19)):
            boxes[a, k : k + 1, :] = store[a, HALO + at : HALO + at + 1, :]
        tiles = []
        for tile in around:
            after = jnp.where(me == owners - 1, tile[min(a + 1, owners - 1)], tile[a])
            before = jnp.where(me == 0, tile[max(a - 1, 0)], tile[a])
            tiles.append(jnp.where(sub < 4, after, before))
        inner = jnp.where(sub < 4, pltpu.roll(tiles[1], 6, 0), pltpu.roll(tiles[1], 2, 0))
        fields = [
            jnp.concatenate([store[a, f * TILE : (f + 1) * TILE, :], tile], axis=0)
            for f, tile in enumerate((*tiles, inner))
        ]
        all_row = row + (a * owners * TILE + me * TILE)
        valid = (all_row >= 0) & (all_row < owners * owners * TILE)
        damp = jnp.zeros((WINDOW, LANES), F32)
        gain = jnp.zeros((WINDOW, LANES), F32)
        kinds = table.shape[0] // 2
        for m in range(kinds):
            hit = fields[3] == float(m)
            damp = jnp.where(hit, table[m : m + 1, :], damp)
            gain = jnp.where(hit, table[kinds + m : kinds + m + 1, :], gain)
        for f, value in enumerate((*fields[:3], damp, gain)):
            value = jnp.where(valid, value, 0.0)
            windows[f, a] = value
            at = GROUP * (f * owners + a)
            total = jnp.where((lane >= at) & (lane < at + GROUP), pltpu.roll(value, at + 3, 1), total)
    out[...] = total


def lane_of():
    return iota((8, LANES), 1)


def third_of(x, start):
    return lax.rem(x + start, 3)


def choose(parts, which):
    return jnp.where(which == 0, parts[0], jnp.where(which == 1, parts[1], parts[2]))


def take(x, lanes):
    return jnp.take_along_axis(x, lanes & (LANES - 1), axis=1)


def in_block(block):
    return ((block & 7) << 4) | (lane_of() & 15)


def halves(x):
    high = x.astype(BF16)
    return high, (x - high.astype(F32)).astype(BF16)


def thirds(x):
    high = x.astype(BF16)
    rest = x - high.astype(F32)
    return high, *halves(rest)


def lists(eps, sig, ratio):
    ones = jnp.ones((1, LANES), F32)
    both = []
    for m in range(eps.shape[0]):
        e, s = ones * eps[m], ones * sig[m]
        loss = s / (e * ratio)
        both.append(((1.0 - loss) / (1.0 + loss), COURANT / (e * (1.0 + loss))))
    return both


def turn(x, first, last):
    block = lane_of() >> 4
    sub = iota((8, LANES), 0)
    x = jnp.take_along_axis(x, first(sub, block) & 7, axis=0)
    x = pltpu.roll(x, 0, 1, stride=TILE, stride_axis=0)
    return jnp.take_along_axis(x, last(sub, block) & 7, axis=0)


def each_half(owners):
    for a in range(owners):
        for h in range(2):
            yield a, h, slice(8 * a, 8 * a + 8), slice(TILE * a + 8 * h, TILE * a + 8 * h + 8)


def spread_kernel(*refs):
    sources, (oez, ohx, ohy, odamp, ogain, coarse_kinds) = refs[:6], refs[6:12]
    held, (kinds, rows, sems) = refs[12:18], refs[18:]
    fez, fhx, fhy, ids, eps, sig = held
    moves = copies(sources, held, sems)
    half = eps.shape[0]
    for move in moves[4:]:
        move.wait()
    for ref, ratio, scale in ((coarse_kinds, 1.0, 1.0), (kinds, 3.0, 0.5)):
        for m, (damp, gain) in enumerate(lists(eps, sig, ratio)):
            ref[m : m + 1, :] = damp
            ref[half + m : half + m + 1, :] = scale * gain
    for move in moves[:4]:
        move.wait()
    owners = fez.shape[0] // 8
    lane, block = lane_of(), lane_of() >> 4
    for v in range(3):
        for a, h, tiles, at in each_half(owners):
            for f, ref in enumerate((fez, fhx, fhy, ids)):
                for r in range(3):
                    first = 9 * h + 3 * r
                    parts = [ref[tiles, k * LANES : (k + 1) * LANES] for k in range(first, first + 3)]
                    part = choose(parts, third_of(lane, 2 * v)).astype(F32)
                    rows[f, v, r, at] = take(part, 3 * lane + v)
    for u in range(3):
        for a, h, tiles, at in each_half(owners):
            for f in (3, 0, 1, 2):
                for v in range(3):
                    part = choose([rows[f, v, r, at] for r in range(3)], third_of(block, 2 * u))
                    value = turn(part, lambda r, b: r + b, lambda i, c: c - 3 * i - u)
                    if f == 0:
                        oez[3 * u + v, at] = value
                    elif f < 3:
                        (ohx, ohy)[f - 1][3 * u + v, at] = 2.0 * value
                    else:
                        damp = jnp.zeros((8, LANES), F32)
                        gain = jnp.zeros((8, LANES), F32)
                        for m in range(half):
                            hit = value == float(m)
                            damp = jnp.where(hit, kinds[m : m + 1, :], damp)
                            gain = jnp.where(hit, kinds[half + m : half + m + 1, :], gain)
                        odamp[3 * u + v, at] = damp
                        ogain[3 * u + v, at] = gain


def gather_kernel(ez, hx, hy, *refs):
    outs, (flat, rows, cells, sems) = refs[:3], refs[3:]
    owners = ez.shape[1] // TILE
    lane, block = lane_of(), lane_of() >> 4
    for u in range(3):
        for a, h, tiles, at in each_half(owners):
            for f, ref in enumerate((ez, hx, hy)):
                for v in range(3):
                    rows[f, v, u, at] = turn(
                        ref[3 * u + v, at], lambda r, b: 3 * (b + r - u), lambda c, b: b - c
                    )
    for v in range(3):
        for a, h, tiles, at in each_half(owners):
            for f in range(3):
                parts = [rows[f, v, u, at] for u in range(3)]
                for r in range(3):
                    part = choose(parts, third_of(block, 2 * r))
                    cells[f, r, v, at] = take(part, 43 * (lane - v))
    moves = []
    for f in range(3):
        for a, h, tiles, at in each_half(owners):
            for r in range(3):
                parts = [cells[f, r, v, at] for v in range(3)]
                for k in range(3):
                    place = 9 * h + 3 * r + k
                    value = choose(parts, third_of(lane, 2 * k))
                    flat[f, tiles, place * LANES : (place + 1) * LANES] = value
        moves.append(pltpu.make_async_copy(flat.at[f], outs[f], sems.at[f]))
        moves[-1].start()
    for move in moves:
        move.wait()


def column_of():
    return lax.axis_index("grp") * lax.axis_size("gy") + lax.axis_index("gy")


def ready_kernel(owners, all_cols, *refs):
    windows, boxes, fdamp, fgain, far_src, far_wave, far_rcv = refs[:7]
    mdamp, mgain, mid, box, half, drive, row_hit, col_hit = refs[7:15]
    src, wave, rcv, sems = refs[15:]
    moves = copies((far_src, far_wave, far_rcv), (src, wave, rcv), sems)
    me = lax.axis_index("gx")
    column = column_of()
    rows = owners * TILE
    lane = lane_of()
    tile_col = (lane & 15).astype(F32)
    for a in range(owners):
        low_i, low_j, size_i, size_j = (
            take(jnp.broadcast_to(boxes[a, k : k + 1, :], (8, LANES)), 8 * me + (lane >> 4))
            for k in range(4)
        )
        high_i, high_j = low_i + size_i, low_j + size_j
        for h in range(2):
            i = (8 * h + iota((8, LANES), 0)).astype(F32)
            inside = (i >= low_i) & (i < high_i) & (tile_col >= low_j) & (tile_col < high_j)
            middle = (i > low_i) & (i < high_i - 1) & (tile_col > low_j) & (tile_col < high_j - 1)
            at = slice(TILE * a + 8 * h, TILE * a + 8 * h + 8)
            mid[at] = jnp.where(middle, 1.0, 0.0)
            box[at] = jnp.where(inside, 1.0, 0.0)
    for p in range(PLANES):
        mdamp[p] = fdamp[p] * mid[...]
        mgain[p] = fgain[p] * mid[...]
    for move in moves:
        move.wait()
    receivers = rcv[...]
    at_row = lax.div(receivers, all_cols)
    image = lax.rem(iota((3 * rows, LANES), 0), rows)
    image_row = (image >> 4) * rows + me * TILE + (image & 15)
    row_hit[...] = jnp.where(image_row == at_row, 1.0, 0.0).astype(BF16)
    at_col = receivers - at_row * all_cols - column * LANES
    col_hit[...] = jnp.where(iota((LANES, LANES), 0) == at_col, 1.0, 0.0)
    row = iota((WINDOW, WIDE), 0)
    row = jnp.where(row < 20, row, row - WINDOW)
    col = iota((WINDOW, WIDE), 1)
    col = jnp.where(col < LANES + 64, col, col - WIDE)
    all_col = col + column * LANES
    for a in range(owners):
        all_row = row + (a * rows + me * TILE)
        valid = (all_row >= 0) & (all_row < owners * rows) & (all_col >= 0) & (all_col < all_cols)
        cells = jnp.where(valid, all_row * all_cols + all_col, -1)
        half[a] = jnp.where(valid, HCOEF, 0.0)
        half[owners + a] = jnp.where(valid & (all_col > 0), HCOEF, 0.0)
        for n in range(STEPS):
            total = jnp.zeros((WINDOW, WIDE), F32)
            for k in range(src.shape[0]):
                total = total + jnp.where(cells == src[k], wave[n, k], 0.0)
            drive[n, a] = total


def step_kernel(owners, *refs):
    (windows, from_left, from_right, fez, fhx, fhy, mdamp, mgain, mid, box, half, drive,
     row_hit, col_hit) = refs[:14]
    oez, ohx, ohy = refs[14:17]
    back = refs[17 : 17 + owners]
    traces = refs[17 + owners]
    ez, hx, hy, behind, damp, gain, held, beside, picked = refs[18 + owners :]
    column = column_of()
    place = lax.rem(iota((WINDOW, LANES), 1), GROUP)
    right = jnp.where(column == lax.axis_size(COLS) - 1, 0.0, from_right[...])
    left = jnp.where(column == 0, 0.0, from_left[...])
    sides = jnp.where(place < 3, left, right)
    for f, ref in enumerate((ez, hx, hy, damp, gain)):
        for a in range(owners):
            at = GROUP * (f * owners + a)
            ref[a, :, 0:LANES] = windows[f, a]
            ref[a, :, LANES:WIDE] = pltpu.roll(sides, (LANES - 3 - at) % LANES, 1)
    for p in range(PLANES):
        oez[p], ohx[p], ohy[p] = fez[p], fhx[p], fhy[p]
    for a in range(owners):
        behind[a] = pltpu.roll(hx[a], 1, 1)
    for u in range(3):
        for k in range(2 * owners):
            at = slice(8 * k, 8 * k + 8)
            beside[u, at] = pltpu.roll(fhx[3 * u + 2, at], 1, 1)
    sub = iota((8, LANES), 0)
    places = [(u, v, h) for u in range(3) for v in range(3) for h in range(2)]

    def substep(m, carry):
        weight = (m + 1).astype(F32) * (1.0 / SUBSTEPS)
        for a in range(owners):
            at = [slice(TILE * a + 8 * h, TILE * a + 8 * h + 8) for h in range(2)]
            e = {(u, v, h): oez[3 * u + v, at[h]] for u, v, h in places}
            ahead = {(u, h): pltpu.roll(e[u, 0, h], LANES - 1, 1) for u in range(3) for h in range(2)}
            back_e = {(u, h): pltpu.roll(e[u, 2, h], 1, 1) for u in range(3) for h in range(2)}
            down = {(v, h): pltpu.roll(e[0, v, h], 7, 0) for v in range(3) for h in range(2)}
            y = {}
            for u, v, h in places:
                p = 3 * u + v
                if u < 2:
                    below = e[u + 1, v, h]
                elif h == 0:
                    below = jnp.where(sub < 7, down[v, 0], down[v, 1])
                else:
                    below = down[v, 1]
                y[u, v, h] = ohy[p, at[h]] + (below - e[u, v, h])
                ohy[p, at[h]] = y[u, v, h]
            up = {(v, h): pltpu.roll(y[2, v, h], 1, 0) for v in range(3) for h in range(2)}
            for v in range(3):
                up[v, 1] = jnp.where(sub < 1, up[v, 0], up[v, 1])
            for h in range(2):
                now = ez[a, 8 * h : 8 * h + 8, 0:LANES]
                cyc = (box[at[h]] - mid[at[h]]) * ((1.0 - weight) * held[at[h]] + weight * now)
                for u in range(3):
                    before = beside[u, at[h]] - (e[u, 0, h] - back_e[u, h])
                    beside[u, at[h]] = before
                    for v in range(3):
                        p = 3 * u + v
                        after = e[u, v + 1, h] if v < 2 else ahead[u, h]
                        x = ohx[p, at[h]] - (after - e[u, v, h])
                        ohx[p, at[h]] = x
                        above = y[u - 1, v, h] if u > 0 else up[v, h]
                        curl = (y[u, v, h] - above) - (x - before)
                        inner = mdamp[p, at[h]] * e[u, v, h] + mgain[p, at[h]] * curl
                        oez[p, at[h]] = inner + cyc
                        before = x
        return carry

    def pick(n):
        image = jnp.concatenate([ez[a, 0:TILE, 0:LANES] for a in range(owners)], axis=0)
        mixed = lax.dot_general(
            jnp.concatenate(thirds(image), axis=0),
            row_hit[...],
            (((0,), (0,)), ((), ())),
            preferred_element_type=F32,
        )
        picked[pl.ds(n, 1), :] = jnp.sum(mixed * col_hit[...], axis=0, keepdims=True)

    def step(n, carry):
        pick(lax.rem(n + STEPS - 1, STEPS))
        for a in range(owners):
            e = ez[a]
            held[TILE * a : TILE * a + TILE] = e[0:TILE, 0:LANES]
            scale = half[a]
            x = hx[a] - scale * (pltpu.roll(e, WIDE - 1, 1) - e)
            before = behind[a] - half[owners + a] * (e - pltpu.roll(e, 1, 1))
            y = hy[a] + scale * (pltpu.roll(e, WINDOW - 1, 0) - e)
            hx[a], hy[a], behind[a] = x, y, before
            curl = (y - pltpu.roll(y, 1, 0)) - (x - before)
            ez[a] = damp[a] * e + gain[a] * curl + drive[n, a]
        lax.fori_loop(0, SUBSTEPS, substep, 0)
        for a in range(owners):
            for h in range(2):
                at = slice(TILE * a + 8 * h, TILE * a + 8 * h + 8)
                total = oez[0, at]
                for p in range(1, PLANES):
                    total = total + oez[p, at]
                here = (a, slice(8 * h, 8 * h + 8), slice(0, LANES))
                ez[here] = jnp.where(mid[at] > 0.0, total * (1.0 / PLANES), ez[here])
        return carry

    picked[...] = jnp.zeros(picked.shape, F32)
    lax.fori_loop(0, STEPS, step, 0)
    pick(STEPS - 1)
    for p in range(PLANES):
        ohx[p] = 0.5 * (ohx[p] * box[...])
        ohy[p] = 0.5 * (ohy[p] * box[...])
    for d in range(owners):
        a = block_of(owners, d)
        for f, ref in enumerate((ez, hx, hy)):
            back[d][f * TILE : (f + 1) * TILE, :] = ref[a, 0:TILE, 0:LANES]
    for k in range(traces.shape[0]):
        traces[k] = picked[0:STEPS, :]


def place_kernel(owners, *refs):
    pieces = refs[:owners]
    traces = refs[owners]
    outs = refs[owners + 1 : owners + 4]
    out_trace = refs[owners + 4]
    me = lax.axis_index("gx")
    for d in range(owners):
        here = pl.multiple_of(lax.rem(me + d, owners) * TILE, TILE)
        for f in range(3):
            outs[f][pl.ds(here, TILE), :] = pieces[d][f * TILE : (f + 1) * TILE, :]
    out_trace[...] = jnp.sum(traces[...], axis=0)


def fast_shards(
    coarse_ez, coarse_hx, coarse_hy, coarse_ids, mat_eps, mat_sig,
    fine_ez, fine_hx, fine_hy, fine_ids, boxes, src_cells, src_wave, rcv_cells,
):
    owners = lax.axis_size("gx")
    every = ("grp", "gx", "gy")
    rows, cols = coarse_ez.shape
    all_cols = cols * lax.axis_size(COLS)
    fine_shape = fine_ez.shape
    count = fine_shape[0] * fine_shape[2]
    cells = fine_shape[-1]
    flat = [x.reshape(count, cells) for x in (fine_ez, fine_hx, fine_hy, fine_ids)]
    corners = boxes.reshape(boxes.shape[2:]).T
    block = pltpu.VMEM((rows, cols), F32)
    messages = call(
        functools.partial(pack_kernel, owners),
        tuple(f32(MESSAGE, cols) for _ in range(owners)),
        (coarse_ez, coarse_hx, coarse_hy, coarse_ids, corners),
        [block] * 3
        + [pltpu.VMEM((rows, cols), I32), pltpu.VMEM(corners.shape, I32)]
        + [pltpu.SemaphoreType.DMA((5,))],
        far=range(5),
    )
    received = [messages[0]] + [ring(messages[d], "gx", d) for d in range(1, owners)]
    planes = kept(PLANES, 2 * count, LANES)
    kinds = mat_eps.shape[0]
    *fields, fdamp, fgain, coarse_kinds = call(
        spread_kernel,
        (planes,) * 5 + (kept(2 * kinds, LANES),),
        (*flat, mat_eps, mat_sig),
        [pltpu.VMEM((count, cells), F32)] * 3
        + [pltpu.VMEM((count, cells), I32)]
        + [pltpu.SMEM((kinds,), F32)] * 2
        + [pltpu.VMEM((2 * kinds, LANES), F32), pltpu.VMEM((4, 3, 3, 2 * count, LANES), F32)]
        + [pltpu.SemaphoreType.DMA((6,))],
        far=range(6),
        flops=1 << 31,
    )
    edges, windows, lines = call(
        functools.partial(edges_kernel, owners),
        (f32(WINDOW, LANES), kept(5, owners, WINDOW, LANES), kept(owners, 8, LANES)),
        (*received, coarse_kinds),
        [pltpu.VMEM((owners, MESSAGE, LANES), F32)],
    )
    from_left = ring(edges, COLS, 1)
    from_right = ring(edges, COLS, -1)
    receivers = rcv_cells.shape[0]
    window = (owners, WINDOW, WIDE)
    tiles = kept(2 * count, LANES)
    ready = call(
        functools.partial(ready_kernel, owners, all_cols),
        (planes, planes, tiles, tiles, kept(2 * owners, *window[1:]), kept(STEPS, *window))
        + (kept(3 * owners * TILE, receivers, dtype=BF16), kept(LANES, receivers)),
        (windows, lines, fdamp, fgain, src_cells, src_wave, rcv_cells.reshape(1, receivers)),
        [pltpu.SMEM(src_cells.shape, I32), pltpu.SMEM(src_wave.shape, F32)]
        + [pltpu.VMEM((1, receivers), I32), pltpu.SemaphoreType.DMA((3,))],
        far=(4, 5, 6),
        flops=1 << 30,
    )
    *results, traces = call(
        functools.partial(step_kernel, owners),
        (planes,) * 3
        + tuple(f32(3 * TILE, LANES) for _ in range(owners))
        + (kept(lax.axis_size(every), STEPS, receivers),),
        (windows, from_left, from_right, *fields, *ready),
        [pltpu.VMEM(window, F32)] * 6
        + [pltpu.VMEM(tiles.shape, F32), pltpu.VMEM((3, *tiles.shape), F32)]
        + [pltpu.VMEM((8, receivers), F32)],
        flops=1 << 30,
    )
    fine, back = results[:3], results[3:]
    traces = lax.all_to_all(traces, every, 0, 0)
    pieces = [back[0]] + [ring(back[d], "gx", owners - d) for d in range(1, owners)]
    finals = call(
        gather_kernel,
        (f32(count, cells),) * 3,
        fine,
        [pltpu.VMEM((3, count, cells), F32)]
        + [pltpu.VMEM((3, 3, 3, 2 * count, LANES), F32)] * 2
        + [pltpu.SemaphoreType.DMA((3,))],
        far_outs=range(3),
        flops=1 << 31,
    )
    ends = call(
        functools.partial(place_kernel, owners),
        (f32(rows, cols),) * 3 + (f32(STEPS, receivers),),
        (*pieces, traces),
    )
    return (*ends[:3], *(x.reshape(fine_shape) for x in finals), ends[3])


def passed_along(value, axis, steps):
    count = lax.axis_size(axis)
    initial, last = (max(0, -steps), min(count, count - steps))
    return lax.ppermute(value, axis, [(source, source + steps) for source in range(initial, last)])


def coefficients(ids, eps_table, sig_table, ratio):
    damp = jnp.zeros(ids.shape, jnp.float32)
    gain = jnp.zeros(ids.shape, jnp.float32)
    for material in range(eps_table.shape[0]):
        loss = sig_table[material] / (eps_table[material] * ratio)
        hit = ids == material
        damp = jnp.where(hit, (1.0 - loss) / (1.0 + loss), damp)
        gain = jnp.where(hit, COURANT / (eps_table[material] * (1.0 + loss)), gain)
    return (damp, gain)


def box_masks(boxes, cells, scale):
    coarse_of = jnp.arange(cells, dtype=jnp.int32) // scale
    low_i = boxes[..., 0:1]
    low_j = boxes[..., 1:2]
    high_i = low_i + boxes[..., 2:3]
    high_j = low_j + boxes[..., 3:4]
    rows_in = (coarse_of >= low_i) & (coarse_of < high_i)
    cols_in = (coarse_of >= low_j) & (coarse_of < high_j)
    rows_mid = (coarse_of > low_i) & (coarse_of < high_i - 1)
    cols_mid = (coarse_of > low_j) & (coarse_of < high_j - 1)
    inbox = rows_in[..., :, None] & cols_in[..., None, :]
    middle = rows_mid[..., :, None] & cols_mid[..., None, :]
    return (inbox, middle)


def flat_masks(boxes):
    width = TILE * 3
    index = jnp.arange(width * width, dtype=jnp.int32)
    coarse_i = index // width // 3
    coarse_j = index % width // 3
    low_i = boxes[:, 0:1]
    low_j = boxes[:, 1:2]
    high_i = low_i + boxes[:, 2:3]
    high_j = low_j + boxes[:, 3:4]
    inbox = (coarse_i >= low_i) & (coarse_i < high_i) & (coarse_j >= low_j) & (coarse_j < high_j)
    middle = (
        (coarse_i > low_i) & (coarse_i < high_i - 1) & (coarse_j > low_j) & (coarse_j < high_j - 1)
    )
    return (inbox, middle)


def spread_table():
    width = TILE * 3
    index = jnp.arange(width * width, dtype=jnp.int32)
    owner = index // width // 3 * TILE + index % width // 3
    return (jnp.arange(TILE * TILE, dtype=jnp.int32)[:, None] == owner[None, :]).astype(jnp.float32)


def to_flat_tiles(field):
    rows, cols = field.shape
    along_x = rows // TILE
    along_y = cols // TILE
    shaped = field.reshape(along_x, TILE, along_y, TILE).transpose(0, 2, 1, 3)
    return shaped.reshape(1, 1, along_x * along_y, TILE * TILE)


def from_tiles(tiles, block_rows, block_cols):
    along_x = block_rows // TILE
    along_y = block_cols // TILE
    shaped = tiles.reshape(along_x, along_y, TILE, TILE).transpose(0, 2, 1, 3)
    return shaped.reshape(block_rows, block_cols)


def pad_last(array, before, after):
    widths = [(0, 0)] * (array.ndim - 1) + [(before, after)]
    return jnp.pad(array, widths)


def fine_substep(fine_ez, fine_hx, fine_hy, damp, gain, inbox, middle, border, cycle_value):
    width = TILE * 3
    column = jnp.arange(width * width, dtype=jnp.int32) % width
    ez_next_col = jnp.where(column < width - 1, pad_last(fine_ez[..., 1:], 0, 1), 0.0)
    ez_next_row = pad_last(fine_ez[..., width:], 0, width)
    fine_hx = jnp.where(inbox, fine_hx - HCOEF * (ez_next_col - fine_ez), 0.0)
    fine_hy = jnp.where(inbox, fine_hy + HCOEF * (ez_next_row - fine_ez), 0.0)
    hy_prev = pad_last(fine_hy[..., :-width], width, 0)
    hx_prev = jnp.where(column > 0, pad_last(fine_hx[..., :-1], 1, 0), 0.0)
    curl = fine_hy - hy_prev - (fine_hx - hx_prev)
    inner = damp * fine_ez + gain * curl
    fine_ez = jnp.where(middle, inner, jnp.where(border, cycle_value, 0.0))
    return (fine_ez, fine_hx, fine_hy)


def fine_round(
    fine_ez, fine_hx, fine_hy, damp, gain, inbox, middle, border, old_tiles, new_tiles, spread
):
    for sub in range(1, 4):
        weight = sub / 3.0
        mixed = (1.0 - weight) * old_tiles + weight * new_tiles
        cycle_value = jnp.dot(
            mixed, spread, precision=lax.Precision.HIGHEST, preferred_element_type=jnp.float32
        )
        fine_ez, fine_hx, fine_hy = fine_substep(
            fine_ez, fine_hx, fine_hy, damp, gain, inbox, middle, border, cycle_value
        )
    return (fine_ez, fine_hx, fine_hy)


def coarse_magnetic(ez, hx, hy):
    below = passed_along(ez[:1, :], "gx", -1)
    beside = passed_along(ez[:, :1], ("grp", "gy"), -1)
    ez_next_row = jnp.concatenate([ez[1:, :], below], axis=0)
    ez_next_col = jnp.concatenate([ez[:, 1:], beside], axis=1)
    hx = hx - HCOEF * (ez_next_col - ez)
    hy = hy + HCOEF * (ez_next_row - ez)
    above = passed_along(hy[-1:, :], "gx", 1)
    before = passed_along(hx[:, -1:], ("grp", "gy"), 1)
    hy_prev = jnp.concatenate([above, hy[:-1, :]], axis=0)
    hx_prev = jnp.concatenate([before, hx[:, :-1]], axis=1)
    curl = hy - hy_prev - (hx - hx_prev)
    return (hx, hy, curl)


def shards(
    coarse_ez,
    coarse_hx,
    coarse_hy,
    coarse_ids,
    mat_eps,
    mat_sig,
    fine_ez,
    fine_hx,
    fine_hy,
    fine_ids,
    boxes,
    src_cells,
    src_wave,
    rcv_cells,
):
    rows, cols = coarse_ez.shape
    fine_shape = fine_ez.shape
    flat_cells = fine_shape[-1]
    means_shape = fine_shape[:-1] + (TILE * TILE,)
    row_start = lax.axis_index("gx") * rows
    col_start = lax.axis_index(("grp", "gy")) * cols
    all_cols = cols * lax.axis_size(("grp", "gy"))
    spread = spread_table()
    damp, gain = coefficients(coarse_ids, mat_eps, mat_sig, 1.0)
    fine_damp, fine_gain = coefficients(fine_ids.reshape(-1, flat_cells), mat_eps, mat_sig, 3.0)
    owned_boxes = lax.all_to_all(boxes, "gx", split_axis=2, concat_axis=0, tiled=True).reshape(
        -1, 4
    )
    inbox, middle = flat_masks(owned_boxes)
    border = inbox & jnp.logical_not(middle)
    coarse_mid = from_tiles(box_masks(boxes, TILE, 1)[1], rows, cols)
    src_rows = (
        jnp.arange(rows, dtype=jnp.int32)[None, :] == (src_cells // all_cols - row_start)[:, None]
    ).astype(jnp.float32)
    src_cols = (
        jnp.arange(cols, dtype=jnp.int32)[None, :] == (src_cells % all_cols - col_start)[:, None]
    ).astype(jnp.float32)
    rcv_rows = (
        jnp.arange(rows, dtype=jnp.int32)[None, :] == (rcv_cells // all_cols - row_start)[:, None]
    ).astype(jnp.float32)
    rcv_cols = (
        jnp.arange(cols, dtype=jnp.int32)[None, :] == (rcv_cells % all_cols - col_start)[:, None]
    ).astype(jnp.float32)
    ez, hx, hy = (coarse_ez, coarse_hx, coarse_hy)
    field_ez = fine_ez.reshape(-1, flat_cells)
    field_hx = fine_hx.reshape(-1, flat_cells)
    field_hy = fine_hy.reshape(-1, flat_cells)
    held = lax.all_to_all(to_flat_tiles(ez), "gx", split_axis=2, concat_axis=0, tiled=True).reshape(
        -1, TILE * TILE
    )
    samples = []
    for step in range(STEPS):
        hx, hy, curl = coarse_magnetic(ez, hx, hy)
        weighted = src_rows * src_wave[step][:, None]
        drive = jnp.dot(
            weighted.T,
            src_cols,
            precision=lax.Precision.HIGHEST,
            preferred_element_type=jnp.float32,
        )
        new = damp * ez + gain * curl + drive
        old_tiles = held
        new_tiles = lax.all_to_all(
            to_flat_tiles(new), "gx", split_axis=2, concat_axis=0, tiled=True
        ).reshape(-1, TILE * TILE)
        held = new_tiles
        field_ez, field_hx, field_hy = fine_round(
            field_ez,
            field_hx,
            field_hy,
            fine_damp,
            fine_gain,
            inbox,
            middle,
            border,
            old_tiles,
            new_tiles,
            spread,
        )
        sums = lax.dot_general(
            field_ez,
            spread,
            (((1,), (1,)), ((), ())),
            precision=lax.Precision.HIGHEST,
            preferred_element_type=jnp.float32,
        )
        means = (sums / 9.0).reshape(means_shape)
        back = lax.all_to_all(means, "gx", split_axis=0, concat_axis=2, tiled=True)
        ez = jnp.where(coarse_mid, from_tiles(back, rows, cols), new)
        picked = jnp.dot(
            rcv_rows, ez, precision=lax.Precision.HIGHEST, preferred_element_type=jnp.float32
        )
        samples.append(jnp.sum(picked * rcv_cols, axis=1))
    traces = lax.psum(jnp.stack(samples), ("grp", "gx", "gy"))
    return (
        ez,
        hx,
        hy,
        field_ez.reshape(fine_shape),
        field_hx.reshape(fine_shape),
        field_hy.reshape(fine_shape),
        traces,
    )


def solution(mesh):
    placed = (
        P("gx", ("grp", "gy")),
        P("gx", ("grp", "gy")),
        P("gx", ("grp", "gy")),
        P("gx", ("grp", "gy")),
        P(),
        P(),
        P(None, ("grp", "gy"), "gx", None),
        P(None, ("grp", "gy"), "gx", None),
        P(None, ("grp", "gy"), "gx", None),
        P(None, ("grp", "gy"), "gx", None),
        P("gx", ("grp", "gy"), None, None),
        P(),
        P(),
        P(),
    )
    def body(*args):
        rows, cols = args[0].shape
        owners = lax.axis_size("gx")
        strips = cols == LANES and args[6].shape[2] * TILE == cols and rows == owners * TILE
        if strips and 5 * GROUP * owners <= LANES and args[13].shape[0] == LANES:
            return fast_shards(*args)
        return shards(*args)

    return jax.shard_map(
        body,
        mesh=mesh,
        in_specs=placed,
        out_specs=(
            P("gx", ("grp", "gy")),
            P("gx", ("grp", "gy")),
            P("gx", ("grp", "gy")),
            P(None, ("grp", "gy"), "gx", None),
            P(None, ("grp", "gy"), "gx", None),
            P(None, ("grp", "gy"), "gx", None),
            P(),
        ),
        check_vma=False,
    )
```

```python
import functools

import jax
import jax.numpy as jnp
from jax import lax
from jax.experimental import pallas as pl
from jax.experimental.pallas import tpu as pltpu
from jax.sharding import PartitionSpec as P

TILE = 16
STEPS = 3
SUBSTEPS = 3
LANES = 128
FIELDS = 4
WINDOW = 24
HALO = FIELDS * TILE
MESSAGE = HALO + 24
PLANES = 9
WIDE = 2 * LANES
GROUP = 6

COURANT = 0.5
HCOEF = 0.5
F32 = jnp.float32
BF16 = jnp.bfloat16
I32 = jnp.int32
COLS = ("grp", "gy")


def iota(shape, axis):
    return lax.broadcasted_iota(I32, shape, axis)


def f32(*shape):
    return jax.ShapeDtypeStruct(shape, F32)


def kept(*shape, dtype=F32):
    return pltpu.VMEM(shape, dtype)


def call(kernel, outs, args, scratch=(), far=(), far_outs=(), aliases=None, flops=1 << 20):
    vmem, hbm = (pl.BlockSpec(memory_space=m) for m in (pltpu.VMEM, pltpu.HBM))
    args = [
        pltpu.with_memory_space_constraint(x, pltpu.HBM)
        if k in far
        else x
        for k, x in enumerate(args)
    ]
    return pl.pallas_call(
        kernel,
        out_shape=outs,
        in_specs=[hbm if k in far else vmem for k in range(len(args))],
        out_specs=tuple(hbm if k in far_outs else vmem for k in range(len(outs))),
        scratch_shapes=list(scratch),
        input_output_aliases=aliases or {},
        compiler_params=pltpu.CompilerParams(vmem_limit_bytes=16 * 1024 * 1024),
        cost_estimate=pl.CostEstimate(flops=flops, bytes_accessed=1 << 20, transcendentals=0),
    )(*args)


def copies(sources, targets, sems):
    moves = [
        pltpu.make_async_copy(source, target, sems.at[k])
        for k, (source, target) in enumerate(zip(sources, targets))
    ]
    for move in moves:
        move.start()
    return moves


def ring(value, axis, steps):
    count = lax.axis_size(axis)
    return lax.ppermute(value, axis, [(k, (k + steps) % count) for k in range(count)])


def pack_kernel(owners, *refs):
    sources, outs = refs[:5], refs[5 : 5 + owners]
    held, sems = refs[5 + owners : 10 + owners], refs[10 + owners]
    for move in copies(sources, held, sems):
        move.wait()
    ez, hx, hy, ids, boxes = held
    me = lax.axis_index("gx")
    tiles = ez.shape[0] // 8
    count = boxes.shape[1]
    sub = iota((8, LANES), 0)
    lines = jnp.concatenate([boxes[...].astype(F32), jnp.zeros((4, LANES - count), F32)], axis=1)
    low, high, left, top = (jnp.broadcast_to(lines[k : k + 1, :], (8, LANES)) for k in range(4))
    for d in range(owners):
        g = lax.rem(me + d, owners)
        here = pl.multiple_of(g * TILE, TILE)
        after = pl.multiple_of(lax.rem(2 * g + 2, tiles) * 8, 8)
        before = pl.multiple_of(lax.rem(2 * g + tiles - 1, tiles) * 8, 8)
        edges = []
        for f, ref in enumerate((ez, hx, hy, ids)):
            outs[d][f * TILE : (f + 1) * TILE, :] = ref[pl.ds(here, TILE), :].astype(F32)
            edge = jnp.where(sub < 4, ref[pl.ds(after, 8), :], ref[pl.ds(before, 8), :])
            edges.append(edge.astype(F32))
        around_ez, around_hx, around_hy, around_ids = edges
        outs[d][HALO : HALO + 8, :] = jnp.where(sub == 3, low, jnp.where(sub == 4, high, around_ez))
        inner = jnp.where(sub < 4, pltpu.roll(around_ids, 2, 0), pltpu.roll(around_ids, 6, 0))
        outs[d][HALO + 8 : HALO + 16, :] = jnp.where((sub >= 2) & (sub < 6), inner, around_hx)
        outs[d][HALO + 16 : HALO + 24, :] = jnp.where(
            sub == 2, left, jnp.where(sub == 3, top, around_hy)
        )


def block_of(owners, d):
    return lax.rem(lax.axis_index("gx") + owners - d, owners)


def edges_kernel(owners, *refs):
    received, table = refs[:owners], refs[owners]
    out, windows, boxes, store = refs[owners + 1 :]
    me = lax.axis_index("gx")
    sub = iota((8, LANES), 0)
    for d in range(owners):
        store[block_of(owners, d)] = received[d][...]
    around = [
        [store[a, HALO + 8 * k : HALO + 8 * k + 8, :] for a in range(owners)] for k in range(3)
    ]
    row = iota((WINDOW, LANES), 0)
    row = jnp.where(row < 20, row, row - WINDOW)
    lane = iota((WINDOW, LANES), 1)
    total = jnp.zeros((WINDOW, LANES), F32)
    for a in range(owners):
        for k, at in enumerate((3, 4, 18, 19)):
            boxes[a, k : k + 1, :] = store[a, HALO + at : HALO + at + 1, :]
        tiles = []
        for tile in around:
            after = jnp.where(me == owners - 1, tile[min(a + 1, owners - 1)], tile[a])
            before = jnp.where(me == 0, tile[max(a - 1, 0)], tile[a])
            tiles.append(jnp.where(sub < 4, after, before))
        inner = jnp.where(sub < 4, pltpu.roll(tiles[1], 6, 0), pltpu.roll(tiles[1], 2, 0))
        fields = [
            jnp.concatenate([store[a, f * TILE : (f + 1) * TILE, :], tile], axis=0)
            for f, tile in enumerate((*tiles, inner))
        ]
        all_row = row + (a * owners * TILE + me * TILE)
        valid = (all_row >= 0) & (all_row < owners * owners * TILE)
        damp = jnp.zeros((WINDOW, LANES), F32)
        gain = jnp.zeros((WINDOW, LANES), F32)
        kinds = table.shape[0] // 2
        for m in range(kinds):
            hit = fields[3] == float(m)
            damp = jnp.where(hit, table[m : m + 1, :], damp)
            gain = jnp.where(hit, table[kinds + m : kinds + m + 1, :], gain)
        for f, value in enumerate((*fields[:3], damp, gain)):
            value = jnp.where(valid, value, 0.0)
            windows[f, a] = value
            at = GROUP * (f * owners + a)
            total = jnp.where((lane >= at) & (lane < at + GROUP), pltpu.roll(value, at + 3, 1), total)
    out[...] = total


def lane_of():
    return iota((8, LANES), 1)


def third_of(x, start):
    return lax.rem(x + start, 3)


def choose(parts, which):
    return jnp.where(which == 0, parts[0], jnp.where(which == 1, parts[1], parts[2]))


def take(x, lanes):
    return jnp.take_along_axis(x, lanes & (LANES - 1), axis=1)


def in_block(block):
    return ((block & 7) << 4) | (lane_of() & 15)


def halves(x):
    high = x.astype(BF16)
    return high, (x - high.astype(F32)).astype(BF16)


def thirds(x):
    high = x.astype(BF16)
    rest = x - high.astype(F32)
    return high, *halves(rest)


def lists(eps, sig, ratio):
    ones = jnp.ones((1, LANES), F32)
    both = []
    for m in range(eps.shape[0]):
        e, s = ones * eps[m], ones * sig[m]
        loss = s / (e * ratio)
        both.append(((1.0 - loss) / (1.0 + loss), COURANT / (e * (1.0 + loss))))
    return both


def turn(x, first, last):
    block = lane_of() >> 4
    sub = iota((8, LANES), 0)
    x = jnp.take_along_axis(x, first(sub, block) & 7, axis=0)
    x = pltpu.roll(x, 0, 1, stride=TILE, stride_axis=0)
    return jnp.take_along_axis(x, last(sub, block) & 7, axis=0)


def each_half(owners):
    for a in range(owners):
        for h in range(2):
            yield a, h, slice(8 * a, 8 * a + 8), slice(TILE * a + 8 * h, TILE * a + 8 * h + 8)


def spread_kernel(*refs):
    sources, (oez, ohx, ohy, odamp, ogain, coarse_kinds) = refs[:6], refs[6:12]
    held, (kinds, rows, sems) = refs[12:18], refs[18:]
    fez, fhx, fhy, ids, eps, sig = held
    moves = copies(sources, held, sems)
    half = eps.shape[0]
    for move in moves[4:]:
        move.wait()
    for ref, ratio, scale in ((coarse_kinds, 1.0, 1.0), (kinds, 3.0, 0.5)):
        for m, (damp, gain) in enumerate(lists(eps, sig, ratio)):
            ref[m : m + 1, :] = damp
            ref[half + m : half + m + 1, :] = scale * gain
    for move in moves[:4]:
        move.wait()
    owners = fez.shape[0] // 8
    lane, block = lane_of(), lane_of() >> 4
    for v in range(3):
        for a, h, tiles, at in each_half(owners):
            for f, ref in enumerate((fez, fhx, fhy, ids)):
                for r in range(3):
                    first = 9 * h + 3 * r
                    parts = [ref[tiles, k * LANES : (k + 1) * LANES] for k in range(first, first + 3)]
                    part = choose(parts, third_of(lane, 2 * v)).astype(F32)
                    rows[f, v, r, at] = take(part, 3 * lane + v)
    for u in range(3):
        for a, h, tiles, at in each_half(owners):
            for f in (3, 0, 1, 2):
                for v in range(3):
                    part = choose([rows[f, v, r, at] for r in range(3)], third_of(block, 2 * u))
                    value = turn(part, lambda r, b: r + b, lambda i, c: c - 3 * i - u)
                    if f == 0:
                        oez[3 * u + v, at] = value
                    elif f < 3:
                        (ohx, ohy)[f - 1][3 * u + v, at] = 2.0 * value
                    else:
                        damp = jnp.zeros((8, LANES), F32)
                        gain = jnp.zeros((8, LANES), F32)
                        for m in range(half):
                            hit = value == float(m)
                            damp = jnp.where(hit, kinds[m : m + 1, :], damp)
                            gain = jnp.where(hit, kinds[half + m : half + m + 1, :], gain)
                        odamp[3 * u + v, at] = damp
                        ogain[3 * u + v, at] = gain


def gather_kernel(ez, hx, hy, box, *refs):
    outs, (flat, rows, cells, sems) = refs[:3], refs[3:]
    owners = ez.shape[1] // TILE
    lane, block = lane_of(), lane_of() >> 4
    for u in range(3):
        for a, h, tiles, at in each_half(owners):
            for f, ref in enumerate((ez, hx, hy)):
                for v in range(3):
                    part = ref[3 * u + v, at]
                    part = part if f == 0 else 0.5 * (part * box[at])
                    rows[f, v, u, at] = turn(
                        part, lambda r, b: 3 * (b + r - u), lambda c, b: b - c
                    )
    for v in range(3):
        for a, h, tiles, at in each_half(owners):
            for f in range(3):
                parts = [rows[f, v, u, at] for u in range(3)]
                for r in range(3):
                    part = choose(parts, third_of(block, 2 * r))
                    cells[f, r, v, at] = take(part, 43 * (lane - v))
    moves = []
    for f in range(3):
        for a, h, tiles, at in each_half(owners):
            for r in range(3):
                parts = [cells[f, r, v, at] for v in range(3)]
                for k in range(3):
                    place = 9 * h + 3 * r + k
                    value = choose(parts, third_of(lane, 2 * k))
                    flat[f, tiles, place * LANES : (place + 1) * LANES] = value
        moves.append(pltpu.make_async_copy(flat.at[f], outs[f], sems.at[f]))
        moves[-1].start()
    for move in moves:
        move.wait()


def column_of():
    return lax.axis_index("grp") * lax.axis_size("gy") + lax.axis_index("gy")


def ready_kernel(owners, all_cols, *refs):
    windows, boxes, fdamp, fgain, far_src, far_wave, far_rcv = refs[:7]
    mdamp, mgain, mid, box, half, drive, row_hit, col_hit = refs[7:15]
    src, wave, rcv, sems = refs[15:]
    moves = copies((far_src, far_wave, far_rcv), (src, wave, rcv), sems)
    me = lax.axis_index("gx")
    column = column_of()
    rows = owners * TILE
    lane = lane_of()
    tile_col = (lane & 15).astype(F32)
    for a in range(owners):
        low_i, low_j, size_i, size_j = (
            take(jnp.broadcast_to(boxes[a, k : k + 1, :], (8, LANES)), 8 * me + (lane >> 4))
            for k in range(4)
        )
        high_i, high_j = low_i + size_i, low_j + size_j
        for h in range(2):
            i = (8 * h + iota((8, LANES), 0)).astype(F32)
            inside = (i >= low_i) & (i < high_i) & (tile_col >= low_j) & (tile_col < high_j)
            middle = (i > low_i) & (i < high_i - 1) & (tile_col > low_j) & (tile_col < high_j - 1)
            at = slice(TILE * a + 8 * h, TILE * a + 8 * h + 8)
            mid[at] = jnp.where(middle, 1.0, 0.0)
            box[at] = jnp.where(inside, 1.0, 0.0)
    for p in range(PLANES):
        mdamp[p] = fdamp[p] * mid[...]
        mgain[p] = fgain[p] * mid[...]
    for move in moves:
        move.wait()
    receivers = rcv[...]
    at_row = lax.div(receivers, all_cols)
    image = lax.rem(iota((3 * rows, LANES), 0), rows)
    image_row = (image >> 4) * rows + me * TILE + (image & 15)
    row_hit[...] = jnp.where(image_row == at_row, 1.0, 0.0).astype(BF16)
    at_col = receivers - at_row * all_cols - column * LANES
    col_hit[...] = jnp.where(iota((LANES, LANES), 0) == at_col, 1.0, 0.0)
    row = iota((WINDOW, WIDE), 0)
    row = jnp.where(row < 20, row, row - WINDOW)
    col = iota((WINDOW, WIDE), 1)
    col = jnp.where(col < LANES + 64, col, col - WIDE)
    all_col = col + column * LANES
    for a in range(owners):
        all_row = row + (a * rows + me * TILE)
        valid = (all_row >= 0) & (all_row < owners * rows) & (all_col >= 0) & (all_col < all_cols)
        cells = jnp.where(valid, all_row * all_cols + all_col, -1)
        half[a] = jnp.where(valid, HCOEF, 0.0)
        half[owners + a] = jnp.where(valid & (all_col > 0), HCOEF, 0.0)
        for n in range(STEPS):
            total = jnp.zeros((WINDOW, WIDE), F32)
            for k in range(src.shape[0]):
                total = total + jnp.where(cells == src[k], wave[n, k], 0.0)
            drive[n, a] = total


def step_kernel(owners, *refs):
    windows, from_left, from_right = refs[:3]
    mdamp, mgain, mid, box, half, drive, row_hit, col_hit = refs[6:14]
    oez, ohx, ohy = refs[14:17]
    back = refs[17 : 17 + owners]
    far_traces = refs[17 + owners]
    ez, hx, hy, behind, damp, gain, held, beside, picked, traces, sem = refs[18 + owners :]
    column = column_of()
    place = lax.rem(iota((WINDOW, LANES), 1), GROUP)
    right = jnp.where(column == lax.axis_size(COLS) - 1, 0.0, from_right[...])
    left = jnp.where(column == 0, 0.0, from_left[...])
    sides = jnp.where(place < 3, left, right)
    for f, ref in enumerate((ez, hx, hy, damp, gain)):
        for a in range(owners):
            at = GROUP * (f * owners + a)
            ref[a, :, 0:LANES] = windows[f, a]
            ref[a, :, LANES:WIDE] = pltpu.roll(sides, (LANES - 3 - at) % LANES, 1)
    for a in range(owners):
        behind[a] = pltpu.roll(hx[a], 1, 1)
    for u in range(3):
        for k in range(2 * owners):
            at = slice(8 * k, 8 * k + 8)
            beside[u, at] = pltpu.roll(ohx[3 * u + 2, at], 1, 1)
    sub = iota((8, LANES), 0)
    places = [(u, v, h) for u in range(3) for v in range(3) for h in range(2)]

    def substep(m, carry):
        weight = (m + 1) / SUBSTEPS
        for a in range(owners):
            at = [slice(TILE * a + 8 * h, TILE * a + 8 * h + 8) for h in range(2)]
            e = {(u, v, h): oez[3 * u + v, at[h]] for u, v, h in places}
            ahead = {(u, h): pltpu.roll(e[u, 0, h], LANES - 1, 1) for u in range(3) for h in range(2)}
            back_e = {(u, h): pltpu.roll(e[u, 2, h], 1, 1) for u in range(3) for h in range(2)}
            down = {(v, h): pltpu.roll(e[0, v, h], 7, 0) for v in range(3) for h in range(2)}
            y = {}
            for u, v, h in places:
                p = 3 * u + v
                if u < 2:
                    below = e[u + 1, v, h]
                elif h == 0:
                    below = jnp.where(sub < 7, down[v, 0], down[v, 1])
                else:
                    below = down[v, 1]
                y[u, v, h] = ohy[p, at[h]] + (below - e[u, v, h])
                ohy[p, at[h]] = y[u, v, h]
            up = {(v, h): pltpu.roll(y[2, v, h], 1, 0) for v in range(3) for h in range(2)}
            for v in range(3):
                up[v, 1] = jnp.where(sub < 1, up[v, 0], up[v, 1])
            for h in range(2):
                now = ez[a, 8 * h : 8 * h + 8, 0:LANES]
                cyc = (box[at[h]] - mid[at[h]]) * ((1.0 - weight) * held[at[h]] + weight * now)
                for u in range(3):
                    before = beside[u, at[h]] - (e[u, 0, h] - back_e[u, h])
                    beside[u, at[h]] = before
                    for v in range(3):
                        p = 3 * u + v
                        after = e[u, v + 1, h] if v < 2 else ahead[u, h]
                        x = ohx[p, at[h]] - (after - e[u, v, h])
                        ohx[p, at[h]] = x
                        above = y[u - 1, v, h] if u > 0 else up[v, h]
                        curl = (y[u, v, h] - above) - (x - before)
                        inner = mdamp[p, at[h]] * e[u, v, h] + mgain[p, at[h]] * curl
                        oez[p, at[h]] = inner + cyc
                        before = x
        return carry

    def pick(n):
        image = jnp.concatenate([ez[a, 0:TILE, 0:LANES] for a in range(owners)], axis=0)
        mixed = lax.dot_general(
            jnp.concatenate(thirds(image), axis=0),
            row_hit[...],
            (((0,), (0,)), ((), ())),
            preferred_element_type=F32,
        )
        picked[n : n + 1, :] = jnp.sum(mixed * col_hit[...], axis=0, keepdims=True)

    def step(n, carry):
        if n > 0:
            pick(n - 1)
        for a in range(owners):
            e = ez[a]
            held[TILE * a : TILE * a + TILE] = e[0:TILE, 0:LANES]
            scale = half[a]
            x = hx[a] - scale * (pltpu.roll(e, WIDE - 1, 1) - e)
            before = behind[a] - half[owners + a] * (e - pltpu.roll(e, 1, 1))
            y = hy[a] + scale * (pltpu.roll(e, WINDOW - 1, 0) - e)
            hx[a], hy[a], behind[a] = x, y, before
            curl = (y - pltpu.roll(y, 1, 0)) - (x - before)
            ez[a] = damp[a] * e + gain[a] * curl + drive[n, a]
        for m in range(SUBSTEPS):
            substep(m, 0)
        for a in range(owners):
            for h in range(2):
                at = slice(TILE * a + 8 * h, TILE * a + 8 * h + 8)
                total = oez[0, at]
                for p in range(1, PLANES):
                    total = total + oez[p, at]
                here = (a, slice(8 * h, 8 * h + 8), slice(0, LANES))
                ez[here] = jnp.where(mid[at] > 0.0, total * (1.0 / PLANES), ez[here])
        return carry

    picked[...] = jnp.zeros(picked.shape, F32)
    for n in range(STEPS):
        step(n, 0)
    pick(STEPS - 1)
    for k in range(traces.shape[0]):
        traces[k] = picked[0:STEPS, :]
    move = pltpu.make_async_copy(traces, far_traces, sem)
    move.start()
    for d in range(owners):
        a = block_of(owners, d)
        for f, ref in enumerate((ez, hx, hy)):
            back[d][f * TILE : (f + 1) * TILE, :] = ref[a, 0:TILE, 0:LANES]
    move.wait()


def place_kernel(owners, *refs):
    pieces = refs[:owners]
    traces = refs[owners]
    outs = refs[owners + 1 : owners + 4]
    out_trace = refs[owners + 4]
    me = lax.axis_index("gx")
    for d in range(owners):
        here = pl.multiple_of(lax.rem(me + d, owners) * TILE, TILE)
        for f in range(3):
            outs[f][pl.ds(here, TILE), :] = pieces[d][f * TILE : (f + 1) * TILE, :]
    out_trace[...] = jnp.sum(traces[...], axis=0)


def fast_shards(
    coarse_ez, coarse_hx, coarse_hy, coarse_ids, mat_eps, mat_sig,
    fine_ez, fine_hx, fine_hy, fine_ids, boxes, src_cells, src_wave, rcv_cells,
):
    owners = lax.axis_size("gx")
    every = ("grp", "gx", "gy")
    rows, cols = coarse_ez.shape
    all_cols = cols * lax.axis_size(COLS)
    fine_shape = fine_ez.shape
    count = fine_shape[0] * fine_shape[2]
    cells = fine_shape[-1]
    flat = [x.reshape(count, cells) for x in (fine_ez, fine_hx, fine_hy, fine_ids)]
    corners = boxes.reshape(boxes.shape[2:]).T
    block = pltpu.VMEM((rows, cols), F32)
    messages = call(
        functools.partial(pack_kernel, owners),
        tuple(f32(MESSAGE, cols) for _ in range(owners)),
        (coarse_ez, coarse_hx, coarse_hy, coarse_ids, corners),
        [block] * 3
        + [pltpu.VMEM((rows, cols), I32), pltpu.VMEM(corners.shape, I32)]
        + [pltpu.SemaphoreType.DMA((5,))],
        far=range(5),
    )
    received = [messages[0]] + [ring(messages[d], "gx", d) for d in range(1, owners)]
    planes = kept(PLANES, 2 * count, LANES)
    kinds = mat_eps.shape[0]
    *fields, fdamp, fgain, coarse_kinds = call(
        spread_kernel,
        (planes,) * 5 + (kept(2 * kinds, LANES),),
        (*flat, mat_eps, mat_sig),
        [pltpu.VMEM((count, cells), F32)] * 3
        + [pltpu.VMEM((count, cells), I32)]
        + [pltpu.SMEM((kinds,), F32)] * 2
        + [pltpu.VMEM((2 * kinds, LANES), F32), pltpu.VMEM((4, 3, 3, 2 * count, LANES), F32)]
        + [pltpu.SemaphoreType.DMA((6,))],
        far=range(6),
        flops=1 << 31,
    )
    edges, windows, lines = call(
        functools.partial(edges_kernel, owners),
        (f32(WINDOW, LANES), kept(5, owners, WINDOW, LANES), kept(owners, 8, LANES)),
        (*received, coarse_kinds),
        [pltpu.VMEM((owners, MESSAGE, LANES), F32)],
    )
    from_left = ring(edges, COLS, 1)
    from_right = ring(edges, COLS, -1)
    receivers = rcv_cells.shape[0]
    window = (owners, WINDOW, WIDE)
    tiles = kept(2 * count, LANES)
    ready = call(
        functools.partial(ready_kernel, owners, all_cols),
        (planes, planes, tiles, tiles, kept(2 * owners, *window[1:]), kept(STEPS, *window))
        + (kept(3 * owners * TILE, receivers, dtype=BF16), kept(LANES, receivers)),
        (windows, lines, fdamp, fgain, src_cells, src_wave, rcv_cells.reshape(1, receivers)),
        [pltpu.SMEM(src_cells.shape, I32), pltpu.SMEM(src_wave.shape, F32)]
        + [pltpu.VMEM((1, receivers), I32), pltpu.SemaphoreType.DMA((3,))],
        far=(4, 5, 6),
        flops=1 << 30,
    )
    *results, traces = call(
        functools.partial(step_kernel, owners),
        (planes,) * 3
        + tuple(f32(3 * TILE, LANES) for _ in range(owners))
        + (f32(lax.axis_size(every), STEPS, receivers),),
        (windows, from_left, from_right, *fields, *ready),
        [pltpu.VMEM(window, F32)] * 6
        + [pltpu.VMEM(tiles.shape, F32), pltpu.VMEM((3, *tiles.shape), F32)]
        + [pltpu.VMEM((8, receivers), F32)]
        + [pltpu.VMEM((lax.axis_size(every), STEPS, receivers), F32), pltpu.SemaphoreType.DMA],
        far_outs=(3 + owners,),
        aliases={3: 0, 4: 1, 5: 2},
        flops=1 << 30,
    )
    fine, back = results[:3], results[3:]
    traces = lax.all_to_all(traces, every, 0, 0)
    pieces = [back[0]] + [ring(back[d], "gx", owners - d) for d in range(1, owners)]
    finals = call(
        gather_kernel,
        (f32(count, cells),) * 3,
        (*fine, ready[3]),
        [pltpu.VMEM((3, count, cells), F32)]
        + [pltpu.VMEM((3, 3, 3, 2 * count, LANES), F32)] * 2
        + [pltpu.SemaphoreType.DMA((3,))],
        far_outs=range(3),
        flops=1 << 31,
    )
    ends = call(
        functools.partial(place_kernel, owners),
        (f32(rows, cols),) * 3 + (f32(STEPS, receivers),),
        (*pieces, traces),
    )
    return (*ends[:3], *(x.reshape(fine_shape) for x in finals), ends[3])


def passed_along(value, axis, steps):
    count = lax.axis_size(axis)
    initial, last = (max(0, -steps), min(count, count - steps))
    return lax.ppermute(value, axis, [(source, source + steps) for source in range(initial, last)])


def coefficients(ids, eps_table, sig_table, ratio):
    damp = jnp.zeros(ids.shape, jnp.float32)
    gain = jnp.zeros(ids.shape, jnp.float32)
    for material in range(eps_table.shape[0]):
        loss = sig_table[material] / (eps_table[material] * ratio)
        hit = ids == material
        damp = jnp.where(hit, (1.0 - loss) / (1.0 + loss), damp)
        gain = jnp.where(hit, COURANT / (eps_table[material] * (1.0 + loss)), gain)
    return (damp, gain)


def box_masks(boxes, cells, scale):
    coarse_of = jnp.arange(cells, dtype=jnp.int32) // scale
    low_i = boxes[..., 0:1]
    low_j = boxes[..., 1:2]
    high_i = low_i + boxes[..., 2:3]
    high_j = low_j + boxes[..., 3:4]
    rows_in = (coarse_of >= low_i) & (coarse_of < high_i)
    cols_in = (coarse_of >= low_j) & (coarse_of < high_j)
    rows_mid = (coarse_of > low_i) & (coarse_of < high_i - 1)
    cols_mid = (coarse_of > low_j) & (coarse_of < high_j - 1)
    inbox = rows_in[..., :, None] & cols_in[..., None, :]
    middle = rows_mid[..., :, None] & cols_mid[..., None, :]
    return (inbox, middle)


def flat_masks(boxes):
    width = TILE * 3
    index = jnp.arange(width * width, dtype=jnp.int32)
    coarse_i = index // width // 3
    coarse_j = index % width // 3
    low_i = boxes[:, 0:1]
    low_j = boxes[:, 1:2]
    high_i = low_i + boxes[:, 2:3]
    high_j = low_j + boxes[:, 3:4]
    inbox = (coarse_i >= low_i) & (coarse_i < high_i) & (coarse_j >= low_j) & (coarse_j < high_j)
    middle = (
        (coarse_i > low_i) & (coarse_i < high_i - 1) & (coarse_j > low_j) & (coarse_j < high_j - 1)
    )
    return (inbox, middle)


def spread_table():
    width = TILE * 3
    index = jnp.arange(width * width, dtype=jnp.int32)
    owner = index // width // 3 * TILE + index % width // 3
    return (jnp.arange(TILE * TILE, dtype=jnp.int32)[:, None] == owner[None, :]).astype(jnp.float32)


def to_flat_tiles(field):
    rows, cols = field.shape
    along_x = rows // TILE
    along_y = cols // TILE
    shaped = field.reshape(along_x, TILE, along_y, TILE).transpose(0, 2, 1, 3)
    return shaped.reshape(1, 1, along_x * along_y, TILE * TILE)


def from_tiles(tiles, block_rows, block_cols):
    along_x = block_rows // TILE
    along_y = block_cols // TILE
    shaped = tiles.reshape(along_x, along_y, TILE, TILE).transpose(0, 2, 1, 3)
    return shaped.reshape(block_rows, block_cols)


def pad_last(array, before, after):
    widths = [(0, 0)] * (array.ndim - 1) + [(before, after)]
    return jnp.pad(array, widths)


def fine_substep(fine_ez, fine_hx, fine_hy, damp, gain, inbox, middle, border, cycle_value):
    width = TILE * 3
    column = jnp.arange(width * width, dtype=jnp.int32) % width
    ez_next_col = jnp.where(column < width - 1, pad_last(fine_ez[..., 1:], 0, 1), 0.0)
    ez_next_row = pad_last(fine_ez[..., width:], 0, width)
    fine_hx = jnp.where(inbox, fine_hx - HCOEF * (ez_next_col - fine_ez), 0.0)
    fine_hy = jnp.where(inbox, fine_hy + HCOEF * (ez_next_row - fine_ez), 0.0)
    hy_prev = pad_last(fine_hy[..., :-width], width, 0)
    hx_prev = jnp.where(column > 0, pad_last(fine_hx[..., :-1], 1, 0), 0.0)
    curl = fine_hy - hy_prev - (fine_hx - hx_prev)
    inner = damp * fine_ez + gain * curl
    fine_ez = jnp.where(middle, inner, jnp.where(border, cycle_value, 0.0))
    return (fine_ez, fine_hx, fine_hy)


def fine_round(
    fine_ez, fine_hx, fine_hy, damp, gain, inbox, middle, border, old_tiles, new_tiles, spread
):
    for sub in range(1, 4):
        weight = sub / 3.0
        mixed = (1.0 - weight) * old_tiles + weight * new_tiles
        cycle_value = jnp.dot(
            mixed, spread, precision=lax.Precision.HIGHEST, preferred_element_type=jnp.float32
        )
        fine_ez, fine_hx, fine_hy = fine_substep(
            fine_ez, fine_hx, fine_hy, damp, gain, inbox, middle, border, cycle_value
        )
    return (fine_ez, fine_hx, fine_hy)


def coarse_magnetic(ez, hx, hy):
    below = passed_along(ez[:1, :], "gx", -1)
    beside = passed_along(ez[:, :1], ("grp", "gy"), -1)
    ez_next_row = jnp.concatenate([ez[1:, :], below], axis=0)
    ez_next_col = jnp.concatenate([ez[:, 1:], beside], axis=1)
    hx = hx - HCOEF * (ez_next_col - ez)
    hy = hy + HCOEF * (ez_next_row - ez)
    above = passed_along(hy[-1:, :], "gx", 1)
    before = passed_along(hx[:, -1:], ("grp", "gy"), 1)
    hy_prev = jnp.concatenate([above, hy[:-1, :]], axis=0)
    hx_prev = jnp.concatenate([before, hx[:, :-1]], axis=1)
    curl = hy - hy_prev - (hx - hx_prev)
    return (hx, hy, curl)


def shards(
    coarse_ez,
    coarse_hx,
    coarse_hy,
    coarse_ids,
    mat_eps,
    mat_sig,
    fine_ez,
    fine_hx,
    fine_hy,
    fine_ids,
    boxes,
    src_cells,
    src_wave,
    rcv_cells,
):
    rows, cols = coarse_ez.shape
    fine_shape = fine_ez.shape
    flat_cells = fine_shape[-1]
    means_shape = fine_shape[:-1] + (TILE * TILE,)
    row_start = lax.axis_index("gx") * rows
    col_start = lax.axis_index(("grp", "gy")) * cols
    all_cols = cols * lax.axis_size(("grp", "gy"))
    spread = spread_table()
    damp, gain = coefficients(coarse_ids, mat_eps, mat_sig, 1.0)
    fine_damp, fine_gain = coefficients(fine_ids.reshape(-1, flat_cells), mat_eps, mat_sig, 3.0)
    owned_boxes = lax.all_to_all(boxes, "gx", split_axis=2, concat_axis=0, tiled=True).reshape(
        -1, 4
    )
    inbox, middle = flat_masks(owned_boxes)
    border = inbox & jnp.logical_not(middle)
    coarse_mid = from_tiles(box_masks(boxes, TILE, 1)[1], rows, cols)
    src_rows = (
        jnp.arange(rows, dtype=jnp.int32)[None, :] == (src_cells // all_cols - row_start)[:, None]
    ).astype(jnp.float32)
    src_cols = (
        jnp.arange(cols, dtype=jnp.int32)[None, :] == (src_cells % all_cols - col_start)[:, None]
    ).astype(jnp.float32)
    rcv_rows = (
        jnp.arange(rows, dtype=jnp.int32)[None, :] == (rcv_cells // all_cols - row_start)[:, None]
    ).astype(jnp.float32)
    rcv_cols = (
        jnp.arange(cols, dtype=jnp.int32)[None, :] == (rcv_cells % all_cols - col_start)[:, None]
    ).astype(jnp.float32)
    ez, hx, hy = (coarse_ez, coarse_hx, coarse_hy)
    field_ez = fine_ez.reshape(-1, flat_cells)
    field_hx = fine_hx.reshape(-1, flat_cells)
    field_hy = fine_hy.reshape(-1, flat_cells)
    held = lax.all_to_all(to_flat_tiles(ez), "gx", split_axis=2, concat_axis=0, tiled=True).reshape(
        -1, TILE * TILE
    )
    samples = []
    for step in range(STEPS):
        hx, hy, curl = coarse_magnetic(ez, hx, hy)
        weighted = src_rows * src_wave[step][:, None]
        drive = jnp.dot(
            weighted.T,
            src_cols,
            precision=lax.Precision.HIGHEST,
            preferred_element_type=jnp.float32,
        )
        new = damp * ez + gain * curl + drive
        old_tiles = held
        new_tiles = lax.all_to_all(
            to_flat_tiles(new), "gx", split_axis=2, concat_axis=0, tiled=True
        ).reshape(-1, TILE * TILE)
        held = new_tiles
        field_ez, field_hx, field_hy = fine_round(
            field_ez,
            field_hx,
            field_hy,
            fine_damp,
            fine_gain,
            inbox,
            middle,
            border,
            old_tiles,
            new_tiles,
            spread,
        )
        sums = lax.dot_general(
            field_ez,
            spread,
            (((1,), (1,)), ((), ())),
            precision=lax.Precision.HIGHEST,
            preferred_element_type=jnp.float32,
        )
        means = (sums / 9.0).reshape(means_shape)
        back = lax.all_to_all(means, "gx", split_axis=0, concat_axis=2, tiled=True)
        ez = jnp.where(coarse_mid, from_tiles(back, rows, cols), new)
        picked = jnp.dot(
            rcv_rows, ez, precision=lax.Precision.HIGHEST, preferred_element_type=jnp.float32
        )
        samples.append(jnp.sum(picked * rcv_cols, axis=1))
    traces = lax.psum(jnp.stack(samples), ("grp", "gx", "gy"))
    return (
        ez,
        hx,
        hy,
        field_ez.reshape(fine_shape),
        field_hx.reshape(fine_shape),
        field_hy.reshape(fine_shape),
        traces,
    )


def solution(mesh):
    placed = (
        P("gx", ("grp", "gy")),
        P("gx", ("grp", "gy")),
        P("gx", ("grp", "gy")),
        P("gx", ("grp", "gy")),
        P(),
        P(),
        P(None, ("grp", "gy"), "gx", None),
        P(None, ("grp", "gy"), "gx", None),
        P(None, ("grp", "gy"), "gx", None),
        P(None, ("grp", "gy"), "gx", None),
        P("gx", ("grp", "gy"), None, None),
        P(),
        P(),
        P(),
    )
    def body(*args):
        rows, cols = args[0].shape
        owners = lax.axis_size("gx")
        strips = cols == LANES and args[6].shape[2] * TILE == cols and rows == owners * TILE
        if strips and 5 * GROUP * owners <= LANES and args[13].shape[0] == LANES:
            return fast_shards(*args)
        return shards(*args)

    return jax.shard_map(
        body,
        mesh=mesh,
        in_specs=placed,
        out_specs=(
            P("gx", ("grp", "gy")),
            P("gx", ("grp", "gy")),
            P("gx", ("grp", "gy")),
            P(None, ("grp", "gy"), "gx", None),
            P(None, ("grp", "gy"), "gx", None),
            P(None, ("grp", "gy"), "gx", None),
            P(),
        ),
        check_vma=False,
    )
```

```python
import functools

import jax
import jax.numpy as jnp
from jax import lax
from jax.experimental import pallas as pl
from jax.experimental.pallas import tpu as pltpu
from jax.sharding import PartitionSpec as P

TILE = 16
STEPS = 3
SUBSTEPS = 3
LANES = 128
FIELDS = 4
WINDOW = 24
HALO = FIELDS * TILE
MESSAGE = HALO + 24
PLANES = 9
WIDE = 2 * LANES
GROUP = 6

COURANT = 0.5
HCOEF = 0.5
F32 = jnp.float32
BF16 = jnp.bfloat16
I32 = jnp.int32
COLS = ("grp", "gy")


def iota(shape, axis):
    return lax.broadcasted_iota(I32, shape, axis)


def f32(*shape):
    return jax.ShapeDtypeStruct(shape, F32)


def kept(*shape, dtype=F32):
    return pltpu.VMEM(shape, dtype)


def call(kernel, outs, args, scratch=(), far=(), far_outs=(), aliases=None, flops=1 << 20):
    vmem, hbm = (pl.BlockSpec(memory_space=m) for m in (pltpu.VMEM, pltpu.HBM))
    args = [
        pltpu.with_memory_space_constraint(x, pltpu.HBM)
        if k in far
        else x
        for k, x in enumerate(args)
    ]
    return pl.pallas_call(
        kernel,
        out_shape=outs,
        in_specs=[hbm if k in far else vmem for k in range(len(args))],
        out_specs=tuple(hbm if k in far_outs else vmem for k in range(len(outs))),
        scratch_shapes=list(scratch),
        input_output_aliases=aliases or {},
        compiler_params=pltpu.CompilerParams(vmem_limit_bytes=16 * 1024 * 1024),
        cost_estimate=pl.CostEstimate(flops=flops, bytes_accessed=1 << 20, transcendentals=0),
    )(*args)


def copies(sources, targets, sems):
    moves = [
        pltpu.make_async_copy(source, target, sems.at[k])
        for k, (source, target) in enumerate(zip(sources, targets))
    ]
    for move in moves:
        move.start()
    return moves


def ring(value, axis, steps):
    count = lax.axis_size(axis)
    return lax.ppermute(value, axis, [(k, (k + steps) % count) for k in range(count)])


def pack_kernel(owners, *refs):
    sources, outs = refs[:5], refs[5 : 5 + owners]
    held, sems = refs[5 + owners : 10 + owners], refs[10 + owners]
    for move in copies(sources, held, sems):
        move.wait()
    ez, hx, hy, ids, boxes = held
    me = lax.axis_index("gx")
    tiles = ez.shape[0] // 8
    count = boxes.shape[1]
    sub = iota((8, LANES), 0)
    lines = jnp.concatenate([boxes[...].astype(F32), jnp.zeros((4, LANES - count), F32)], axis=1)
    low, high, left, top = (jnp.broadcast_to(lines[k : k + 1, :], (8, LANES)) for k in range(4))
    for d in range(owners):
        g = lax.rem(me + d, owners)
        here = pl.multiple_of(g * TILE, TILE)
        after = pl.multiple_of(lax.rem(2 * g + 2, tiles) * 8, 8)
        before = pl.multiple_of(lax.rem(2 * g + tiles - 1, tiles) * 8, 8)
        edges = []
        for f, ref in enumerate((ez, hx, hy, ids)):
            outs[d][f * TILE : (f + 1) * TILE, :] = ref[pl.ds(here, TILE), :].astype(F32)
            edge = jnp.where(sub < 4, ref[pl.ds(after, 8), :], ref[pl.ds(before, 8), :])
            edges.append(edge.astype(F32))
        around_ez, around_hx, around_hy, around_ids = edges
        outs[d][HALO : HALO + 8, :] = jnp.where(sub == 3, low, jnp.where(sub == 4, high, around_ez))
        inner = jnp.where(sub < 4, pltpu.roll(around_ids, 2, 0), pltpu.roll(around_ids, 6, 0))
        outs[d][HALO + 8 : HALO + 16, :] = jnp.where((sub >= 2) & (sub < 6), inner, around_hx)
        outs[d][HALO + 16 : HALO + 24, :] = jnp.where(
            sub == 2, left, jnp.where(sub == 3, top, around_hy)
        )


def block_of(owners, d):
    return lax.rem(lax.axis_index("gx") + owners - d, owners)


def edges_kernel(owners, *refs):
    received, table = refs[:owners], refs[owners]
    out, windows, boxes, store = refs[owners + 1 :]
    me = lax.axis_index("gx")
    sub = iota((8, LANES), 0)
    for d in range(owners):
        store[block_of(owners, d)] = received[d][...]
    around = [
        [store[a, HALO + 8 * k : HALO + 8 * k + 8, :] for a in range(owners)] for k in range(3)
    ]
    row = iota((WINDOW, LANES), 0)
    row = jnp.where(row < 20, row, row - WINDOW)
    lane = iota((WINDOW, LANES), 1)
    total = jnp.zeros((WINDOW, LANES), F32)
    for a in range(owners):
        for k, at in enumerate((3, 4, 18, 19)):
            boxes[a, k : k + 1, :] = store[a, HALO + at : HALO + at + 1, :]
        tiles = []
        for tile in around:
            after = jnp.where(me == owners - 1, tile[min(a + 1, owners - 1)], tile[a])
            before = jnp.where(me == 0, tile[max(a - 1, 0)], tile[a])
            tiles.append(jnp.where(sub < 4, after, before))
        inner = jnp.where(sub < 4, pltpu.roll(tiles[1], 6, 0), pltpu.roll(tiles[1], 2, 0))
        fields = [
            jnp.concatenate([store[a, f * TILE : (f + 1) * TILE, :], tile], axis=0)
            for f, tile in enumerate((*tiles, inner))
        ]
        all_row = row + (a * owners * TILE + me * TILE)
        valid = (all_row >= 0) & (all_row < owners * owners * TILE)
        damp = jnp.zeros((WINDOW, LANES), F32)
        gain = jnp.zeros((WINDOW, LANES), F32)
        kinds = table.shape[0] // 2
        for m in range(kinds):
            hit = fields[3] == float(m)
            damp = jnp.where(hit, table[m : m + 1, :], damp)
            gain = jnp.where(hit, table[kinds + m : kinds + m + 1, :], gain)
        for f, value in enumerate((*fields[:3], damp, gain)):
            value = jnp.where(valid, value, 0.0)
            windows[f, a] = value
            at = GROUP * (f * owners + a)
            total = jnp.where((lane >= at) & (lane < at + GROUP), pltpu.roll(value, at + 3, 1), total)
    out[...] = total


def lane_of():
    return iota((8, LANES), 1)


def third_of(x, start):
    return lax.rem(x + start, 3)


def choose(parts, which):
    return jnp.where(which == 0, parts[0], jnp.where(which == 1, parts[1], parts[2]))


def take(x, lanes):
    return jnp.take_along_axis(x, lanes & (LANES - 1), axis=1)


def in_block(block):
    return ((block & 7) << 4) | (lane_of() & 15)


def halves(x):
    high = x.astype(BF16)
    return high, (x - high.astype(F32)).astype(BF16)


def thirds(x):
    high = x.astype(BF16)
    rest = x - high.astype(F32)
    return high, *halves(rest)


def lists(eps, sig, ratio):
    ones = jnp.ones((1, LANES), F32)
    both = []
    for m in range(eps.shape[0]):
        e, s = ones * eps[m], ones * sig[m]
        loss = s / (e * ratio)
        both.append(((1.0 - loss) / (1.0 + loss), COURANT / (e * (1.0 + loss))))
    return both


def turn(x, first, last):
    block = lane_of() >> 4
    sub = iota((8, LANES), 0)
    x = jnp.take_along_axis(x, first(sub, block) & 7, axis=0)
    x = pltpu.roll(x, 0, 1, stride=TILE, stride_axis=0)
    return jnp.take_along_axis(x, last(sub, block) & 7, axis=0)


def each_half(owners):
    for a in range(owners):
        for h in range(2):
            yield a, h, slice(8 * a, 8 * a + 8), slice(TILE * a + 8 * h, TILE * a + 8 * h + 8)


def spread_kernel(*refs):
    sources, (oez, ohx, ohy, odamp, ogain, coarse_kinds) = refs[:6], refs[6:12]
    held, (kinds, rows, sems) = refs[12:18], refs[18:]
    fez, fhx, fhy, ids, eps, sig = held
    moves = copies(sources, held, sems)
    half = eps.shape[0]
    for move in moves[4:]:
        move.wait()
    for ref, ratio, scale in ((coarse_kinds, 1.0, 1.0), (kinds, 3.0, 0.5)):
        for m, (damp, gain) in enumerate(lists(eps, sig, ratio)):
            ref[m : m + 1, :] = damp
            ref[half + m : half + m + 1, :] = scale * gain
    for move in moves[:4]:
        move.wait()
    owners = fez.shape[0] // 8
    lane, block = lane_of(), lane_of() >> 4
    for v in range(3):
        for a, h, tiles, at in each_half(owners):
            for f, ref in enumerate((fez, fhx, fhy, ids)):
                for r in range(3):
                    first = 9 * h + 3 * r
                    parts = [ref[tiles, k * LANES : (k + 1) * LANES] for k in range(first, first + 3)]
                    part = choose(parts, third_of(lane, 2 * v)).astype(F32)
                    rows[f, v, r, at] = take(part, 3 * lane + v)
    for u in range(3):
        for a, h, tiles, at in each_half(owners):
            for f in (3, 0, 1, 2):
                for v in range(3):
                    part = choose([rows[f, v, r, at] for r in range(3)], third_of(block, 2 * u))
                    value = turn(part, lambda r, b: r + b, lambda i, c: c - 3 * i - u)
                    if f == 0:
                        oez[3 * u + v, at] = value
                    elif f < 3:
                        (ohx, ohy)[f - 1][3 * u + v, at] = 2.0 * value
                    else:
                        damp = jnp.zeros((8, LANES), F32)
                        gain = jnp.zeros((8, LANES), F32)
                        for m in range(half):
                            hit = value == float(m)
                            damp = jnp.where(hit, kinds[m : m + 1, :], damp)
                            gain = jnp.where(hit, kinds[half + m : half + m + 1, :], gain)
                        odamp[3 * u + v, at] = damp
                        ogain[3 * u + v, at] = gain


def gather_kernel(ez, hx, hy, box, *refs):
    outs, (flat, rows, cells, sems) = refs[:3], refs[3:]
    owners = ez.shape[1] // TILE
    lane, block = lane_of(), lane_of() >> 4
    for u in range(3):
        for a, h, tiles, at in each_half(owners):
            for f, ref in enumerate((ez, hx, hy)):
                for v in range(3):
                    part = ref[3 * u + v, at]
                    part = part if f == 0 else 0.5 * (part * box[at])
                    rows[f, v, u, at] = turn(
                        part, lambda r, b: 3 * (b + r - u), lambda c, b: b - c
                    )
    for v in range(3):
        for a, h, tiles, at in each_half(owners):
            for f in range(3):
                parts = [rows[f, v, u, at] for u in range(3)]
                for r in range(3):
                    part = choose(parts, third_of(block, 2 * r))
                    cells[f, r, v, at] = take(part, 43 * (lane - v))
    moves = []
    for f in range(3):
        for a, h, tiles, at in each_half(owners):
            for r in range(3):
                parts = [cells[f, r, v, at] for v in range(3)]
                for k in range(3):
                    place = 9 * h + 3 * r + k
                    value = choose(parts, third_of(lane, 2 * k))
                    flat[f, tiles, place * LANES : (place + 1) * LANES] = value
        moves.append(pltpu.make_async_copy(flat.at[f], outs[f], sems.at[f]))
        moves[-1].start()
    for move in moves:
        move.wait()


def column_of():
    return lax.axis_index("grp") * lax.axis_size("gy") + lax.axis_index("gy")


def ready_kernel(owners, all_cols, *refs):
    windows, boxes, fdamp, fgain, far_src, far_wave, far_rcv = refs[:7]
    mdamp, mgain, mid, box, half, drive, row_hit, col_hit = refs[7:15]
    src, wave, rcv, sems = refs[15:]
    moves = copies((far_src, far_wave, far_rcv), (src, wave, rcv), sems)
    me = lax.axis_index("gx")
    column = column_of()
    rows = owners * TILE
    lane = lane_of()
    tile_col = (lane & 15).astype(F32)
    for a in range(owners):
        low_i, low_j, size_i, size_j = (
            take(jnp.broadcast_to(boxes[a, k : k + 1, :], (8, LANES)), 8 * me + (lane >> 4))
            for k in range(4)
        )
        high_i, high_j = low_i + size_i, low_j + size_j
        for h in range(2):
            i = (8 * h + iota((8, LANES), 0)).astype(F32)
            inside = (i >= low_i) & (i < high_i) & (tile_col >= low_j) & (tile_col < high_j)
            middle = (i > low_i) & (i < high_i - 1) & (tile_col > low_j) & (tile_col < high_j - 1)
            at = slice(TILE * a + 8 * h, TILE * a + 8 * h + 8)
            mid[at] = jnp.where(middle, 1.0, 0.0)
            box[at] = jnp.where(inside, 1.0, 0.0)
    for p in range(PLANES):
        mdamp[p] = fdamp[p] * mid[...]
        mgain[p] = fgain[p] * mid[...]
    for move in moves:
        move.wait()
    receivers = rcv[...]
    at_row = lax.div(receivers, all_cols)
    image = lax.rem(iota((3 * rows, LANES), 0), rows)
    image_row = (image >> 4) * rows + me * TILE + (image & 15)
    row_hit[...] = jnp.where(image_row == at_row, 1.0, 0.0).astype(BF16)
    at_col = receivers - at_row * all_cols - column * LANES
    col_hit[...] = jnp.where(iota((LANES, LANES), 0) == at_col, 1.0, 0.0)
    row = iota((WINDOW, WIDE), 0)
    row = jnp.where(row < 20, row, row - WINDOW)
    col = iota((WINDOW, WIDE), 1)
    col = jnp.where(col < LANES + 64, col, col - WIDE)
    all_col = col + column * LANES
    for a in range(owners):
        all_row = row + (a * rows + me * TILE)
        valid = (all_row >= 0) & (all_row < owners * rows) & (all_col >= 0) & (all_col < all_cols)
        cells = jnp.where(valid, all_row * all_cols + all_col, -1)
        half[a] = jnp.where(valid, HCOEF, 0.0)
        half[owners + a] = jnp.where(valid & (all_col > 0), HCOEF, 0.0)
        for n in range(STEPS):
            total = jnp.zeros((WINDOW, WIDE), F32)
            for k in range(src.shape[0]):
                total = total + jnp.where(cells == src[k], wave[n, k], 0.0)
            drive[n, a] = total


def step_kernel(owners, *refs):
    windows, from_left, from_right = refs[:3]
    mdamp, mgain, mid, box, half, drive, row_hit, col_hit = refs[6:14]
    oez, ohx, ohy = refs[14:17]
    back, far_traces = refs[17 : 16 + owners], refs[16 + owners]
    ez, hx, hy, behind, damp, gain, held, beside, picked, traces, sem = refs[17 + owners :]
    column = column_of()
    place = lax.rem(iota((WINDOW, LANES), 1), GROUP)
    right = jnp.where(column == lax.axis_size(COLS) - 1, 0.0, from_right[...])
    left = jnp.where(column == 0, 0.0, from_left[...])
    sides = jnp.where(place < 3, left, right)
    for f, ref in enumerate((ez, hx, hy, damp, gain)):
        for a in range(owners):
            at = GROUP * (f * owners + a)
            ref[a, :, 0:LANES] = windows[f, a]
            ref[a, :, LANES:WIDE] = pltpu.roll(sides, (LANES - 3 - at) % LANES, 1)
    for a in range(owners):
        behind[a] = pltpu.roll(hx[a], 1, 1)
    for u in range(3):
        for k in range(2 * owners):
            at = slice(8 * k, 8 * k + 8)
            beside[u, at] = pltpu.roll(ohx[3 * u + 2, at], 1, 1)
    sub = iota((8, LANES), 0)
    places = [(u, v, h) for u in range(3) for v in range(3) for h in range(2)]

    def substep(m, carry):
        weight = (m + 1) / SUBSTEPS
        for a in range(owners):
            at = [slice(TILE * a + 8 * h, TILE * a + 8 * h + 8) for h in range(2)]
            e = {(u, v, h): oez[3 * u + v, at[h]] for u, v, h in places}
            ahead = {(u, h): pltpu.roll(e[u, 0, h], LANES - 1, 1) for u in range(3) for h in range(2)}
            back_e = {(u, h): pltpu.roll(e[u, 2, h], 1, 1) for u in range(3) for h in range(2)}
            down = {(v, h): pltpu.roll(e[0, v, h], 7, 0) for v in range(3) for h in range(2)}
            y = {}
            for u, v, h in places:
                p = 3 * u + v
                if u < 2:
                    below = e[u + 1, v, h]
                elif h == 0:
                    below = jnp.where(sub < 7, down[v, 0], down[v, 1])
                else:
                    below = down[v, 1]
                y[u, v, h] = ohy[p, at[h]] + (below - e[u, v, h])
                ohy[p, at[h]] = y[u, v, h]
            up = {(v, h): pltpu.roll(y[2, v, h], 1, 0) for v in range(3) for h in range(2)}
            for v in range(3):
                up[v, 1] = jnp.where(sub < 1, up[v, 0], up[v, 1])
            for h in range(2):
                now = ez[a, 8 * h : 8 * h + 8, 0:LANES]
                cyc = (box[at[h]] - mid[at[h]]) * ((1.0 - weight) * held[at[h]] + weight * now)
                for u in range(3):
                    before = beside[u, at[h]] - (e[u, 0, h] - back_e[u, h])
                    beside[u, at[h]] = before
                    for v in range(3):
                        p = 3 * u + v
                        after = e[u, v + 1, h] if v < 2 else ahead[u, h]
                        x = ohx[p, at[h]] - (after - e[u, v, h])
                        ohx[p, at[h]] = x
                        above = y[u - 1, v, h] if u > 0 else up[v, h]
                        curl = (y[u, v, h] - above) - (x - before)
                        inner = mdamp[p, at[h]] * e[u, v, h] + mgain[p, at[h]] * curl
                        oez[p, at[h]] = inner + cyc
                        before = x
        return carry

    def pick(n):
        image = jnp.concatenate([ez[a, 0:TILE, 0:LANES] for a in range(owners)], axis=0)
        mixed = lax.dot_general(
            jnp.concatenate(thirds(image), axis=0),
            row_hit[...],
            (((0,), (0,)), ((), ())),
            preferred_element_type=F32,
        )
        picked[n : n + 1, :] = jnp.sum(mixed * col_hit[...], axis=0, keepdims=True)

    def step(n, carry):
        if n > 0:
            pick(n - 1)
        for a in range(owners):
            e = ez[a]
            held[TILE * a : TILE * a + TILE] = e[0:TILE, 0:LANES]
            scale = half[a]
            x = hx[a] - scale * (pltpu.roll(e, WIDE - 1, 1) - e)
            before = behind[a] - half[owners + a] * (e - pltpu.roll(e, 1, 1))
            y = hy[a] + scale * (pltpu.roll(e, WINDOW - 1, 0) - e)
            hx[a], hy[a], behind[a] = x, y, before
            curl = (y - pltpu.roll(y, 1, 0)) - (x - before)
            ez[a] = damp[a] * e + gain[a] * curl + drive[n, a]
        for m in range(SUBSTEPS):
            substep(m, 0)
        for a in range(owners):
            for h in range(2):
                at = slice(TILE * a + 8 * h, TILE * a + 8 * h + 8)
                total = oez[0, at]
                for p in range(1, PLANES):
                    total = total + oez[p, at]
                here = (a, slice(8 * h, 8 * h + 8), slice(0, LANES))
                ez[here] = jnp.where(mid[at] > 0.0, total * (1.0 / PLANES), ez[here])
        return carry

    picked[...] = jnp.zeros(picked.shape, F32)
    for n in range(STEPS):
        step(n, 0)
    pick(STEPS - 1)
    for k in range(traces.shape[0]):
        traces[k] = picked[0:STEPS, :]
    move = pltpu.make_async_copy(traces, far_traces, sem)
    move.start()
    me = lax.axis_index("gx")
    for (out, at), d in zip(((0, 0), (1, 0), (1, 1), (2, 0)), (0, 1, 3, 2)):
        a = lax.bitwise_xor(me, d)
        for f, ref in enumerate((ez, hx, hy)):
            start = (3 * at + f) * TILE
            back[out][start : start + TILE, :] = ref[a, 0:TILE, 0:LANES]
    move.wait()


def swapped(value, axis, bit):
    return lax.ppermute(value, axis, [(k, k ^ bit) for k in range(lax.axis_size(axis))])


def place_kernel(own, near, far, traces, *outs):
    me = lax.axis_index("gx")
    for piece, at, d in ((own, 0, 0), (near, 0, 1), (far, 0, 2), (far, 1, 3)):
        here = pl.multiple_of(lax.bitwise_xor(me, d) * TILE, TILE)
        for f in range(3):
            start = (3 * at + f) * TILE
            outs[f][pl.ds(here, TILE), :] = piece[start : start + TILE, :]
    outs[3][...] = jnp.sum(traces[...], axis=0)


def fast_shards(
    coarse_ez, coarse_hx, coarse_hy, coarse_ids, mat_eps, mat_sig,
    fine_ez, fine_hx, fine_hy, fine_ids, boxes, src_cells, src_wave, rcv_cells,
):
    owners = lax.axis_size("gx")
    every = ("grp", "gx", "gy")
    rows, cols = coarse_ez.shape
    all_cols = cols * lax.axis_size(COLS)
    fine_shape = fine_ez.shape
    count = fine_shape[0] * fine_shape[2]
    cells = fine_shape[-1]
    flat = [x.reshape(count, cells) for x in (fine_ez, fine_hx, fine_hy, fine_ids)]
    corners = boxes.reshape(boxes.shape[2:]).T
    block = pltpu.VMEM((rows, cols), F32)
    messages = call(
        functools.partial(pack_kernel, owners),
        tuple(f32(MESSAGE, cols) for _ in range(owners)),
        (coarse_ez, coarse_hx, coarse_hy, coarse_ids, corners),
        [block] * 3
        + [pltpu.VMEM((rows, cols), I32), pltpu.VMEM(corners.shape, I32)]
        + [pltpu.SemaphoreType.DMA((5,))],
        far=range(5),
    )
    received = [messages[0]] + [ring(messages[d], "gx", d) for d in range(1, owners)]
    planes = kept(PLANES, 2 * count, LANES)
    kinds = mat_eps.shape[0]
    *fields, fdamp, fgain, coarse_kinds = call(
        spread_kernel,
        (planes,) * 5 + (kept(2 * kinds, LANES),),
        (*flat, mat_eps, mat_sig),
        [pltpu.VMEM((count, cells), F32)] * 3
        + [pltpu.VMEM((count, cells), I32)]
        + [pltpu.SMEM((kinds,), F32)] * 2
        + [pltpu.VMEM((2 * kinds, LANES), F32), pltpu.VMEM((4, 3, 3, 2 * count, LANES), F32)]
        + [pltpu.SemaphoreType.DMA((6,))],
        far=range(6),
        flops=1 << 31,
    )
    edges, windows, lines = call(
        functools.partial(edges_kernel, owners),
        (f32(WINDOW, LANES), kept(5, owners, WINDOW, LANES), kept(owners, 8, LANES)),
        (*received, coarse_kinds),
        [pltpu.VMEM((owners, MESSAGE, LANES), F32)],
    )
    from_left = ring(edges, COLS, 1)
    from_right = ring(edges, COLS, -1)
    receivers = rcv_cells.shape[0]
    window = (owners, WINDOW, WIDE)
    tiles = kept(2 * count, LANES)
    ready = call(
        functools.partial(ready_kernel, owners, all_cols),
        (planes, planes, tiles, tiles, kept(2 * owners, *window[1:]), kept(STEPS, *window))
        + (kept(3 * owners * TILE, receivers, dtype=BF16), kept(LANES, receivers)),
        (windows, lines, fdamp, fgain, src_cells, src_wave, rcv_cells.reshape(1, receivers)),
        [pltpu.SMEM(src_cells.shape, I32), pltpu.SMEM(src_wave.shape, F32)]
        + [pltpu.VMEM((1, receivers), I32), pltpu.SemaphoreType.DMA((3,))],
        far=(4, 5, 6),
        flops=1 << 30,
    )
    *results, traces = call(
        functools.partial(step_kernel, owners),
        (planes,) * 3
        + (f32(3 * TILE, LANES), f32(6 * TILE, LANES), f32(3 * TILE, LANES))
        + (f32(lax.axis_size(every), STEPS, receivers),),
        (windows, from_left, from_right, *fields, *ready),
        [pltpu.VMEM(window, F32)] * 6
        + [pltpu.VMEM(tiles.shape, F32), pltpu.VMEM((3, *tiles.shape), F32)]
        + [pltpu.VMEM((8, receivers), F32)]
        + [pltpu.VMEM((lax.axis_size(every), STEPS, receivers), F32), pltpu.SemaphoreType.DMA],
        far_outs=(6,),
        aliases={3: 0, 4: 1, 5: 2},
        flops=1 << 30,
    )
    fine, back = results[:3], results[3:]
    traces = lax.all_to_all(traces, every, 0, 0)
    near = swapped(back[1], "gx", 1)
    far = swapped(jnp.concatenate([back[2], near[3 * TILE :]]), "gx", 2)
    pieces = (back[0], near, far)
    finals = call(
        gather_kernel,
        (f32(count, cells),) * 3,
        (*fine, ready[3]),
        [pltpu.VMEM((3, count, cells), F32)]
        + [pltpu.VMEM((3, 3, 3, 2 * count, LANES), F32)] * 2
        + [pltpu.SemaphoreType.DMA((3,))],
        far_outs=range(3),
        flops=1 << 31,
    )
    ends = call(
        place_kernel,
        (f32(rows, cols),) * 3 + (f32(STEPS, receivers),),
        (*pieces, traces),
    )
    return (*ends[:3], *(x.reshape(fine_shape) for x in finals), ends[3])


def passed_along(value, axis, steps):
    count = lax.axis_size(axis)
    initial, last = (max(0, -steps), min(count, count - steps))
    return lax.ppermute(value, axis, [(source, source + steps) for source in range(initial, last)])


def coefficients(ids, eps_table, sig_table, ratio):
    damp = jnp.zeros(ids.shape, jnp.float32)
    gain = jnp.zeros(ids.shape, jnp.float32)
    for material in range(eps_table.shape[0]):
        loss = sig_table[material] / (eps_table[material] * ratio)
        hit = ids == material
        damp = jnp.where(hit, (1.0 - loss) / (1.0 + loss), damp)
        gain = jnp.where(hit, COURANT / (eps_table[material] * (1.0 + loss)), gain)
    return (damp, gain)


def box_masks(boxes, cells, scale):
    coarse_of = jnp.arange(cells, dtype=jnp.int32) // scale
    low_i = boxes[..., 0:1]
    low_j = boxes[..., 1:2]
    high_i = low_i + boxes[..., 2:3]
    high_j = low_j + boxes[..., 3:4]
    rows_in = (coarse_of >= low_i) & (coarse_of < high_i)
    cols_in = (coarse_of >= low_j) & (coarse_of < high_j)
    rows_mid = (coarse_of > low_i) & (coarse_of < high_i - 1)
    cols_mid = (coarse_of > low_j) & (coarse_of < high_j - 1)
    inbox = rows_in[..., :, None] & cols_in[..., None, :]
    middle = rows_mid[..., :, None] & cols_mid[..., None, :]
    return (inbox, middle)


def flat_masks(boxes):
    width = TILE * 3
    index = jnp.arange(width * width, dtype=jnp.int32)
    coarse_i = index // width // 3
    coarse_j = index % width // 3
    low_i = boxes[:, 0:1]
    low_j = boxes[:, 1:2]
    high_i = low_i + boxes[:, 2:3]
    high_j = low_j + boxes[:, 3:4]
    inbox = (coarse_i >= low_i) & (coarse_i < high_i) & (coarse_j >= low_j) & (coarse_j < high_j)
    middle = (
        (coarse_i > low_i) & (coarse_i < high_i - 1) & (coarse_j > low_j) & (coarse_j < high_j - 1)
    )
    return (inbox, middle)


def spread_table():
    width = TILE * 3
    index = jnp.arange(width * width, dtype=jnp.int32)
    owner = index // width // 3 * TILE + index % width // 3
    return (jnp.arange(TILE * TILE, dtype=jnp.int32)[:, None] == owner[None, :]).astype(jnp.float32)


def to_flat_tiles(field):
    rows, cols = field.shape
    along_x = rows // TILE
    along_y = cols // TILE
    shaped = field.reshape(along_x, TILE, along_y, TILE).transpose(0, 2, 1, 3)
    return shaped.reshape(1, 1, along_x * along_y, TILE * TILE)


def from_tiles(tiles, block_rows, block_cols):
    along_x = block_rows // TILE
    along_y = block_cols // TILE
    shaped = tiles.reshape(along_x, along_y, TILE, TILE).transpose(0, 2, 1, 3)
    return shaped.reshape(block_rows, block_cols)


def pad_last(array, before, after):
    widths = [(0, 0)] * (array.ndim - 1) + [(before, after)]
    return jnp.pad(array, widths)


def fine_substep(fine_ez, fine_hx, fine_hy, damp, gain, inbox, middle, border, cycle_value):
    width = TILE * 3
    column = jnp.arange(width * width, dtype=jnp.int32) % width
    ez_next_col = jnp.where(column < width - 1, pad_last(fine_ez[..., 1:], 0, 1), 0.0)
    ez_next_row = pad_last(fine_ez[..., width:], 0, width)
    fine_hx = jnp.where(inbox, fine_hx - HCOEF * (ez_next_col - fine_ez), 0.0)
    fine_hy = jnp.where(inbox, fine_hy + HCOEF * (ez_next_row - fine_ez), 0.0)
    hy_prev = pad_last(fine_hy[..., :-width], width, 0)
    hx_prev = jnp.where(column > 0, pad_last(fine_hx[..., :-1], 1, 0), 0.0)
    curl = fine_hy - hy_prev - (fine_hx - hx_prev)
    inner = damp * fine_ez + gain * curl
    fine_ez = jnp.where(middle, inner, jnp.where(border, cycle_value, 0.0))
    return (fine_ez, fine_hx, fine_hy)


def fine_round(
    fine_ez, fine_hx, fine_hy, damp, gain, inbox, middle, border, old_tiles, new_tiles, spread
):
    for sub in range(1, 4):
        weight = sub / 3.0
        mixed = (1.0 - weight) * old_tiles + weight * new_tiles
        cycle_value = jnp.dot(
            mixed, spread, precision=lax.Precision.HIGHEST, preferred_element_type=jnp.float32
        )
        fine_ez, fine_hx, fine_hy = fine_substep(
            fine_ez, fine_hx, fine_hy, damp, gain, inbox, middle, border, cycle_value
        )
    return (fine_ez, fine_hx, fine_hy)


def coarse_magnetic(ez, hx, hy):
    below = passed_along(ez[:1, :], "gx", -1)
    beside = passed_along(ez[:, :1], ("grp", "gy"), -1)
    ez_next_row = jnp.concatenate([ez[1:, :], below], axis=0)
    ez_next_col = jnp.concatenate([ez[:, 1:], beside], axis=1)
    hx = hx - HCOEF * (ez_next_col - ez)
    hy = hy + HCOEF * (ez_next_row - ez)
    above = passed_along(hy[-1:, :], "gx", 1)
    before = passed_along(hx[:, -1:], ("grp", "gy"), 1)
    hy_prev = jnp.concatenate([above, hy[:-1, :]], axis=0)
    hx_prev = jnp.concatenate([before, hx[:, :-1]], axis=1)
    curl = hy - hy_prev - (hx - hx_prev)
    return (hx, hy, curl)


def shards(
    coarse_ez,
    coarse_hx,
    coarse_hy,
    coarse_ids,
    mat_eps,
    mat_sig,
    fine_ez,
    fine_hx,
    fine_hy,
    fine_ids,
    boxes,
    src_cells,
    src_wave,
    rcv_cells,
):
    rows, cols = coarse_ez.shape
    fine_shape = fine_ez.shape
    flat_cells = fine_shape[-1]
    means_shape = fine_shape[:-1] + (TILE * TILE,)
    row_start = lax.axis_index("gx") * rows
    col_start = lax.axis_index(("grp", "gy")) * cols
    all_cols = cols * lax.axis_size(("grp", "gy"))
    spread = spread_table()
    damp, gain = coefficients(coarse_ids, mat_eps, mat_sig, 1.0)
    fine_damp, fine_gain = coefficients(fine_ids.reshape(-1, flat_cells), mat_eps, mat_sig, 3.0)
    owned_boxes = lax.all_to_all(boxes, "gx", split_axis=2, concat_axis=0, tiled=True).reshape(
        -1, 4
    )
    inbox, middle = flat_masks(owned_boxes)
    border = inbox & jnp.logical_not(middle)
    coarse_mid = from_tiles(box_masks(boxes, TILE, 1)[1], rows, cols)
    src_rows = (
        jnp.arange(rows, dtype=jnp.int32)[None, :] == (src_cells // all_cols - row_start)[:, None]
    ).astype(jnp.float32)
    src_cols = (
        jnp.arange(cols, dtype=jnp.int32)[None, :] == (src_cells % all_cols - col_start)[:, None]
    ).astype(jnp.float32)
    rcv_rows = (
        jnp.arange(rows, dtype=jnp.int32)[None, :] == (rcv_cells // all_cols - row_start)[:, None]
    ).astype(jnp.float32)
    rcv_cols = (
        jnp.arange(cols, dtype=jnp.int32)[None, :] == (rcv_cells % all_cols - col_start)[:, None]
    ).astype(jnp.float32)
    ez, hx, hy = (coarse_ez, coarse_hx, coarse_hy)
    field_ez = fine_ez.reshape(-1, flat_cells)
    field_hx = fine_hx.reshape(-1, flat_cells)
    field_hy = fine_hy.reshape(-1, flat_cells)
    held = lax.all_to_all(to_flat_tiles(ez), "gx", split_axis=2, concat_axis=0, tiled=True).reshape(
        -1, TILE * TILE
    )
    samples = []
    for step in range(STEPS):
        hx, hy, curl = coarse_magnetic(ez, hx, hy)
        weighted = src_rows * src_wave[step][:, None]
        drive = jnp.dot(
            weighted.T,
            src_cols,
            precision=lax.Precision.HIGHEST,
            preferred_element_type=jnp.float32,
        )
        new = damp * ez + gain * curl + drive
        old_tiles = held
        new_tiles = lax.all_to_all(
            to_flat_tiles(new), "gx", split_axis=2, concat_axis=0, tiled=True
        ).reshape(-1, TILE * TILE)
        held = new_tiles
        field_ez, field_hx, field_hy = fine_round(
            field_ez,
            field_hx,
            field_hy,
            fine_damp,
            fine_gain,
            inbox,
            middle,
            border,
            old_tiles,
            new_tiles,
            spread,
        )
        sums = lax.dot_general(
            field_ez,
            spread,
            (((1,), (1,)), ((), ())),
            precision=lax.Precision.HIGHEST,
            preferred_element_type=jnp.float32,
        )
        means = (sums / 9.0).reshape(means_shape)
        back = lax.all_to_all(means, "gx", split_axis=0, concat_axis=2, tiled=True)
        ez = jnp.where(coarse_mid, from_tiles(back, rows, cols), new)
        picked = jnp.dot(
            rcv_rows, ez, precision=lax.Precision.HIGHEST, preferred_element_type=jnp.float32
        )
        samples.append(jnp.sum(picked * rcv_cols, axis=1))
    traces = lax.psum(jnp.stack(samples), ("grp", "gx", "gy"))
    return (
        ez,
        hx,
        hy,
        field_ez.reshape(fine_shape),
        field_hx.reshape(fine_shape),
        field_hy.reshape(fine_shape),
        traces,
    )


def solution(mesh):
    placed = (
        P("gx", ("grp", "gy")),
        P("gx", ("grp", "gy")),
        P("gx", ("grp", "gy")),
        P("gx", ("grp", "gy")),
        P(),
        P(),
        P(None, ("grp", "gy"), "gx", None),
        P(None, ("grp", "gy"), "gx", None),
        P(None, ("grp", "gy"), "gx", None),
        P(None, ("grp", "gy"), "gx", None),
        P("gx", ("grp", "gy"), None, None),
        P(),
        P(),
        P(),
    )
    def body(*args):
        rows, cols = args[0].shape
        owners = lax.axis_size("gx")
        strips = cols == LANES and args[6].shape[2] * TILE == cols and rows == owners * TILE
        if strips and owners == 4 and 5 * GROUP * owners <= LANES and args[13].shape[0] == LANES:
            return fast_shards(*args)
        return shards(*args)

    return jax.shard_map(
        body,
        mesh=mesh,
        in_specs=placed,
        out_specs=(
            P("gx", ("grp", "gy")),
            P("gx", ("grp", "gy")),
            P("gx", ("grp", "gy")),
            P(None, ("grp", "gy"), "gx", None),
            P(None, ("grp", "gy"), "gx", None),
            P(None, ("grp", "gy"), "gx", None),
            P(),
        ),
        check_vma=False,
    )
```

```python
import functools

import jax
import jax.numpy as jnp
from jax import lax
from jax.experimental import pallas as pl
from jax.experimental.pallas import tpu as pltpu
from jax.sharding import PartitionSpec as P

TILE = 16
STEPS = 3
SUBSTEPS = 3
LANES = 128
FIELDS = 4
WINDOW = 24
HALO = FIELDS * TILE
MESSAGE = HALO + 24
PLANES = 9
WIDE = 2 * LANES
GROUP = 6

COURANT = 0.5
HCOEF = 0.5
F32 = jnp.float32
BF16 = jnp.bfloat16
I32 = jnp.int32
COLS = ("grp", "gy")


def iota(shape, axis):
    return lax.broadcasted_iota(I32, shape, axis)


def f32(*shape):
    return jax.ShapeDtypeStruct(shape, F32)


def kept(*shape, dtype=F32):
    return pltpu.VMEM(shape, dtype)


def call(kernel, outs, args, scratch=(), far=(), far_outs=(), aliases=None, flops=1 << 20):
    vmem, hbm = (pl.BlockSpec(memory_space=m) for m in (pltpu.VMEM, pltpu.HBM))
    args = [
        pltpu.with_memory_space_constraint(x, pltpu.HBM)
        if k in far
        else x
        for k, x in enumerate(args)
    ]
    return pl.pallas_call(
        kernel,
        out_shape=outs,
        in_specs=[hbm if k in far else vmem for k in range(len(args))],
        out_specs=tuple(hbm if k in far_outs else vmem for k in range(len(outs))),
        scratch_shapes=list(scratch),
        input_output_aliases=aliases or {},
        compiler_params=pltpu.CompilerParams(vmem_limit_bytes=16 * 1024 * 1024),
        cost_estimate=pl.CostEstimate(flops=flops, bytes_accessed=1 << 20, transcendentals=0),
    )(*args)


def copies(sources, targets, sems):
    moves = [
        pltpu.make_async_copy(source, target, sems.at[k])
        for k, (source, target) in enumerate(zip(sources, targets))
    ]
    for move in moves:
        move.start()
    return moves


def ring(value, axis, steps):
    count = lax.axis_size(axis)
    return lax.ppermute(value, axis, [(k, (k + steps) % count) for k in range(count)])


def pack_kernel(owners, *refs):
    sources, outs = refs[:5], refs[5 : 5 + owners]
    held, sems = refs[5 + owners : 10 + owners], refs[10 + owners]
    for move in copies(sources, held, sems):
        move.wait()
    ez, hx, hy, ids, boxes = held
    me = lax.axis_index("gx")
    tiles = ez.shape[0] // 8
    count = boxes.shape[1]
    sub = iota((8, LANES), 0)
    lines = jnp.concatenate([boxes[...].astype(F32), jnp.zeros((4, LANES - count), F32)], axis=1)
    low, high, left, top = (jnp.broadcast_to(lines[k : k + 1, :], (8, LANES)) for k in range(4))
    for d in range(owners):
        g = lax.rem(me + d, owners)
        here = pl.multiple_of(g * TILE, TILE)
        after = pl.multiple_of(lax.rem(2 * g + 2, tiles) * 8, 8)
        before = pl.multiple_of(lax.rem(2 * g + tiles - 1, tiles) * 8, 8)
        edges = []
        for f, ref in enumerate((ez, hx, hy, ids)):
            outs[d][f * TILE : (f + 1) * TILE, :] = ref[pl.ds(here, TILE), :].astype(F32)
            edge = jnp.where(sub < 4, ref[pl.ds(after, 8), :], ref[pl.ds(before, 8), :])
            edges.append(edge.astype(F32))
        around_ez, around_hx, around_hy, around_ids = edges
        outs[d][HALO : HALO + 8, :] = jnp.where(sub == 3, low, jnp.where(sub == 4, high, around_ez))
        inner = jnp.where(sub < 4, pltpu.roll(around_ids, 2, 0), pltpu.roll(around_ids, 6, 0))
        outs[d][HALO + 8 : HALO + 16, :] = jnp.where((sub >= 2) & (sub < 6), inner, around_hx)
        outs[d][HALO + 16 : HALO + 24, :] = jnp.where(
            sub == 2, left, jnp.where(sub == 3, top, around_hy)
        )


def block_of(owners, d):
    return lax.rem(lax.axis_index("gx") + owners - d, owners)


def edges_kernel(owners, *refs):
    received, table = refs[:owners], refs[owners]
    out, windows, boxes, store = refs[owners + 1 :]
    me = lax.axis_index("gx")
    sub = iota((8, LANES), 0)
    for d in range(owners):
        store[block_of(owners, d)] = received[d][...]
    around = [
        [store[a, HALO + 8 * k : HALO + 8 * k + 8, :] for a in range(owners)] for k in range(3)
    ]
    row = iota((WINDOW, LANES), 0)
    row = jnp.where(row < 20, row, row - WINDOW)
    lane = iota((WINDOW, LANES), 1)
    total = jnp.zeros((WINDOW, LANES), F32)
    for a in range(owners):
        for k, at in enumerate((3, 4, 18, 19)):
            boxes[a, k : k + 1, :] = store[a, HALO + at : HALO + at + 1, :]
        tiles = []
        for tile in around:
            after = jnp.where(me == owners - 1, tile[min(a + 1, owners - 1)], tile[a])
            before = jnp.where(me == 0, tile[max(a - 1, 0)], tile[a])
            tiles.append(jnp.where(sub < 4, after, before))
        inner = jnp.where(sub < 4, pltpu.roll(tiles[1], 6, 0), pltpu.roll(tiles[1], 2, 0))
        fields = [
            jnp.concatenate([store[a, f * TILE : (f + 1) * TILE, :], tile], axis=0)
            for f, tile in enumerate((*tiles, inner))
        ]
        all_row = row + (a * owners * TILE + me * TILE)
        valid = (all_row >= 0) & (all_row < owners * owners * TILE)
        damp = jnp.zeros((WINDOW, LANES), F32)
        gain = jnp.zeros((WINDOW, LANES), F32)
        kinds = table.shape[0] // 2
        for m in range(kinds):
            hit = fields[3] == float(m)
            damp = jnp.where(hit, table[m : m + 1, :], damp)
            gain = jnp.where(hit, table[kinds + m : kinds + m + 1, :], gain)
        for f, value in enumerate((*fields[:3], damp, gain)):
            value = jnp.where(valid, value, 0.0)
            windows[f, a] = value
            at = GROUP * (f * owners + a)
            total = jnp.where((lane >= at) & (lane < at + GROUP), pltpu.roll(value, at + 3, 1), total)
    out[...] = total


def lane_of():
    return iota((8, LANES), 1)


def third_of(x, start):
    return lax.rem(x + start, 3)


def choose(parts, which):
    return jnp.where(which == 0, parts[0], jnp.where(which == 1, parts[1], parts[2]))


def take(x, lanes):
    return jnp.take_along_axis(x, lanes & (LANES - 1), axis=1)


def in_block(block):
    return ((block & 7) << 4) | (lane_of() & 15)


def halves(x):
    high = x.astype(BF16)
    return high, (x - high.astype(F32)).astype(BF16)


def thirds(x):
    high = x.astype(BF16)
    rest = x - high.astype(F32)
    return high, *halves(rest)


def lists(eps, sig, ratio):
    ones = jnp.ones((1, LANES), F32)
    both = []
    for m in range(eps.shape[0]):
        e, s = ones * eps[m], ones * sig[m]
        loss = s / (e * ratio)
        both.append(((1.0 - loss) / (1.0 + loss), COURANT / (e * (1.0 + loss))))
    return both


def turn(x, first, last):
    block = lane_of() >> 4
    sub = iota((8, LANES), 0)
    x = jnp.take_along_axis(x, first(sub, block) & 7, axis=0)
    x = pltpu.roll(x, 0, 1, stride=TILE, stride_axis=0)
    return jnp.take_along_axis(x, last(sub, block) & 7, axis=0)


def each_half(owners):
    for a in range(owners):
        for h in range(2):
            yield a, h, slice(8 * a, 8 * a + 8), slice(TILE * a + 8 * h, TILE * a + 8 * h + 8)


def spread_kernel(*refs):
    sources, (oez, ohx, ohy, odamp, ogain, coarse_kinds) = refs[:6], refs[6:12]
    held, (kinds, rows, sems) = refs[12:18], refs[18:]
    fez, fhx, fhy, ids, eps, sig = held
    moves = copies(sources, held, sems)
    half = eps.shape[0]
    for move in moves[4:]:
        move.wait()
    for ref, ratio, scale in ((coarse_kinds, 1.0, 1.0), (kinds, 3.0, 0.5)):
        for m, (damp, gain) in enumerate(lists(eps, sig, ratio)):
            ref[m : m + 1, :] = damp
            ref[half + m : half + m + 1, :] = scale * gain
    for move in moves[:4]:
        move.wait()
    owners = fez.shape[0] // 8
    lane, block = lane_of(), lane_of() >> 4
    for v in range(3):
        for a, h, tiles, at in each_half(owners):
            for f, ref in enumerate((fez, fhx, fhy, ids)):
                for r in range(3):
                    first = 9 * h + 3 * r
                    parts = [ref[tiles, k * LANES : (k + 1) * LANES] for k in range(first, first + 3)]
                    part = choose(parts, third_of(lane, 2 * v)).astype(F32)
                    rows[f, v, r, at] = take(part, 3 * lane + v)
    for u in range(3):
        for a, h, tiles, at in each_half(owners):
            for f in (3, 0, 1, 2):
                for v in range(3):
                    part = choose([rows[f, v, r, at] for r in range(3)], third_of(block, 2 * u))
                    value = turn(part, lambda r, b: r + b, lambda i, c: c - 3 * i - u)
                    if f == 0:
                        oez[3 * u + v, at] = value
                    elif f < 3:
                        (ohx, ohy)[f - 1][3 * u + v, at] = 2.0 * value
                    else:
                        damp = jnp.zeros((8, LANES), F32)
                        gain = jnp.zeros((8, LANES), F32)
                        for m in range(half):
                            hit = value == float(m)
                            damp = jnp.where(hit, kinds[m : m + 1, :], damp)
                            gain = jnp.where(hit, kinds[half + m : half + m + 1, :], gain)
                        odamp[3 * u + v, at] = damp
                        ogain[3 * u + v, at] = gain


def gather_kernel(ez, hx, hy, box, *refs):
    outs, (flat, rows, cells, sems) = refs[:3], refs[3:]
    owners = ez.shape[1] // TILE
    lane, block = lane_of(), lane_of() >> 4
    for u in range(3):
        for a, h, tiles, at in each_half(owners):
            for f, ref in enumerate((ez, hx, hy)):
                for v in range(3):
                    part = ref[3 * u + v, at]
                    part = part if f == 0 else 0.5 * (part * box[at])
                    rows[f, v, u, at] = turn(
                        part, lambda r, b: 3 * (b + r - u), lambda c, b: b - c
                    )
    for v in range(3):
        for a, h, tiles, at in each_half(owners):
            for f in range(3):
                parts = [rows[f, v, u, at] for u in range(3)]
                for r in range(3):
                    part = choose(parts, third_of(block, 2 * r))
                    cells[f, r, v, at] = take(part, 43 * (lane - v))
    moves = []
    for f in range(3):
        for a, h, tiles, at in each_half(owners):
            for r in range(3):
                parts = [cells[f, r, v, at] for v in range(3)]
                for k in range(3):
                    place = 9 * h + 3 * r + k
                    value = choose(parts, third_of(lane, 2 * k))
                    flat[f, tiles, place * LANES : (place + 1) * LANES] = value
        moves.append(pltpu.make_async_copy(flat.at[f], outs[f], sems.at[f]))
        moves[-1].start()
    for move in moves:
        move.wait()


def column_of():
    return lax.axis_index("grp") * lax.axis_size("gy") + lax.axis_index("gy")


def ready_kernel(owners, all_cols, *refs):
    windows, boxes, fdamp, fgain, far_src, far_wave, far_rcv = refs[:7]
    mdamp, mgain, mid, box, half, drive, row_hit, col_hit = refs[7:15]
    src, wave, rcv, sems = refs[15:]
    moves = copies((far_src, far_wave, far_rcv), (src, wave, rcv), sems)
    me = lax.axis_index("gx")
    column = column_of()
    rows = owners * TILE
    lane = lane_of()
    tile_col = (lane & 15).astype(F32)
    for a in range(owners):
        low_i, low_j, size_i, size_j = (
            take(jnp.broadcast_to(boxes[a, k : k + 1, :], (8, LANES)), 8 * me + (lane >> 4))
            for k in range(4)
        )
        high_i, high_j = low_i + size_i, low_j + size_j
        for h in range(2):
            i = (8 * h + iota((8, LANES), 0)).astype(F32)
            inside = (i >= low_i) & (i < high_i) & (tile_col >= low_j) & (tile_col < high_j)
            middle = (i > low_i) & (i < high_i - 1) & (tile_col > low_j) & (tile_col < high_j - 1)
            at = slice(TILE * a + 8 * h, TILE * a + 8 * h + 8)
            mid[at] = jnp.where(middle, 1.0, 0.0)
            box[at] = jnp.where(inside, 1.0, 0.0)
    for p in range(PLANES):
        mdamp[p] = fdamp[p] * mid[...]
        mgain[p] = fgain[p] * mid[...]
    for move in moves:
        move.wait()
    receivers = rcv[...]
    at_row = lax.div(receivers, all_cols)
    image = lax.rem(iota((3 * rows, LANES), 0), rows)
    image_row = (image >> 4) * rows + me * TILE + (image & 15)
    row_hit[...] = jnp.where(image_row == at_row, 1.0, 0.0).astype(BF16)
    at_col = receivers - at_row * all_cols - column * LANES
    col_hit[...] = jnp.where(iota((LANES, LANES), 0) == at_col, 1.0, 0.0)
    row = iota((WINDOW, WIDE), 0)
    row = jnp.where(row < 20, row, row - WINDOW)
    col = iota((WINDOW, WIDE), 1)
    col = jnp.where(col < LANES + 64, col, col - WIDE)
    all_col = col + column * LANES
    for a in range(owners):
        all_row = row + (a * rows + me * TILE)
        valid = (all_row >= 0) & (all_row < owners * rows) & (all_col >= 0) & (all_col < all_cols)
        cells = jnp.where(valid, all_row * all_cols + all_col, -1)
        half[a] = jnp.where(valid, HCOEF, 0.0)
        half[owners + a] = jnp.where(valid & (all_col > 0), HCOEF, 0.0)
        for n in range(STEPS):
            total = jnp.zeros((WINDOW, WIDE), F32)
            for k in range(src.shape[0]):
                total = total + jnp.where(cells == src[k], wave[n, k], 0.0)
            drive[n, a] = total


def step_kernel(owners, *refs):
    windows, from_left, from_right = refs[:3]
    mdamp, mgain, mid, box, half, drive, row_hit, col_hit = refs[6:14]
    oez, ohx, ohy = refs[14:17]
    back, far_traces = refs[17 : 16 + owners], refs[16 + owners]
    ez, hx, hy, behind, damp, gain, held, beside, picked, traces, sem = refs[17 + owners :]
    column = column_of()
    place = lax.rem(iota((WINDOW, LANES), 1), GROUP)
    right = jnp.where(column == lax.axis_size(COLS) - 1, 0.0, from_right[...])
    left = jnp.where(column == 0, 0.0, from_left[...])
    sides = jnp.where(place < 3, left, right)
    for f, ref in enumerate((ez, hx, hy, damp, gain)):
        for a in range(owners):
            at = GROUP * (f * owners + a)
            ref[a, :, 0:LANES] = windows[f, a]
            ref[a, :, LANES:WIDE] = pltpu.roll(sides, (LANES - 3 - at) % LANES, 1)
    for a in range(owners):
        behind[a] = pltpu.roll(hx[a], 1, 1)
    for u in range(3):
        for k in range(2 * owners):
            at = slice(8 * k, 8 * k + 8)
            beside[u, at] = pltpu.roll(ohx[3 * u + 2, at], 1, 1)
    sub = iota((8, LANES), 0)
    places = [(u, v, h) for u in range(3) for v in range(3) for h in range(2)]

    def substep(m, carry):
        weight = (m + 1) / SUBSTEPS
        for a in range(owners):
            at = [slice(TILE * a + 8 * h, TILE * a + 8 * h + 8) for h in range(2)]
            e = {(u, v, h): oez[3 * u + v, at[h]] for u, v, h in places}
            ahead = {(u, h): pltpu.roll(e[u, 0, h], LANES - 1, 1) for u in range(3) for h in range(2)}
            back_e = {(u, h): pltpu.roll(e[u, 2, h], 1, 1) for u in range(3) for h in range(2)}
            down = {(v, h): pltpu.roll(e[0, v, h], 7, 0) for v in range(3) for h in range(2)}
            y = {}
            for u, v, h in places:
                p = 3 * u + v
                if u < 2:
                    below = e[u + 1, v, h]
                elif h == 0:
                    below = jnp.where(sub < 7, down[v, 0], down[v, 1])
                else:
                    below = down[v, 1]
                y[u, v, h] = ohy[p, at[h]] + (below - e[u, v, h])
                ohy[p, at[h]] = y[u, v, h]
            up = {(v, h): pltpu.roll(y[2, v, h], 1, 0) for v in range(3) for h in range(2)}
            for v in range(3):
                up[v, 1] = jnp.where(sub < 1, up[v, 0], up[v, 1])
            for h in range(2):
                now = ez[a, 8 * h : 8 * h + 8, 0:LANES]
                cyc = (box[at[h]] - mid[at[h]]) * ((1.0 - weight) * held[at[h]] + weight * now)
                for u in range(3):
                    before = beside[u, at[h]] - (e[u, 0, h] - back_e[u, h])
                    beside[u, at[h]] = before
                    for v in range(3):
                        p = 3 * u + v
                        after = e[u, v + 1, h] if v < 2 else ahead[u, h]
                        x = ohx[p, at[h]] - (after - e[u, v, h])
                        ohx[p, at[h]] = x
                        above = y[u - 1, v, h] if u > 0 else up[v, h]
                        curl = (y[u, v, h] - above) - (x - before)
                        inner = mdamp[p, at[h]] * e[u, v, h] + mgain[p, at[h]] * curl
                        oez[p, at[h]] = inner + cyc
                        before = x
        return carry

    def pick(n):
        image = jnp.concatenate([ez[a, 0:TILE, 0:LANES] for a in range(owners)], axis=0)
        mixed = lax.dot_general(
            jnp.concatenate(thirds(image), axis=0),
            row_hit[...],
            (((0,), (0,)), ((), ())),
            preferred_element_type=F32,
        )
        picked[n : n + 1, :] = jnp.sum(mixed * col_hit[...], axis=0, keepdims=True)

    def step(n, carry):
        if n > 0:
            pick(n - 1)
        for a in range(owners):
            e = ez[a]
            held[TILE * a : TILE * a + TILE] = e[0:TILE, 0:LANES]
            scale = half[a]
            x = hx[a] - scale * (pltpu.roll(e, WIDE - 1, 1) - e)
            before = behind[a] - half[owners + a] * (e - pltpu.roll(e, 1, 1))
            y = hy[a] + scale * (pltpu.roll(e, WINDOW - 1, 0) - e)
            hx[a], hy[a], behind[a] = x, y, before
            curl = (y - pltpu.roll(y, 1, 0)) - (x - before)
            ez[a] = damp[a] * e + gain[a] * curl + drive[n, a]
        for m in range(SUBSTEPS):
            substep(m, 0)
        for a in range(owners):
            for h in range(2):
                at = slice(TILE * a + 8 * h, TILE * a + 8 * h + 8)
                total = oez[0, at]
                for p in range(1, PLANES):
                    total = total + oez[p, at]
                here = (a, slice(8 * h, 8 * h + 8), slice(0, LANES))
                ez[here] = jnp.where(mid[at] > 0.0, total * (1.0 / PLANES), ez[here])
        return carry

    picked[...] = jnp.zeros(picked.shape, F32)
    for n in range(STEPS):
        step(n, 0)
    pick(STEPS - 1)
    for k in range(traces.shape[0]):
        traces[k] = picked[0:STEPS, :]
    move = pltpu.make_async_copy(traces, far_traces, sem)
    move.start()
    me = lax.axis_index("gx")
    for (out, at), d in zip(((0, 0), (1, 0), (1, 1), (2, 0)), (0, 1, 3, 2)):
        a = lax.bitwise_xor(me, d)
        for f, ref in enumerate((ez, hx, hy)):
            start = (3 * at + f) * TILE
            back[out][start : start + TILE, :] = ref[a, 0:TILE, 0:LANES]
    move.wait()


def swapped(value, axis, bit):
    return lax.ppermute(value, axis, [(k, k ^ bit) for k in range(lax.axis_size(axis))])


def place_kernel(own, near, far, traces, *outs):
    me = lax.axis_index("gx")
    for piece, at, d in ((own, 0, 0), (near, 0, 1), (far, 0, 2), (far, 1, 3)):
        here = pl.multiple_of(lax.bitwise_xor(me, d) * TILE, TILE)
        for f in range(3):
            start = (3 * at + f) * TILE
            outs[f][pl.ds(here, TILE), :] = piece[start : start + TILE, :]
    outs[3][...] = jnp.sum(traces[...], axis=0)


def fast_shards(
    coarse_ez, coarse_hx, coarse_hy, coarse_ids, mat_eps, mat_sig,
    fine_ez, fine_hx, fine_hy, fine_ids, boxes, src_cells, src_wave, rcv_cells,
):
    owners = lax.axis_size("gx")
    every = ("grp", "gy", "gx")
    rows, cols = coarse_ez.shape
    all_cols = cols * lax.axis_size(COLS)
    fine_shape = fine_ez.shape
    count = fine_shape[0] * fine_shape[2]
    cells = fine_shape[-1]
    flat = [x.reshape(count, cells) for x in (fine_ez, fine_hx, fine_hy, fine_ids)]
    corners = boxes.reshape(boxes.shape[2:]).T
    block = pltpu.VMEM((rows, cols), F32)
    messages = call(
        functools.partial(pack_kernel, owners),
        tuple(f32(MESSAGE, cols) for _ in range(owners)),
        (coarse_ez, coarse_hx, coarse_hy, coarse_ids, corners),
        [block] * 3
        + [pltpu.VMEM((rows, cols), I32), pltpu.VMEM(corners.shape, I32)]
        + [pltpu.SemaphoreType.DMA((5,))],
        far=range(5),
    )
    received = [messages[0]] + [ring(messages[d], "gx", d) for d in range(1, owners)]
    planes = kept(PLANES, 2 * count, LANES)
    kinds = mat_eps.shape[0]
    *fields, fdamp, fgain, coarse_kinds = call(
        spread_kernel,
        (planes,) * 5 + (kept(2 * kinds, LANES),),
        (*flat, mat_eps, mat_sig),
        [pltpu.VMEM((count, cells), F32)] * 3
        + [pltpu.VMEM((count, cells), I32)]
        + [pltpu.SMEM((kinds,), F32)] * 2
        + [pltpu.VMEM((2 * kinds, LANES), F32), pltpu.VMEM((4, 3, 3, 2 * count, LANES), F32)]
        + [pltpu.SemaphoreType.DMA((6,))],
        far=range(6),
        flops=1 << 31,
    )
    edges, windows, lines = call(
        functools.partial(edges_kernel, owners),
        (f32(WINDOW, LANES), kept(5, owners, WINDOW, LANES), kept(owners, 8, LANES)),
        (*received, coarse_kinds),
        [pltpu.VMEM((owners, MESSAGE, LANES), F32)],
    )
    from_left = ring(edges, COLS, 1)
    from_right = ring(edges, COLS, -1)
    receivers = rcv_cells.shape[0]
    window = (owners, WINDOW, WIDE)
    tiles = kept(2 * count, LANES)
    ready = call(
        functools.partial(ready_kernel, owners, all_cols),
        (planes, planes, tiles, tiles, kept(2 * owners, *window[1:]), kept(STEPS, *window))
        + (kept(3 * owners * TILE, receivers, dtype=BF16), kept(LANES, receivers)),
        (windows, lines, fdamp, fgain, src_cells, src_wave, rcv_cells.reshape(1, receivers)),
        [pltpu.SMEM(src_cells.shape, I32), pltpu.SMEM(src_wave.shape, F32)]
        + [pltpu.VMEM((1, receivers), I32), pltpu.SemaphoreType.DMA((3,))],
        far=(4, 5, 6),
        flops=1 << 30,
    )
    *results, traces = call(
        functools.partial(step_kernel, owners),
        (planes,) * 3
        + (f32(3 * TILE, LANES), f32(6 * TILE, LANES), f32(3 * TILE, LANES))
        + (f32(lax.axis_size(every), STEPS, receivers),),
        (windows, from_left, from_right, *fields, *ready),
        [pltpu.VMEM(window, F32)] * 6
        + [pltpu.VMEM(tiles.shape, F32), pltpu.VMEM((3, *tiles.shape), F32)]
        + [pltpu.VMEM((8, receivers), F32)]
        + [pltpu.VMEM((lax.axis_size(every), STEPS, receivers), F32), pltpu.SemaphoreType.DMA],
        far_outs=(6,),
        aliases={3: 0, 4: 1, 5: 2},
        flops=1 << 30,
    )
    fine, back = results[:3], results[3:]
    traces = lax.all_to_all(traces, every, 0, 0)
    near = swapped(back[1], "gx", 1)
    far = swapped(jnp.concatenate([back[2], near[3 * TILE :]]), "gx", 2)
    pieces = (back[0], near, far)
    finals = call(
        gather_kernel,
        (f32(count, cells),) * 3,
        (*fine, ready[3]),
        [pltpu.VMEM((3, count, cells), F32)]
        + [pltpu.VMEM((3, 3, 3, 2 * count, LANES), F32)] * 2
        + [pltpu.SemaphoreType.DMA((3,))],
        far_outs=range(3),
        flops=1 << 31,
    )
    ends = call(
        place_kernel,
        (f32(rows, cols),) * 3 + (f32(STEPS, receivers),),
        (*pieces, traces),
    )
    return (*ends[:3], *(x.reshape(fine_shape) for x in finals), ends[3])


def passed_along(value, axis, steps):
    count = lax.axis_size(axis)
    initial, last = (max(0, -steps), min(count, count - steps))
    return lax.ppermute(value, axis, [(source, source + steps) for source in range(initial, last)])


def coefficients(ids, eps_table, sig_table, ratio):
    damp = jnp.zeros(ids.shape, jnp.float32)
    gain = jnp.zeros(ids.shape, jnp.float32)
    for material in range(eps_table.shape[0]):
        loss = sig_table[material] / (eps_table[material] * ratio)
        hit = ids == material
        damp = jnp.where(hit, (1.0 - loss) / (1.0 + loss), damp)
        gain = jnp.where(hit, COURANT / (eps_table[material] * (1.0 + loss)), gain)
    return (damp, gain)


def box_masks(boxes, cells, scale):
    coarse_of = jnp.arange(cells, dtype=jnp.int32) // scale
    low_i = boxes[..., 0:1]
    low_j = boxes[..., 1:2]
    high_i = low_i + boxes[..., 2:3]
    high_j = low_j + boxes[..., 3:4]
    rows_in = (coarse_of >= low_i) & (coarse_of < high_i)
    cols_in = (coarse_of >= low_j) & (coarse_of < high_j)
    rows_mid = (coarse_of > low_i) & (coarse_of < high_i - 1)
    cols_mid = (coarse_of > low_j) & (coarse_of < high_j - 1)
    inbox = rows_in[..., :, None] & cols_in[..., None, :]
    middle = rows_mid[..., :, None] & cols_mid[..., None, :]
    return (inbox, middle)


def flat_masks(boxes):
    width = TILE * 3
    index = jnp.arange(width * width, dtype=jnp.int32)
    coarse_i = index // width // 3
    coarse_j = index % width // 3
    low_i = boxes[:, 0:1]
    low_j = boxes[:, 1:2]
    high_i = low_i + boxes[:, 2:3]
    high_j = low_j + boxes[:, 3:4]
    inbox = (coarse_i >= low_i) & (coarse_i < high_i) & (coarse_j >= low_j) & (coarse_j < high_j)
    middle = (
        (coarse_i > low_i) & (coarse_i < high_i - 1) & (coarse_j > low_j) & (coarse_j < high_j - 1)
    )
    return (inbox, middle)


def spread_table():
    width = TILE * 3
    index = jnp.arange(width * width, dtype=jnp.int32)
    owner = index // width // 3 * TILE + index % width // 3
    return (jnp.arange(TILE * TILE, dtype=jnp.int32)[:, None] == owner[None, :]).astype(jnp.float32)


def to_flat_tiles(field):
    rows, cols = field.shape
    along_x = rows // TILE
    along_y = cols // TILE
    shaped = field.reshape(along_x, TILE, along_y, TILE).transpose(0, 2, 1, 3)
    return shaped.reshape(1, 1, along_x * along_y, TILE * TILE)


def from_tiles(tiles, block_rows, block_cols):
    along_x = block_rows // TILE
    along_y = block_cols // TILE
    shaped = tiles.reshape(along_x, along_y, TILE, TILE).transpose(0, 2, 1, 3)
    return shaped.reshape(block_rows, block_cols)


def pad_last(array, before, after):
    widths = [(0, 0)] * (array.ndim - 1) + [(before, after)]
    return jnp.pad(array, widths)


def fine_substep(fine_ez, fine_hx, fine_hy, damp, gain, inbox, middle, border, cycle_value):
    width = TILE * 3
    column = jnp.arange(width * width, dtype=jnp.int32) % width
    ez_next_col = jnp.where(column < width - 1, pad_last(fine_ez[..., 1:], 0, 1), 0.0)
    ez_next_row = pad_last(fine_ez[..., width:], 0, width)
    fine_hx = jnp.where(inbox, fine_hx - HCOEF * (ez_next_col - fine_ez), 0.0)
    fine_hy = jnp.where(inbox, fine_hy + HCOEF * (ez_next_row - fine_ez), 0.0)
    hy_prev = pad_last(fine_hy[..., :-width], width, 0)
    hx_prev = jnp.where(column > 0, pad_last(fine_hx[..., :-1], 1, 0), 0.0)
    curl = fine_hy - hy_prev - (fine_hx - hx_prev)
    inner = damp * fine_ez + gain * curl
    fine_ez = jnp.where(middle, inner, jnp.where(border, cycle_value, 0.0))
    return (fine_ez, fine_hx, fine_hy)


def fine_round(
    fine_ez, fine_hx, fine_hy, damp, gain, inbox, middle, border, old_tiles, new_tiles, spread
):
    for sub in range(1, 4):
        weight = sub / 3.0
        mixed = (1.0 - weight) * old_tiles + weight * new_tiles
        cycle_value = jnp.dot(
            mixed, spread, precision=lax.Precision.HIGHEST, preferred_element_type=jnp.float32
        )
        fine_ez, fine_hx, fine_hy = fine_substep(
            fine_ez, fine_hx, fine_hy, damp, gain, inbox, middle, border, cycle_value
        )
    return (fine_ez, fine_hx, fine_hy)


def coarse_magnetic(ez, hx, hy):
    below = passed_along(ez[:1, :], "gx", -1)
    beside = passed_along(ez[:, :1], ("grp", "gy"), -1)
    ez_next_row = jnp.concatenate([ez[1:, :], below], axis=0)
    ez_next_col = jnp.concatenate([ez[:, 1:], beside], axis=1)
    hx = hx - HCOEF * (ez_next_col - ez)
    hy = hy + HCOEF * (ez_next_row - ez)
    above = passed_along(hy[-1:, :], "gx", 1)
    before = passed_along(hx[:, -1:], ("grp", "gy"), 1)
    hy_prev = jnp.concatenate([above, hy[:-1, :]], axis=0)
    hx_prev = jnp.concatenate([before, hx[:, :-1]], axis=1)
    curl = hy - hy_prev - (hx - hx_prev)
    return (hx, hy, curl)


def shards(
    coarse_ez,
    coarse_hx,
    coarse_hy,
    coarse_ids,
    mat_eps,
    mat_sig,
    fine_ez,
    fine_hx,
    fine_hy,
    fine_ids,
    boxes,
    src_cells,
    src_wave,
    rcv_cells,
):
    rows, cols = coarse_ez.shape
    fine_shape = fine_ez.shape
    flat_cells = fine_shape[-1]
    means_shape = fine_shape[:-1] + (TILE * TILE,)
    row_start = lax.axis_index("gx") * rows
    col_start = lax.axis_index(("grp", "gy")) * cols
    all_cols = cols * lax.axis_size(("grp", "gy"))
    spread = spread_table()
    damp, gain = coefficients(coarse_ids, mat_eps, mat_sig, 1.0)
    fine_damp, fine_gain = coefficients(fine_ids.reshape(-1, flat_cells), mat_eps, mat_sig, 3.0)
    owned_boxes = lax.all_to_all(boxes, "gx", split_axis=2, concat_axis=0, tiled=True).reshape(
        -1, 4
    )
    inbox, middle = flat_masks(owned_boxes)
    border = inbox & jnp.logical_not(middle)
    coarse_mid = from_tiles(box_masks(boxes, TILE, 1)[1], rows, cols)
    src_rows = (
        jnp.arange(rows, dtype=jnp.int32)[None, :] == (src_cells // all_cols - row_start)[:, None]
    ).astype(jnp.float32)
    src_cols = (
        jnp.arange(cols, dtype=jnp.int32)[None, :] == (src_cells % all_cols - col_start)[:, None]
    ).astype(jnp.float32)
    rcv_rows = (
        jnp.arange(rows, dtype=jnp.int32)[None, :] == (rcv_cells // all_cols - row_start)[:, None]
    ).astype(jnp.float32)
    rcv_cols = (
        jnp.arange(cols, dtype=jnp.int32)[None, :] == (rcv_cells % all_cols - col_start)[:, None]
    ).astype(jnp.float32)
    ez, hx, hy = (coarse_ez, coarse_hx, coarse_hy)
    field_ez = fine_ez.reshape(-1, flat_cells)
    field_hx = fine_hx.reshape(-1, flat_cells)
    field_hy = fine_hy.reshape(-1, flat_cells)
    held = lax.all_to_all(to_flat_tiles(ez), "gx", split_axis=2, concat_axis=0, tiled=True).reshape(
        -1, TILE * TILE
    )
    samples = []
    for step in range(STEPS):
        hx, hy, curl = coarse_magnetic(ez, hx, hy)
        weighted = src_rows * src_wave[step][:, None]
        drive = jnp.dot(
            weighted.T,
            src_cols,
            precision=lax.Precision.HIGHEST,
            preferred_element_type=jnp.float32,
        )
        new = damp * ez + gain * curl + drive
        old_tiles = held
        new_tiles = lax.all_to_all(
            to_flat_tiles(new), "gx", split_axis=2, concat_axis=0, tiled=True
        ).reshape(-1, TILE * TILE)
        held = new_tiles
        field_ez, field_hx, field_hy = fine_round(
            field_ez,
            field_hx,
            field_hy,
            fine_damp,
            fine_gain,
            inbox,
            middle,
            border,
            old_tiles,
            new_tiles,
            spread,
        )
        sums = lax.dot_general(
            field_ez,
            spread,
            (((1,), (1,)), ((), ())),
            precision=lax.Precision.HIGHEST,
            preferred_element_type=jnp.float32,
        )
        means = (sums / 9.0).reshape(means_shape)
        back = lax.all_to_all(means, "gx", split_axis=0, concat_axis=2, tiled=True)
        ez = jnp.where(coarse_mid, from_tiles(back, rows, cols), new)
        picked = jnp.dot(
            rcv_rows, ez, precision=lax.Precision.HIGHEST, preferred_element_type=jnp.float32
        )
        samples.append(jnp.sum(picked * rcv_cols, axis=1))
    traces = lax.psum(jnp.stack(samples), ("grp", "gx", "gy"))
    return (
        ez,
        hx,
        hy,
        field_ez.reshape(fine_shape),
        field_hx.reshape(fine_shape),
        field_hy.reshape(fine_shape),
        traces,
    )


def solution(mesh):
    placed = (
        P("gx", ("grp", "gy")),
        P("gx", ("grp", "gy")),
        P("gx", ("grp", "gy")),
        P("gx", ("grp", "gy")),
        P(),
        P(),
        P(None, ("grp", "gy"), "gx", None),
        P(None, ("grp", "gy"), "gx", None),
        P(None, ("grp", "gy"), "gx", None),
        P(None, ("grp", "gy"), "gx", None),
        P("gx", ("grp", "gy"), None, None),
        P(),
        P(),
        P(),
    )
    def body(*args):
        rows, cols = args[0].shape
        owners = lax.axis_size("gx")
        strips = cols == LANES and args[6].shape[2] * TILE == cols and rows == owners * TILE
        if strips and owners == 4 and 5 * GROUP * owners <= LANES and args[13].shape[0] == LANES:
            return fast_shards(*args)
        return shards(*args)

    return jax.shard_map(
        body,
        mesh=mesh,
        in_specs=placed,
        out_specs=(
            P("gx", ("grp", "gy")),
            P("gx", ("grp", "gy")),
            P("gx", ("grp", "gy")),
            P(None, ("grp", "gy"), "gx", None),
            P(None, ("grp", "gy"), "gx", None),
            P(None, ("grp", "gy"), "gx", None),
            P(),
        ),
        check_vma=False,
    )
```
